8 devices in a mesh: dp: 2 (over z, y), tp: 4 (over x, core).
Axes of the slice: x: 2, y: 2, z: 1, core: 2. Of those that a mesh axis runs over, the one named last changes fastest.
Arguments:
- x_rows: bfloat16 [8192, 1536], P(('dp', 'tp')), parts along dimension 0
- norm_gain: float32 [1536], replicated
- w_q: bfloat16 [1536, 12, 128], P(None, 'tp')
- w_k: bfloat16 [1536, 256], P(None, 'tp')
- w_v: bfloat16 [1536, 256], P(None, 'tp')
Outputs:
- output 1: bfloat16 [8192, 12, 128], P('dp', 'tp'), parts along dimension 0
- output 2: bfloat16 [8192, 4, 128], P('dp', 'tp'), parts along dimension 0
- output 3: bfloat16 [8192, 4, 128], P('dp', 'tp'), parts along dimension 0
There are 2 independent parts. The reference program is written for one: setup_inputs(seed, part) draws one part's arguments, and reference() takes and returns one part's arrays. A program takes and returns all parts, laid end to end along the dimension named above; an argument that names none is the same for every part.
All inputs are finite; a program needn't handle non-finite values.
Results may differ from the reference program's by a relative error of at most 0.001.
Values are sent between devices in bfloat16 or wider.
A program may use at most 1 GiB of HBM per device.

```python
import jax
import jax.numpy as jnp
from jax import lax

TOKENS = 4096
D_MODEL = 1536
Q_HEADS = 12
KV_COUNT = 2
HEAD_DIM = 128
GROUP_SIZE = 4
EPSILON = 1e-6


def setup_inputs(seed: int = 0, part: int = 0) -> dict:
    key = jax.random.key(seed)
    shared_key, rows_key = jax.random.split(key)
    part_key = jax.random.fold_in(rows_key, part)
    x_rows = jax.random.normal(part_key, (TOKENS, D_MODEL), jnp.float32).astype(jnp.bfloat16)
    gain_key, q_key, k_key, v_key = jax.random.split(shared_key, 4)
    norm_gain = jax.random.uniform(gain_key, (D_MODEL,), jnp.float32, 0.4, 1.6)
    weight_scale = D_MODEL ** -0.5
    w_q = (jax.random.normal(q_key, (D_MODEL, Q_HEADS, HEAD_DIM), jnp.float32) * weight_scale).astype(jnp.bfloat16)
    w_k = (jax.random.normal(k_key, (D_MODEL, KV_COUNT * HEAD_DIM), jnp.float32) * weight_scale).astype(jnp.bfloat16)
    w_v = (jax.random.normal(v_key, (D_MODEL, KV_COUNT * HEAD_DIM), jnp.float32) * weight_scale).astype(jnp.bfloat16)
    return {"x_rows": x_rows, "norm_gain": norm_gain, "w_q": w_q, "w_k": w_k, "w_v": w_v}


def reference(x_rows, norm_gain, w_q, w_k, w_v):
    x_wide = x_rows.astype(jnp.float32)
    mean_sq = jnp.mean(x_wide * x_wide, axis=-1, keepdims=True)
    normed = (x_wide * lax.rsqrt(mean_sq + EPSILON) * norm_gain).astype(jnp.bfloat16)
    q_flat = jnp.dot(normed, w_q.reshape(D_MODEL, Q_HEADS * HEAD_DIM), preferred_element_type=jnp.float32)
    q_out = q_flat.astype(jnp.bfloat16).reshape(TOKENS, Q_HEADS, HEAD_DIM)
    head_share = GROUP_SIZE // KV_COUNT
    k_flat = jnp.dot(normed, w_k, preferred_element_type=jnp.float32).astype(jnp.bfloat16)
    v_flat = jnp.dot(normed, w_v, preferred_element_type=jnp.float32).astype(jnp.bfloat16)
    k_out = jnp.repeat(k_flat.reshape(TOKENS, KV_COUNT, HEAD_DIM), head_share, axis=1)
    v_out = jnp.repeat(v_flat.reshape(TOKENS, KV_COUNT, HEAD_DIM), head_share, axis=1)
    return (q_out, k_out, v_out)
```

```python
import functools

import jax
import jax.numpy as jnp
from jax import lax
from jax.experimental import pallas as pl
from jax.experimental.pallas import tpu as pltpu
from jax.sharding import PartitionSpec as P

EPSILON = 1e-6
MESH = pl.DeviceIdType.MESH
LANES = 128
K_PIECE, V_PIECE, FIRST_HEAD = 0, 1, 2


def qkv_kernel(
    x_hbm, gain_hbm, wq_hbm, wk_hbm, wv_hbm,
    q_out, k_out, v_out,
    rows_buf, gain_buf, wq_buf, wkv_buf, q_stage, kv_stage,
    x_sem, gain_sem, load_sem,
    part_send, part_recv, link_send, link_recv, core_send, core_recv, side_send, side_recv, last_send, last_recv,
    near_send, near_recv, far_send, far_recv, cross_send, cross_recv, pass_send, pass_recv,
    *, norm_tile, dot_tile,
):
    n_rows, depth = rows_buf.shape
    heads = wq_hbm.shape[0]
    share = wk_hbm.shape[0]
    half = depth // 2
    pieces = FIRST_HEAD + heads

    group, member = lax.axis_index("dp"), lax.axis_index("tp")
    chip, core = member // 2, member % 2
    partner = (group, chip * 2 + (1 - core))
    across = (group, (1 - chip) * 2 + core)
    across_other = (group, (1 - chip) * 2 + (1 - core))
    beside = (1 - group, member)

    sources = [wk_hbm, wv_hbm] + [wq_hbm.at[h] for h in range(heads)]

    def piece_at(j, slot, depth_half=None):
        if j < FIRST_HEAD:
            rows = pl.ds(pl.multiple_of(j * 2 * share + core * share, share), share)
            if depth_half is None:
                return wkv_buf.at[slot // 2, rows]
            return wkv_buf.at[slot // 2, rows, pl.ds(pl.multiple_of(depth_half * half, half), half)]
        if depth_half is None:
            return wq_buf.at[slot, j - FIRST_HEAD]
        return wq_buf.at[slot, j - FIRST_HEAD, pl.ds(pl.multiple_of(depth_half * half, half), half)]

    loads = [pltpu.make_async_copy(sources[j], piece_at(j, 0), load_sem.at[j]) for j in range(pieces)]
    for load in loads:
        load.start()
    gain_load = pltpu.make_async_copy(gain_hbm, gain_buf, gain_sem)
    gain_load.start()
    n_tiles = n_rows // norm_tile
    x_loads = [
        pltpu.make_async_copy(x_hbm.at[pl.ds(i * norm_tile, norm_tile)], rows_buf.at[pl.ds(i * norm_tile, norm_tile)], x_sem.at[i])
        for i in range(n_tiles)
    ]
    for load in x_loads:
        load.start()

    barrier = pltpu.get_barrier_semaphore()
    for other in (across, beside, across_other, partner):
        pl.semaphore_signal(barrier, inc=1, device_id=other, device_id_type=MESH)
    pl.semaphore_wait(barrier, 4)

    def remote(src, dst, send, recv, device):
        return pltpu.make_async_remote_copy(src_ref=src, dst_ref=dst, send_sem=send, recv_sem=recv, device_id=device, device_id_type=MESH)

    part, link, hand, side, last = [], [], [], [], []
    for j in range(pieces):
        part.append(remote(piece_at(j, 0), piece_at(j, 0 if j < FIRST_HEAD else 1), part_send.at[j], part_recv.at[j], partner))
        link.append(remote(piece_at(j, 0, group), piece_at(j, 2, group), link_send.at[j], link_recv.at[j], across))
        arrived, other_half = piece_at(j, 2, group), piece_at(j, 2, 1 - group)
        hand.append(remote(arrived, piece_at(j, 2 if j < FIRST_HEAD else 3, group), core_send.at[j], core_recv.at[j], partner))
        side.append(remote(arrived, arrived, side_send.at[j], side_recv.at[j], beside))
        last.append(remote(other_half, piece_at(j, 2 if j < FIRST_HEAD else 3, 1 - group), last_send.at[j], last_recv.at[j], partner))

    my_rows = pl.ds(pl.multiple_of(member * n_rows, n_rows), n_rows)
    across_rows = pl.ds(pl.multiple_of(((1 - chip) * 2 + core) * n_rows, n_rows), n_rows)
    near = [remote(k_out.at[0, my_rows], k_out.at[0, my_rows], near_send.at[0], near_recv.at[0], partner),
            remote(v_out.at[0, my_rows], v_out.at[0, my_rows], near_send.at[1], near_recv.at[1], partner)]
    far = [remote(kv_stage.at[0], k_out.at[0, my_rows], far_send.at[0], far_recv.at[0], across),
           remote(kv_stage.at[1], v_out.at[0, my_rows], far_send.at[1], far_recv.at[1], across)]
    passed = [remote(k_out.at[0, across_rows], k_out.at[0, across_rows], pass_send.at[0], pass_recv.at[0], partner),
              remote(v_out.at[0, across_rows], v_out.at[0, across_rows], pass_send.at[1], pass_recv.at[1], partner)]
    cross = []
    for h in range(heads):
        near.append(remote(q_stage.at[0, h], q_out.at[h, my_rows], near_send.at[2 + h], near_recv.at[2 + h], partner))
        far.append(remote(q_stage.at[1, h], q_out.at[h, my_rows], far_send.at[2 + h], far_recv.at[2 + h], across))
        cross.append(remote(q_stage.at[2, h], q_out.at[h, my_rows], cross_send.at[h], cross_recv.at[h], across_other))

    for j in range(pieces):
        loads[j].wait()
        link[j].start()
        part[j].start()

    gain_load.wait()
    chunks = depth // LANES
    sub = 64

    for i in range(n_tiles):
        x_loads[i].wait()

    def norm_step(s, carry):
        here = pl.ds(pl.multiple_of(s * sub, sub), sub)
        total = jnp.zeros((sub, LANES), jnp.float32)
        for c in range(chunks):
            wide = rows_buf[here, c * LANES:(c + 1) * LANES].astype(jnp.float32)
            total = total + wide * wide
        scale = lax.rsqrt(jnp.sum(total, axis=-1, keepdims=True) / depth + EPSILON)
        for c in range(chunks):
            cols = slice(c * LANES, (c + 1) * LANES)
            wide = rows_buf[here, cols].astype(jnp.float32)
            rows_buf[here, cols] = (wide * scale * gain_buf[cols][None, :]).astype(jnp.bfloat16)
        return carry

    lax.fori_loop(0, n_rows // sub, norm_step, 0)

    def over_tiles(step):
        lax.fori_loop(0, n_rows // dot_tile, lambda i, carry: (step(i * dot_tile), carry)[1], 0)

    def q_block(slot, h, store):
        def step(start):
            tile = rows_buf[pl.ds(pl.multiple_of(start, dot_tile), dot_tile), :]
            store(start, jnp.dot(tile, wq_buf[slot, h], preferred_element_type=jnp.float32).astype(jnp.bfloat16))
        over_tiles(step)

    def kv_block(which, store):
        def step(start):
            tile = rows_buf[pl.ds(pl.multiple_of(start, dot_tile), dot_tile), :]
            both = lax.dot_general(tile, wkv_buf[which], (((1,), (1,)), ((), ())), preferred_element_type=jnp.float32)
            store(start, both.astype(jnp.bfloat16))
        over_tiles(step)

    def rows_at(start):
        return pl.ds(pl.multiple_of(start, dot_tile), dot_tile)

    def own_rows_at(start):
        return pl.ds(pl.multiple_of(member * n_rows + start, dot_tile), dot_tile)

    def own_q(h):
        def store(start, value):
            q_out[h, own_rows_at(start), :] = value
        q_block(0, h, store)

    def staged_q(stage, slot, h):
        def store(start, value):
            q_stage[stage, h, rows_at(start), :] = value
        q_block(slot, h, store)

    def own_kv():
        def store(start, value):
            k_out[0, own_rows_at(start), :] = value[:, :LANES]
            v_out[0, own_rows_at(start), :] = value[:, LANES:]
        kv_block(0, store)

    def far_kv():
        def store(start, value):
            kv_stage[0, rows_at(start), :] = value[:, :LANES]
            kv_stage[1, rows_at(start), :] = value[:, LANES:]
        kv_block(1, store)

    def from_link(j):
        link[j].wait_recv()
        side[j].start()
        hand[j].start()

    def from_side(j):
        side[j].wait_recv()
        last[j].start()

    def complete(j):
        hand[j].wait_recv()
        last[j].wait_recv()

    from_link(K_PIECE)
    from_link(V_PIECE)
    part[K_PIECE].wait_recv()
    part[V_PIECE].wait_recv()
    own_kv()
    from_side(K_PIECE)
    near[0].start()
    near[1].start()
    from_link(2)
    from_side(V_PIECE)
    own_q(0)
    complete(K_PIECE)
    complete(V_PIECE)
    far_kv()
    own_q(1)
    far[0].start()
    far[1].start()
    from_link(3)
    own_q(2)
    from_side(2)
    staged_q(1, 2, 0)
    from_link(4)
    complete(2)
    staged_q(2, 3, 0)
    far[2].start()
    from_side(3)
    staged_q(1, 2, 1)
    cross[0].start()
    complete(3)
    staged_q(2, 3, 1)
    far[3].start()
    from_side(4)
    staged_q(1, 2, 2)
    cross[1].start()
    complete(4)
    staged_q(2, 3, 2)
    far[4].start()
    for h in range(heads):
        part[FIRST_HEAD + h].wait_recv()
        staged_q(0, 1, h)
        if h == 0:
            cross[2].start()
        else:
            near[2 + h - 1].start()
    far[0].wait_recv()
    passed[0].start()
    far[1].wait_recv()
    passed[1].start()
    near[2 + heads - 1].start()

    for copy in part + link + hand + side + last:
        copy.wait_send()
    for copy in near:
        copy.wait()
    for copy in passed:
        copy.wait()
    for j, copy in enumerate(far):
        copy.wait_send()
        if j >= FIRST_HEAD:
            copy.wait_recv()
    for copy in cross:
        copy.wait()


def solution(mesh):
    def local_step(x_rows, norm_gain, w_q, w_k, w_v):
        n_rows, depth = x_rows.shape
        heads, width = w_q.shape[1:]
        share = w_k.shape[1]
        members = mesh.shape["tp"]
        pieces = FIRST_HEAD + heads
        all_rows = members * n_rows
        dma = pltpu.SemaphoreType.DMA
        norm_tile = n_rows // 4
        out_spec = pl.BlockSpec(memory_space=pltpu.VMEM)
        hbm = pl.BlockSpec(memory_space=pltpu.HBM)
        q, k, v = pl.pallas_call(
            functools.partial(qkv_kernel, norm_tile=norm_tile, dot_tile=256),
            out_shape=(
                jax.ShapeDtypeStruct((heads, all_rows, width), jnp.bfloat16),
                jax.ShapeDtypeStruct((1, all_rows, width), jnp.bfloat16),
                jax.ShapeDtypeStruct((1, all_rows, width), jnp.bfloat16),
            ),
            in_specs=[hbm] * 5,
            out_specs=(out_spec,) * 3,
            scratch_shapes=[
                pltpu.VMEM((n_rows, depth), jnp.bfloat16),
                pltpu.VMEM((depth,), jnp.float32),
                pltpu.VMEM((4, heads, depth, width), jnp.bfloat16),
                pltpu.VMEM((2, 4 * share, depth), jnp.bfloat16),
                pltpu.VMEM((3, heads, n_rows, width), jnp.bfloat16),
                pltpu.VMEM((2, n_rows, width), jnp.bfloat16),
                dma((4,)), dma(()), dma((pieces,)),
                *[dma((pieces,)) for _ in range(10)],
                dma((pieces,)), dma((pieces,)), dma((pieces,)), dma((pieces,)),
                dma((heads,)), dma((heads,)), dma((2,)), dma((2,)),
            ],
            compiler_params=pltpu.CompilerParams(collective_id=0, has_side_effects=True, vmem_limit_bytes=36 * 1024 * 1024),
            cost_estimate=pl.CostEstimate(flops=2 * n_rows * depth * 2048, bytes_accessed=16 * 1024 * 1024, transcendentals=0),
            name="qkv",
        )(*[pltpu.with_memory_space_constraint(a, pltpu.HBM) for a in (x_rows, norm_gain, w_q.transpose(1, 0, 2), w_k.T, w_v.T)])
        return q.transpose(1, 0, 2), k.transpose(1, 0, 2), v.transpose(1, 0, 2)

    return jax.shard_map(
        local_step, mesh=mesh,
        in_specs=(P(("dp", "tp"), None), P(None), P(None, "tp", None), P(None, "tp"), P(None, "tp")),
        out_specs=(P("dp", "tp", None), P("dp", "tp", None), P("dp", "tp", None)),
        check_vma=False,
    )
```

```python
import functools

import jax
import jax.numpy as jnp
from jax import lax
from jax.experimental import pallas as pl
from jax.experimental.pallas import tpu as pltpu
from jax.sharding import PartitionSpec as P

EPSILON = 1e-6
MESH = pl.DeviceIdType.MESH
LANES = 128
K_PIECE, V_PIECE, FIRST_HEAD = 0, 1, 2


def qkv_kernel(
    x_hbm, gain_hbm, wq_hbm, wk_hbm, wv_hbm,
    q_out, k_out, v_out,
    rows_buf, gain_buf, wq_buf, wkv_buf, q_stage, kv_stage,
    x_sem, gain_sem, load_sem,
    part_send, part_recv, link_send, link_recv, core_send, core_recv, side_send, side_recv, last_send, last_recv,
    near_send, near_recv, far_send, far_recv, cross_send, cross_recv, pass_send, pass_recv,
    *, norm_tile, dot_tile,
):
    n_rows, depth = rows_buf.shape
    heads = wq_hbm.shape[0]
    share = wk_hbm.shape[0]
    half = depth // 2
    pieces = FIRST_HEAD + heads

    group, member = lax.axis_index("dp"), lax.axis_index("tp")
    chip, core = member // 2, member % 2
    partner = (group, chip * 2 + (1 - core))
    across = (group, (1 - chip) * 2 + core)
    across_other = (group, (1 - chip) * 2 + (1 - core))
    beside = (1 - group, member)

    barrier = pltpu.get_barrier_semaphore()
    for other in (across_other, across, beside, partner):
        pl.semaphore_signal(barrier, inc=1, device_id=other, device_id_type=MESH)

    sources = [wk_hbm, wv_hbm] + [wq_hbm.at[h] for h in range(heads)]

    def piece_at(j, slot, depth_half=None):
        if j < FIRST_HEAD:
            rows = pl.ds(pl.multiple_of(j * 2 * share + core * share, share), share)
            if depth_half is None:
                return wkv_buf.at[slot // 2, rows]
            return wkv_buf.at[slot // 2, rows, pl.ds(pl.multiple_of(depth_half * half, half), half)]
        if depth_half is None:
            return wq_buf.at[slot, j - FIRST_HEAD]
        return wq_buf.at[slot, j - FIRST_HEAD, pl.ds(pl.multiple_of(depth_half * half, half), half)]

    loads = [pltpu.make_async_copy(sources[j], piece_at(j, 0), load_sem.at[j]) for j in range(pieces)]
    for load in loads:
        load.start()
    gain_load = pltpu.make_async_copy(gain_hbm, gain_buf, gain_sem)
    gain_load.start()
    n_tiles = n_rows // norm_tile
    x_loads = [
        pltpu.make_async_copy(x_hbm.at[pl.ds(i * norm_tile, norm_tile)], rows_buf.at[pl.ds(i * norm_tile, norm_tile)], x_sem.at[i])
        for i in range(n_tiles)
    ]
    for load in x_loads:
        load.start()

    pl.semaphore_wait(barrier, 4)

    def remote(src, dst, send, recv, device):
        return pltpu.make_async_remote_copy(src_ref=src, dst_ref=dst, send_sem=send, recv_sem=recv, device_id=device, device_id_type=MESH)

    part, link, hand, side, last = [], [], [], [], []
    for j in range(pieces):
        part.append(remote(piece_at(j, 0), piece_at(j, 0 if j < FIRST_HEAD else 1), part_send.at[j], part_recv.at[j], partner))
        link.append(remote(piece_at(j, 0, group), piece_at(j, 2, group), link_send.at[j], link_recv.at[j], across))
        arrived, other_half = piece_at(j, 2, group), piece_at(j, 2, 1 - group)
        hand.append(remote(arrived, piece_at(j, 2 if j < FIRST_HEAD else 3, group), core_send.at[j], core_recv.at[j], partner))
        side.append(remote(arrived, arrived, side_send.at[j], side_recv.at[j], beside))
        last.append(remote(other_half, piece_at(j, 2 if j < FIRST_HEAD else 3, 1 - group), last_send.at[j], last_recv.at[j], partner))

    my_rows = pl.ds(pl.multiple_of(member * n_rows, n_rows), n_rows)
    across_rows = pl.ds(pl.multiple_of(((1 - chip) * 2 + core) * n_rows, n_rows), n_rows)
    near = [remote(k_out.at[0, my_rows], k_out.at[0, my_rows], near_send.at[0], near_recv.at[0], partner),
            remote(v_out.at[0, my_rows], v_out.at[0, my_rows], near_send.at[1], near_recv.at[1], partner)]
    far = [remote(kv_stage.at[0], k_out.at[0, my_rows], far_send.at[0], far_recv.at[0], across),
           remote(kv_stage.at[1], v_out.at[0, my_rows], far_send.at[1], far_recv.at[1], across)]
    passed = [remote(k_out.at[0, across_rows], k_out.at[0, across_rows], pass_send.at[0], pass_recv.at[0], partner),
              remote(v_out.at[0, across_rows], v_out.at[0, across_rows], pass_send.at[1], pass_recv.at[1], partner)]
    cross = []
    for h in range(heads):
        near.append(remote(q_stage.at[0, h], q_out.at[h, my_rows], near_send.at[2 + h], near_recv.at[2 + h], partner))
        far.append(remote(q_stage.at[1, h], q_out.at[h, my_rows], far_send.at[2 + h], far_recv.at[2 + h], across))
        cross.append(remote(q_stage.at[2, h], q_out.at[h, my_rows], cross_send.at[h], cross_recv.at[h], across_other))

    for j in range(pieces):
        loads[j].wait()
        link[j].start()
        part[j].start()

    gain_load.wait()
    chunks = depth // LANES
    sub = 64

    for i in range(n_tiles):
        x_loads[i].wait()

    def norm_step(s, carry):
        here = pl.ds(pl.multiple_of(s * sub, sub), sub)
        total = jnp.zeros((sub, LANES), jnp.float32)
        for c in range(chunks):
            wide = rows_buf[here, c * LANES:(c + 1) * LANES].astype(jnp.float32)
            total = total + wide * wide
        scale = lax.rsqrt(jnp.sum(total, axis=-1, keepdims=True) / depth + EPSILON)
        for c in range(chunks):
            cols = slice(c * LANES, (c + 1) * LANES)
            wide = rows_buf[here, cols].astype(jnp.float32)
            rows_buf[here, cols] = (wide * scale * gain_buf[cols][None, :]).astype(jnp.bfloat16)
        return carry

    lax.fori_loop(0, n_rows // sub, norm_step, 0)

    def over_tiles(step):
        lax.fori_loop(0, n_rows // dot_tile, lambda i, carry: (step(i * dot_tile), carry)[1], 0)

    def q_block(slot, h, store):
        def step(start):
            tile = rows_buf[pl.ds(pl.multiple_of(start, dot_tile), dot_tile), :]
            store(start, jnp.dot(tile, wq_buf[slot, h], preferred_element_type=jnp.float32).astype(jnp.bfloat16))
        over_tiles(step)

    def kv_block(which, store):
        def step(start):
            tile = rows_buf[pl.ds(pl.multiple_of(start, dot_tile), dot_tile), :]
            both = lax.dot_general(tile, wkv_buf[which], (((1,), (1,)), ((), ())), preferred_element_type=jnp.float32)
            store(start, both.astype(jnp.bfloat16))
        over_tiles(step)

    def rows_at(start):
        return pl.ds(pl.multiple_of(start, dot_tile), dot_tile)

    def own_rows_at(start):
        return pl.ds(pl.multiple_of(member * n_rows + start, dot_tile), dot_tile)

    def own_q(h):
        def store(start, value):
            q_out[h, own_rows_at(start), :] = value
        q_block(0, h, store)

    def staged_q(stage, slot, h):
        def store(start, value):
            q_stage[stage, h, rows_at(start), :] = value
        q_block(slot, h, store)

    def own_kv():
        def store(start, value):
            k_out[0, own_rows_at(start), :] = value[:, :LANES]
            v_out[0, own_rows_at(start), :] = value[:, LANES:]
        kv_block(0, store)

    def far_kv():
        def store(start, value):
            kv_stage[0, rows_at(start), :] = value[:, :LANES]
            kv_stage[1, rows_at(start), :] = value[:, LANES:]
        kv_block(1, store)

    def from_link(j):
        link[j].wait_recv()
        side[j].start()
        hand[j].start()

    def from_side(j):
        side[j].wait_recv()
        last[j].start()

    def complete(j):
        hand[j].wait_recv()
        last[j].wait_recv()

    from_link(K_PIECE)
    from_link(V_PIECE)
    part[K_PIECE].wait_recv()
    part[V_PIECE].wait_recv()
    own_kv()
    from_side(K_PIECE)
    near[0].start()
    near[1].start()
    from_link(2)
    from_side(V_PIECE)
    own_q(0)
    complete(K_PIECE)
    complete(V_PIECE)
    far_kv()
    own_q(1)
    far[0].start()
    far[1].start()
    from_link(3)
    own_q(2)
    from_side(2)
    staged_q(1, 2, 0)
    from_link(4)
    complete(2)
    staged_q(2, 3, 0)
    far[2].start()
    from_side(3)
    staged_q(1, 2, 1)
    cross[0].start()
    complete(3)
    staged_q(2, 3, 1)
    far[3].start()
    from_side(4)
    staged_q(1, 2, 2)
    cross[1].start()
    complete(4)
    staged_q(2, 3, 2)
    far[4].start()
    for h in range(heads):
        part[FIRST_HEAD + h].wait_recv()
        staged_q(0, 1, h)
        if h == 0:
            cross[2].start()
        else:
            near[2 + h - 1].start()
    far[0].wait_recv()
    passed[0].start()
    far[1].wait_recv()
    passed[1].start()
    near[2 + heads - 1].start()

    for copy in part + link + hand + side + last:
        copy.wait_send()
    for copy in near:
        copy.wait()
    for copy in passed:
        copy.wait()
    for j, copy in enumerate(far):
        copy.wait_send()
        if j >= FIRST_HEAD:
            copy.wait_recv()
    for copy in cross:
        copy.wait()


def finish_kernel(q_ref, k_ref, v_ref, q_out, k_out, v_out, sems, *, cuts):
    copies = []
    for ref, out in ((q_ref, q_out), (k_ref, k_out), (v_ref, v_out)):
        rows = ref.shape[1] // cuts
        for h in range(ref.shape[0]):
            for cut in range(cuts):
                where = pl.ds(cut * rows, rows)
                copies.append(pltpu.make_async_copy(ref.at[h, where], out.at[h, where], sems.at[len(copies)]))
    for copy in copies:
        copy.start()
    for copy in copies:
        copy.wait()


def solution(mesh):
    def local_step(x_rows, norm_gain, w_q, w_k, w_v):
        n_rows, depth = x_rows.shape
        heads, width = w_q.shape[1:]
        share = w_k.shape[1]
        members = mesh.shape["tp"]
        pieces = FIRST_HEAD + heads
        all_rows = members * n_rows
        dma = pltpu.SemaphoreType.DMA
        norm_tile = n_rows // 4
        out_spec = pl.BlockSpec(memory_space=pltpu.VMEM)
        hbm = pl.BlockSpec(memory_space=pltpu.HBM)
        q, k, v = pl.pallas_call(
            functools.partial(qkv_kernel, norm_tile=norm_tile, dot_tile=256),
            out_shape=(
                jax.ShapeDtypeStruct((heads, all_rows, width), jnp.bfloat16),
                jax.ShapeDtypeStruct((1, all_rows, width), jnp.bfloat16),
                jax.ShapeDtypeStruct((1, all_rows, width), jnp.bfloat16),
            ),
            in_specs=[hbm] * 5,
            out_specs=(out_spec,) * 3,
            scratch_shapes=[
                pltpu.VMEM((n_rows, depth), jnp.bfloat16),
                pltpu.VMEM((depth,), jnp.float32),
                pltpu.VMEM((4, heads, depth, width), jnp.bfloat16),
                pltpu.VMEM((2, 4 * share, depth), jnp.bfloat16),
                pltpu.VMEM((3, heads, n_rows, width), jnp.bfloat16),
                pltpu.VMEM((2, n_rows, width), jnp.bfloat16),
                dma((4,)), dma(()), dma((pieces,)),
                *[dma((pieces,)) for _ in range(10)],
                dma((pieces,)), dma((pieces,)), dma((pieces,)), dma((pieces,)),
                dma((heads,)), dma((heads,)), dma((2,)), dma((2,)),
            ],
            compiler_params=pltpu.CompilerParams(collective_id=0, has_side_effects=True, vmem_limit_bytes=36 * 1024 * 1024),
            cost_estimate=pl.CostEstimate(flops=2 * n_rows * depth * 2048, bytes_accessed=16 * 1024 * 1024, transcendentals=0),
            name="qkv",
        )(*[pltpu.with_memory_space_constraint(a, pltpu.HBM) for a in (x_rows, norm_gain, w_q.transpose(1, 0, 2), w_k.T, w_v.T)])
        cuts = 2
        vmem = pl.BlockSpec(memory_space=pltpu.VMEM)
        q, k, v = pl.pallas_call(
            functools.partial(finish_kernel, cuts=cuts),
            out_shape=tuple(jax.ShapeDtypeStruct(a.shape, a.dtype) for a in (q, k, v)),
            in_specs=[vmem] * 3,
            out_specs=(hbm,) * 3,
            scratch_shapes=[dma((cuts * (heads + 2),))],
            compiler_params=pltpu.CompilerParams(vmem_limit_bytes=16 * 1024 * 1024),
            name="finish",
        )(q, k, v)
        return q.transpose(1, 0, 2), k.transpose(1, 0, 2), v.transpose(1, 0, 2)

    return jax.shard_map(
        local_step, mesh=mesh,
        in_specs=(P(("dp", "tp"), None), P(None), P(None, "tp", None), P(None, "tp"), P(None, "tp")),
        out_specs=(P("dp", "tp", None), P("dp", "tp", None), P("dp", "tp", None)),
        check_vma=False,
    )
```

```python
import functools

import jax
import jax.numpy as jnp
from jax import lax
from jax.experimental import pallas as pl
from jax.experimental.pallas import tpu as pltpu
from jax.sharding import PartitionSpec as P

EPSILON = 1e-6
MESH = pl.DeviceIdType.MESH
LANES = 128
K_PIECE, V_PIECE, FIRST_HEAD = 0, 1, 2


def qkv_kernel(
    x_hbm, gain_hbm, wq_hbm, wk_hbm, wv_hbm,
    q_out, k_out, v_out,
    rows_buf, gain_buf, wq_buf, wkv_buf, q_stage, kv_stage,
    x_sem, gain_sem, load_sem,
    part_send, part_recv, link_send, link_recv, core_send, core_recv, side_send, side_recv, last_send, last_recv,
    middle_send, middle_recv, ready_sem,
    near_send, near_recv, far_send, far_recv, cross_send, cross_recv, pass_send, pass_recv,
    *, norm_tile, dot_tile, shift,
):
    n_rows, depth = rows_buf.shape
    heads = wq_hbm.shape[0]
    share = wk_hbm.shape[0]
    half = depth // 2
    pieces = FIRST_HEAD + heads

    group, member = lax.axis_index("dp"), lax.axis_index("tp")
    chip, core = member // 2, member % 2
    partner = (group, chip * 2 + (1 - core))
    across = (group, (1 - chip) * 2 + core)
    across_other = (group, (1 - chip) * 2 + (1 - core))
    beside = (1 - group, member)

    barrier = pltpu.get_barrier_semaphore()
    for other in (across_other, across, partner):
        pl.semaphore_signal(barrier, inc=1, device_id=other, device_id_type=MESH)

    @pl.when(group == 0)
    def _():
        pl.semaphore_signal(barrier, inc=1, device_id=beside, device_id_type=MESH)

    sources = [wk_hbm, wv_hbm] + [wq_hbm.at[h] for h in range(heads)]

    last_head = pieces - 1
    middle = pl.ds(half - shift, 2 * shift)

    def piece_at(j, slot, depth_half=None):
        if j < FIRST_HEAD:
            rows = pl.ds(pl.multiple_of(j * 2 * share + core * share, share), share)
            if depth_half is None:
                return wkv_buf.at[slot // 2, rows]
            return wkv_buf.at[slot // 2, rows, pl.ds(pl.multiple_of(depth_half * half, half), half)]
        if depth_half is None:
            return wq_buf.at[slot, j - FIRST_HEAD]
        if j == last_head:
            start = pl.multiple_of(depth_half * (half + shift), shift)
            return wq_buf.at[slot, j - FIRST_HEAD, pl.ds(start, half - shift)]
        return wq_buf.at[slot, j - FIRST_HEAD, pl.ds(pl.multiple_of(depth_half * half, half), half)]

    loads = [pltpu.make_async_copy(sources[j], piece_at(j, 0), load_sem.at[j]) for j in range(pieces)]
    for load in loads[:FIRST_HEAD]:
        load.start()
    gain_load = pltpu.make_async_copy(gain_hbm, gain_buf, gain_sem)
    n_tiles = n_rows // norm_tile
    x_loads = [
        pltpu.make_async_copy(x_hbm.at[pl.ds(i * norm_tile, norm_tile)], rows_buf.at[pl.ds(i * norm_tile, norm_tile)], x_sem.at[i])
        for i in range(n_tiles)
    ]
    pl.semaphore_wait(barrier, 3 + group)

    def remote(src, dst, send, recv, device):
        return pltpu.make_async_remote_copy(src_ref=src, dst_ref=dst, send_sem=send, recv_sem=recv, device_id=device, device_id_type=MESH)

    part, link, hand, side, last = [], [], [], [], []
    for j in range(pieces):
        part.append(remote(piece_at(j, 0), piece_at(j, 0 if j < FIRST_HEAD else 1), part_send.at[j], part_recv.at[j], partner))
        link.append(remote(piece_at(j, 0, group), piece_at(j, 2, group), link_send.at[j], link_recv.at[j], across))
        arrived, other_half = piece_at(j, 2, group), piece_at(j, 2, 1 - group)
        hand.append(remote(arrived, piece_at(j, 2 if j < FIRST_HEAD else 3, group), core_send.at[j], core_recv.at[j], partner))
        side.append(remote(arrived, arrived, side_send.at[j], side_recv.at[j], beside))
        last.append(remote(other_half, piece_at(j, 2 if j < FIRST_HEAD else 3, 1 - group), last_send.at[j], last_recv.at[j], partner))

    def middle_at(slot):
        return wq_buf.at[slot, heads - 1, middle]

    middle_link = remote(middle_at(0), middle_at(2), middle_send.at[0], middle_recv.at[0], across)
    middle_side = remote(middle_at(2), middle_at(2), middle_send.at[1], middle_recv.at[1], beside)
    middle_hand = remote(middle_at(2), middle_at(3), middle_send.at[2], middle_recv.at[2], partner)

    my_rows = pl.ds(pl.multiple_of(member * n_rows, n_rows), n_rows)
    across_rows = pl.ds(pl.multiple_of(((1 - chip) * 2 + core) * n_rows, n_rows), n_rows)
    near = [remote(k_out.at[0, my_rows], k_out.at[0, my_rows], near_send.at[0], near_recv.at[0], partner),
            remote(v_out.at[0, my_rows], v_out.at[0, my_rows], near_send.at[1], near_recv.at[1], partner)]
    far = [remote(kv_stage.at[0], k_out.at[0, my_rows], far_send.at[0], far_recv.at[0], across),
           remote(kv_stage.at[1], v_out.at[0, my_rows], far_send.at[1], far_recv.at[1], across)]
    passed = [remote(k_out.at[0, across_rows], k_out.at[0, across_rows], pass_send.at[0], pass_recv.at[0], partner),
              remote(v_out.at[0, across_rows], v_out.at[0, across_rows], pass_send.at[1], pass_recv.at[1], partner)]
    cross = []
    for h in range(heads):
        near.append(remote(q_stage.at[0, h], q_out.at[h, my_rows], near_send.at[2 + h], near_recv.at[2 + h], partner))
        far.append(remote(q_stage.at[1, h], q_out.at[h, my_rows], far_send.at[2 + h], far_recv.at[2 + h], across))
        cross.append(remote(q_stage.at[2, h], q_out.at[h, my_rows], cross_send.at[h], cross_recv.at[h], across_other))

    loads[0].wait()
    link[0].start()
    for load in loads[FIRST_HEAD:]:
        load.start()
    gain_load.start()
    for load in x_loads:
        load.start()
    for j in range(1, pieces):
        loads[j].wait()
        link[j].start()

    @pl.when(group == 1)
    def _():
        middle_link.start()
        pl.semaphore_signal(ready_sem, inc=1, device_id=beside, device_id_type=MESH)

    for copy in part:
        copy.start()

    gain_load.wait()
    chunks = depth // LANES
    sub = 64

    for i in range(n_tiles):
        x_loads[i].wait()

    def norm_step(s, carry):
        here = pl.ds(pl.multiple_of(s * sub, sub), sub)
        total = jnp.zeros((sub, LANES), jnp.float32)
        for c in range(chunks):
            wide = rows_buf[here, c * LANES:(c + 1) * LANES].astype(jnp.float32)
            total = total + wide * wide
        scale = lax.rsqrt(jnp.sum(total, axis=-1, keepdims=True) / depth + EPSILON)
        for c in range(chunks):
            cols = slice(c * LANES, (c + 1) * LANES)
            wide = rows_buf[here, cols].astype(jnp.float32)
            rows_buf[here, cols] = (wide * scale * gain_buf[cols][None, :]).astype(jnp.bfloat16)
        return carry

    lax.fori_loop(0, n_rows // sub, norm_step, 0)

    def over_tiles(step):
        lax.fori_loop(0, n_rows // dot_tile, lambda i, carry: (step(i * dot_tile), carry)[1], 0)

    def q_block(slot, h, store):
        def step(start):
            tile = rows_buf[pl.ds(pl.multiple_of(start, dot_tile), dot_tile), :]
            store(start, jnp.dot(tile, wq_buf[slot, h], preferred_element_type=jnp.float32).astype(jnp.bfloat16))
        over_tiles(step)

    def kv_block(which, store):
        def step(start):
            tile = rows_buf[pl.ds(pl.multiple_of(start, dot_tile), dot_tile), :]
            both = lax.dot_general(tile, wkv_buf[which], (((1,), (1,)), ((), ())), preferred_element_type=jnp.float32)
            store(start, both.astype(jnp.bfloat16))
        over_tiles(step)

    def rows_at(start):
        return pl.ds(pl.multiple_of(start, dot_tile), dot_tile)

    def own_rows_at(start):
        return pl.ds(pl.multiple_of(member * n_rows + start, dot_tile), dot_tile)

    def own_q(h):
        def store(start, value):
            q_out[h, own_rows_at(start), :] = value
        q_block(0, h, store)

    def staged_q(stage, slot, h):
        def store(start, value):
            q_stage[stage, h, rows_at(start), :] = value
        q_block(slot, h, store)

    def own_kv():
        def store(start, value):
            k_out[0, own_rows_at(start), :] = value[:, :LANES]
            v_out[0, own_rows_at(start), :] = value[:, LANES:]
        kv_block(0, store)

    def far_kv():
        def store(start, value):
            kv_stage[0, rows_at(start), :] = value[:, :LANES]
            kv_stage[1, rows_at(start), :] = value[:, LANES:]
        kv_block(1, store)

    def from_link(j):
        link[j].wait_recv()
        side[j].start()
        hand[j].start()

    def from_side(j):
        side[j].wait_recv()
        last[j].start()

    def from_middle():
        @pl.when(group == 1)
        def _():
            middle_link.wait_recv()
            middle_side.start()

        @pl.when(group == 0)
        def _():
            middle_side.wait_recv()

        middle_hand.start()

    def complete(j):
        hand[j].wait_recv()
        last[j].wait_recv()

    @pl.when(group == 0)
    def _():
        pl.semaphore_wait(ready_sem, 1)

    from_link(K_PIECE)
    from_link(V_PIECE)
    part[K_PIECE].wait_recv()
    part[V_PIECE].wait_recv()
    own_kv()
    from_side(K_PIECE)
    near[0].start()
    near[1].start()
    from_link(2)
    from_side(V_PIECE)
    own_q(0)
    complete(K_PIECE)
    complete(V_PIECE)
    far_kv()
    own_q(1)
    far[0].start()
    far[1].start()
    from_link(3)
    own_q(2)
    from_side(2)
    staged_q(1, 2, 0)
    from_link(4)
    complete(2)
    staged_q(2, 3, 0)
    far[2].start()
    from_side(3)
    staged_q(1, 2, 1)
    cross[0].start()
    complete(3)
    staged_q(2, 3, 1)
    far[3].start()
    from_side(4)
    from_middle()
    staged_q(1, 2, 2)
    cross[1].start()
    complete(4)
    middle_hand.wait_recv()
    staged_q(2, 3, 2)
    far[4].start()
    for h in range(heads):
        part[FIRST_HEAD + h].wait_recv()
        staged_q(0, 1, h)
        if h == 0:
            cross[2].start()
        else:
            near[2 + h - 1].start()
    far[0].wait_recv()
    passed[0].start()
    far[1].wait_recv()
    passed[1].start()
    near[2 + heads - 1].start()

    for copy in part + link + hand + side + last + [middle_hand]:
        copy.wait_send()

    @pl.when(group == 1)
    def _():
        middle_link.wait_send()
        middle_side.wait_send()

    for copy in near:
        copy.wait()
    for copy in passed:
        copy.wait()
    for j, copy in enumerate(far):
        copy.wait_send()
        if j >= FIRST_HEAD:
            copy.wait_recv()
    for copy in cross:
        copy.wait()


def finish_kernel(q_ref, k_ref, v_ref, q_out, k_out, v_out, sems, *, cuts):
    copies = []
    for ref, out in ((q_ref, q_out), (k_ref, k_out), (v_ref, v_out)):
        rows = ref.shape[1] // cuts
        for h in range(ref.shape[0]):
            for cut in range(cuts):
                where = pl.ds(cut * rows, rows)
                copies.append(pltpu.make_async_copy(ref.at[h, where], out.at[h, where], sems.at[len(copies)]))
    for copy in copies:
        copy.start()
    for copy in copies:
        copy.wait()


def solution(mesh):
    def local_step(x_rows, norm_gain, w_q, w_k, w_v):
        n_rows, depth = x_rows.shape
        heads, width = w_q.shape[1:]
        share = w_k.shape[1]
        members = mesh.shape["tp"]
        pieces = FIRST_HEAD + heads
        all_rows = members * n_rows
        dma = pltpu.SemaphoreType.DMA
        norm_tile = n_rows // 4
        out_spec = pl.BlockSpec(memory_space=pltpu.VMEM)
        hbm = pl.BlockSpec(memory_space=pltpu.HBM)
        q, k, v = pl.pallas_call(
            functools.partial(qkv_kernel, norm_tile=norm_tile, dot_tile=256, shift=LANES),
            out_shape=(
                jax.ShapeDtypeStruct((heads, all_rows, width), jnp.bfloat16),
                jax.ShapeDtypeStruct((1, all_rows, width), jnp.bfloat16),
                jax.ShapeDtypeStruct((1, all_rows, width), jnp.bfloat16),
            ),
            in_specs=[hbm] * 5,
            out_specs=(out_spec,) * 3,
            scratch_shapes=[
                pltpu.VMEM((n_rows, depth), jnp.bfloat16),
                pltpu.VMEM((depth,), jnp.float32),
                pltpu.VMEM((4, heads, depth, width), jnp.bfloat16),
                pltpu.VMEM((2, 4 * share, depth), jnp.bfloat16),
                pltpu.VMEM((3, heads, n_rows, width), jnp.bfloat16),
                pltpu.VMEM((2, n_rows, width), jnp.bfloat16),
                dma((4,)), dma(()), dma((pieces,)),
                *[dma((pieces,)) for _ in range(10)],
                dma((3,)), dma((3,)), pltpu.SemaphoreType.REGULAR,
                dma((pieces,)), dma((pieces,)), dma((pieces,)), dma((pieces,)),
                dma((heads,)), dma((heads,)), dma((2,)), dma((2,)),
            ],
            compiler_params=pltpu.CompilerParams(collective_id=0, has_side_effects=True, vmem_limit_bytes=36 * 1024 * 1024),
            cost_estimate=pl.CostEstimate(flops=2 * n_rows * depth * 2048, bytes_accessed=16 * 1024 * 1024, transcendentals=0),
            name="qkv",
        )(*[pltpu.with_memory_space_constraint(a, pltpu.HBM) for a in (x_rows, norm_gain, w_q.transpose(1, 0, 2), w_k.T, w_v.T)])
        cuts = 2
        vmem = pl.BlockSpec(memory_space=pltpu.VMEM)
        q, k, v = pl.pallas_call(
            functools.partial(finish_kernel, cuts=cuts),
            out_shape=tuple(jax.ShapeDtypeStruct(a.shape, a.dtype) for a in (q, k, v)),
            in_specs=[vmem] * 3,
            out_specs=(hbm,) * 3,
            scratch_shapes=[dma((cuts * (heads + 2),))],
            compiler_params=pltpu.CompilerParams(vmem_limit_bytes=16 * 1024 * 1024),
            name="finish",
        )(q, k, v)
        return q.transpose(1, 0, 2), k.transpose(1, 0, 2), v.transpose(1, 0, 2)

    return jax.shard_map(
        local_step, mesh=mesh,
        in_specs=(P(("dp", "tp"), None), P(None), P(None, "tp", None), P(None, "tp"), P(None, "tp")),
        out_specs=(P("dp", "tp", None), P("dp", "tp", None), P("dp", "tp", None)),
        check_vma=False,
    )
```

```python
import functools

import jax
import jax.numpy as jnp
from jax import lax
from jax.experimental import pallas as pl
from jax.experimental.pallas import tpu as pltpu
from jax.sharding import PartitionSpec as P

EPSILON = 1e-6
MESH = pl.DeviceIdType.MESH
LANES = 128
K_PIECE, V_PIECE, FIRST_HEAD = 0, 1, 2


def qkv_kernel(
    x_hbm, gain_hbm, wq_hbm, wk_hbm, wv_hbm,
    q_out, k_out, v_out,
    rows_buf, gain_buf, wq_buf, wkv_buf, q_stage, kv_stage,
    x_sem, gain_sem, load_sem,
    part_send, part_recv, link_send, link_recv, core_send, core_recv, side_send, side_recv, last_send, last_recv,
    middle_send, middle_recv, ready_sem, pair_sem,
    near_send, near_recv, far_send, far_recv, cross_send, cross_recv, pass_send, pass_recv,
    *, norm_tile, dot_tile, shift,
):
    n_rows, depth = rows_buf.shape
    heads = wq_hbm.shape[0]
    share = wk_hbm.shape[0]
    half = depth // 2
    pieces = FIRST_HEAD + heads

    group, member = lax.axis_index("dp"), lax.axis_index("tp")
    chip, core = member // 2, member % 2
    partner = (group, chip * 2 + (1 - core))
    across = (group, (1 - chip) * 2 + core)
    across_other = (group, (1 - chip) * 2 + (1 - core))
    beside = (1 - group, member)

    barrier = pltpu.get_barrier_semaphore()
    for other in (across, partner):
        pl.semaphore_signal(barrier, inc=1, device_id=other, device_id_type=MESH)

    @pl.when(group == 0)
    def _():
        pl.semaphore_signal(barrier, inc=1, device_id=beside, device_id_type=MESH)

    sources = [wk_hbm, wv_hbm] + [wq_hbm.at[h] for h in range(heads)]

    last_head = pieces - 1
    middle = pl.ds(half - shift, 2 * shift)

    def piece_at(j, slot, depth_half=None):
        if j < FIRST_HEAD:
            rows = pl.ds(pl.multiple_of(j * 2 * share + core * share, share), share)
            if depth_half is None:
                return wkv_buf.at[slot // 2, rows]
            return wkv_buf.at[slot // 2, rows, pl.ds(pl.multiple_of(depth_half * half, half), half)]
        if depth_half is None:
            return wq_buf.at[slot, j - FIRST_HEAD]
        if j == last_head:
            start = pl.multiple_of(depth_half * (half + shift), shift)
            return wq_buf.at[slot, j - FIRST_HEAD, pl.ds(start, half - shift)]
        return wq_buf.at[slot, j - FIRST_HEAD, pl.ds(pl.multiple_of(depth_half * half, half), half)]

    loads = [pltpu.make_async_copy(sources[j], piece_at(j, 0), load_sem.at[j]) for j in range(pieces)]
    for load in loads[:FIRST_HEAD]:
        load.start()
    gain_load = pltpu.make_async_copy(gain_hbm, gain_buf, gain_sem)
    n_tiles = n_rows // norm_tile
    x_loads = [
        pltpu.make_async_copy(x_hbm.at[pl.ds(i * norm_tile, norm_tile)], rows_buf.at[pl.ds(i * norm_tile, norm_tile)], x_sem.at[i])
        for i in range(n_tiles)
    ]
    pl.semaphore_wait(barrier, 2 + group)

    def remote(src, dst, send, recv, device):
        return pltpu.make_async_remote_copy(src_ref=src, dst_ref=dst, send_sem=send, recv_sem=recv, device_id=device, device_id_type=MESH)

    part, link, hand, side, last = [], [], [], [], []
    for j in range(pieces):
        part.append(remote(piece_at(j, 0), piece_at(j, 0 if j < FIRST_HEAD else 1), part_send.at[j], part_recv.at[j], partner))
        link.append(remote(piece_at(j, 0, group), piece_at(j, 2, group), link_send.at[j], link_recv.at[j], across))
        arrived, other_half = piece_at(j, 2, group), piece_at(j, 2, 1 - group)
        hand.append(remote(arrived, piece_at(j, 2 if j < FIRST_HEAD else 3, group), core_send.at[j], core_recv.at[j], partner))
        side.append(remote(arrived, arrived, side_send.at[j], side_recv.at[j], beside))
        last.append(remote(other_half, piece_at(j, 2 if j < FIRST_HEAD else 3, 1 - group), last_send.at[j], last_recv.at[j], partner))

    def middle_at(slot):
        return wq_buf.at[slot, heads - 1, middle]

    middle_link = remote(middle_at(0), middle_at(2), middle_send.at[0], middle_recv.at[0], across)
    middle_side = remote(middle_at(2), middle_at(2), middle_send.at[1], middle_recv.at[1], beside)
    middle_hand = remote(middle_at(2), middle_at(3), middle_send.at[2], middle_recv.at[2], partner)

    my_rows = pl.ds(pl.multiple_of(member * n_rows, n_rows), n_rows)
    across_rows = pl.ds(pl.multiple_of(((1 - chip) * 2 + core) * n_rows, n_rows), n_rows)
    near = [remote(k_out.at[0, my_rows], k_out.at[0, my_rows], near_send.at[0], near_recv.at[0], partner),
            remote(v_out.at[0, my_rows], v_out.at[0, my_rows], near_send.at[1], near_recv.at[1], partner)]
    far = [remote(kv_stage.at[0], k_out.at[0, my_rows], far_send.at[0], far_recv.at[0], across),
           remote(kv_stage.at[1], v_out.at[0, my_rows], far_send.at[1], far_recv.at[1], across)]
    passed = [remote(k_out.at[0, across_rows], k_out.at[0, across_rows], pass_send.at[0], pass_recv.at[0], partner),
              remote(v_out.at[0, across_rows], v_out.at[0, across_rows], pass_send.at[1], pass_recv.at[1], partner)]
    cross = []
    for h in range(heads):
        near.append(remote(q_stage.at[0, h], q_out.at[h, my_rows], near_send.at[2 + h], near_recv.at[2 + h], partner))
        far.append(remote(q_stage.at[1, h], q_out.at[h, my_rows], far_send.at[2 + h], far_recv.at[2 + h], across))
        cross.append(remote(q_stage.at[2, h], q_out.at[h, my_rows], cross_send.at[h], cross_recv.at[h], across_other))

    loads[0].wait()
    link[0].start()
    for load in loads[FIRST_HEAD:]:
        load.start()
    gain_load.start()
    for load in x_loads:
        load.start()
    for j in range(1, pieces):
        loads[j].wait()
        link[j].start()
    pl.semaphore_signal(pair_sem, inc=1, device_id=across, device_id_type=MESH)

    @pl.when(group == 1)
    def _():
        middle_link.start()
        pl.semaphore_signal(ready_sem, inc=1, device_id=beside, device_id_type=MESH)

    for copy in part:
        copy.start()

    gain_load.wait()
    chunks = depth // LANES
    sub = 64

    for i in range(n_tiles):
        x_loads[i].wait()

    def norm_step(s, carry):
        here = pl.ds(pl.multiple_of(s * sub, sub), sub)
        total = jnp.zeros((sub, LANES), jnp.float32)
        for c in range(chunks):
            wide = rows_buf[here, c * LANES:(c + 1) * LANES].astype(jnp.float32)
            total = total + wide * wide
        scale = lax.rsqrt(jnp.sum(total, axis=-1, keepdims=True) / depth + EPSILON)
        for c in range(chunks):
            cols = slice(c * LANES, (c + 1) * LANES)
            wide = rows_buf[here, cols].astype(jnp.float32)
            rows_buf[here, cols] = (wide * scale * gain_buf[cols][None, :]).astype(jnp.bfloat16)
        return carry

    lax.fori_loop(0, n_rows // sub, norm_step, 0)

    def over_tiles(step):
        lax.fori_loop(0, n_rows // dot_tile, lambda i, carry: (step(i * dot_tile), carry)[1], 0)

    def q_block(slot, h, store):
        def step(start):
            tile = rows_buf[pl.ds(pl.multiple_of(start, dot_tile), dot_tile), :]
            store(start, jnp.dot(tile, wq_buf[slot, h], preferred_element_type=jnp.float32).astype(jnp.bfloat16))
        over_tiles(step)

    def kv_block(which, store):
        def step(start):
            tile = rows_buf[pl.ds(pl.multiple_of(start, dot_tile), dot_tile), :]
            both = lax.dot_general(tile, wkv_buf[which], (((1,), (1,)), ((), ())), preferred_element_type=jnp.float32)
            store(start, both.astype(jnp.bfloat16))
        over_tiles(step)

    def rows_at(start):
        return pl.ds(pl.multiple_of(start, dot_tile), dot_tile)

    def own_rows_at(start):
        return pl.ds(pl.multiple_of(member * n_rows + start, dot_tile), dot_tile)

    def own_q(h):
        def store(start, value):
            q_out[h, own_rows_at(start), :] = value
        q_block(0, h, store)

    def staged_q(stage, slot, h):
        def store(start, value):
            q_stage[stage, h, rows_at(start), :] = value
        q_block(slot, h, store)

    def own_kv():
        def store(start, value):
            k_out[0, own_rows_at(start), :] = value[:, :LANES]
            v_out[0, own_rows_at(start), :] = value[:, LANES:]
        kv_block(0, store)

    def far_kv():
        def store(start, value):
            kv_stage[0, rows_at(start), :] = value[:, :LANES]
            kv_stage[1, rows_at(start), :] = value[:, LANES:]
        kv_block(1, store)

    def from_link(j):
        link[j].wait_recv()
        side[j].start()
        hand[j].start()

    def from_side(j):
        side[j].wait_recv()
        last[j].start()

    def from_middle():
        @pl.when(group == 1)
        def _():
            middle_link.wait_recv()
            middle_side.start()

        @pl.when(group == 0)
        def _():
            middle_side.wait_recv()

        middle_hand.start()

    def complete(j):
        hand[j].wait_recv()
        last[j].wait_recv()

    pl.semaphore_wait(pair_sem, 1)

    @pl.when(group == 0)
    def _():
        pl.semaphore_wait(ready_sem, 1)

    from_link(K_PIECE)
    from_link(V_PIECE)
    part[K_PIECE].wait_recv()
    part[V_PIECE].wait_recv()
    own_kv()
    from_side(K_PIECE)
    near[0].start()
    near[1].start()
    from_link(2)
    from_side(V_PIECE)
    own_q(0)
    complete(K_PIECE)
    complete(V_PIECE)
    far_kv()
    own_q(1)
    far[0].start()
    far[1].start()
    from_link(3)
    own_q(2)
    from_side(2)
    staged_q(1, 2, 0)
    from_link(4)
    complete(2)
    staged_q(2, 3, 0)
    far[2].start()
    from_side(3)
    staged_q(1, 2, 1)
    cross[0].start()
    complete(3)
    staged_q(2, 3, 1)
    far[3].start()
    from_side(4)
    from_middle()
    staged_q(1, 2, 2)
    cross[1].start()
    complete(4)
    middle_hand.wait_recv()
    staged_q(2, 3, 2)
    far[4].start()
    for h in range(heads):
        part[FIRST_HEAD + h].wait_recv()
        staged_q(0, 1, h)
        if h == 0:
            cross[2].start()
        else:
            near[2 + h - 1].start()
    far[0].wait_recv()
    passed[0].start()
    far[1].wait_recv()
    passed[1].start()
    near[2 + heads - 1].start()

    for copy in part + link + hand + side + last + [middle_hand]:
        copy.wait_send()

    @pl.when(group == 1)
    def _():
        middle_link.wait_send()
        middle_side.wait_send()

    for copy in near:
        copy.wait()
    for copy in passed:
        copy.wait()
    for j, copy in enumerate(far):
        copy.wait_send()
        if j >= FIRST_HEAD:
            copy.wait_recv()
    for copy in cross:
        copy.wait()


def finish_kernel(q_ref, k_ref, v_ref, q_out, k_out, v_out, sems, *, cuts):
    copies = []
    for ref, out in ((q_ref, q_out), (k_ref, k_out), (v_ref, v_out)):
        rows = ref.shape[1] // cuts
        for h in range(ref.shape[0]):
            for cut in range(cuts):
                where = pl.ds(cut * rows, rows)
                copies.append(pltpu.make_async_copy(ref.at[h, where], out.at[h, where], sems.at[len(copies)]))
    for copy in copies:
        copy.start()
    for copy in copies:
        copy.wait()


def solution(mesh):
    def local_step(x_rows, norm_gain, w_q, w_k, w_v):
        n_rows, depth = x_rows.shape
        heads, width = w_q.shape[1:]
        share = w_k.shape[1]
        members = mesh.shape["tp"]
        pieces = FIRST_HEAD + heads
        all_rows = members * n_rows
        dma = pltpu.SemaphoreType.DMA
        norm_tile = n_rows // 4
        out_spec = pl.BlockSpec(memory_space=pltpu.VMEM)
        hbm = pl.BlockSpec(memory_space=pltpu.HBM)
        q, k, v = pl.pallas_call(
            functools.partial(qkv_kernel, norm_tile=norm_tile, dot_tile=256, shift=LANES),
            out_shape=(
                jax.ShapeDtypeStruct((heads, all_rows, width), jnp.bfloat16),
                jax.ShapeDtypeStruct((1, all_rows, width), jnp.bfloat16),
                jax.ShapeDtypeStruct((1, all_rows, width), jnp.bfloat16),
            ),
            in_specs=[hbm] * 5,
            out_specs=(out_spec,) * 3,
            scratch_shapes=[
                pltpu.VMEM((n_rows, depth), jnp.bfloat16),
                pltpu.VMEM((depth,), jnp.float32),
                pltpu.VMEM((4, heads, depth, width), jnp.bfloat16),
                pltpu.VMEM((2, 4 * share, depth), jnp.bfloat16),
                pltpu.VMEM((3, heads, n_rows, width), jnp.bfloat16),
                pltpu.VMEM((2, n_rows, width), jnp.bfloat16),
                dma((4,)), dma(()), dma((pieces,)),
                *[dma((pieces,)) for _ in range(10)],
                dma((3,)), dma((3,)), pltpu.SemaphoreType.REGULAR, pltpu.SemaphoreType.REGULAR,
                dma((pieces,)), dma((pieces,)), dma((pieces,)), dma((pieces,)),
                dma((heads,)), dma((heads,)), dma((2,)), dma((2,)),
            ],
            compiler_params=pltpu.CompilerParams(collective_id=0, has_side_effects=True, vmem_limit_bytes=36 * 1024 * 1024),
            cost_estimate=pl.CostEstimate(flops=2 * n_rows * depth * 2048, bytes_accessed=16 * 1024 * 1024, transcendentals=0),
            name="qkv",
        )(*[pltpu.with_memory_space_constraint(a, pltpu.HBM) for a in (x_rows, norm_gain, w_q.transpose(1, 0, 2), w_k.T, w_v.T)])
        cuts = 2
        vmem = pl.BlockSpec(memory_space=pltpu.VMEM)
        q, k, v = pl.pallas_call(
            functools.partial(finish_kernel, cuts=cuts),
            out_shape=tuple(jax.ShapeDtypeStruct(a.shape, a.dtype) for a in (q, k, v)),
            in_specs=[vmem] * 3,
            out_specs=(hbm,) * 3,
            scratch_shapes=[dma((cuts * (heads + 2),))],
            compiler_params=pltpu.CompilerParams(vmem_limit_bytes=16 * 1024 * 1024),
            name="finish",
        )(q, k, v)
        return q.transpose(1, 0, 2), k.transpose(1, 0, 2), v.transpose(1, 0, 2)

    return jax.shard_map(
        local_step, mesh=mesh,
        in_specs=(P(("dp", "tp"), None), P(None), P(None, "tp", None), P(None, "tp"), P(None, "tp")),
        out_specs=(P("dp", "tp", None), P("dp", "tp", None), P("dp", "tp", None)),
        check_vma=False,
    )
```

```python
import functools

import jax
import jax.numpy as jnp
from jax import lax
from jax.experimental import pallas as pl
from jax.experimental.pallas import tpu as pltpu
from jax.sharding import PartitionSpec as P

EPSILON = 1e-6
MESH = pl.DeviceIdType.MESH
LANES = 128
GATE = 1


def qkv_kernel(
    x_hbm, gain_hbm, wq_hbm, wk_hbm, wv_hbm,
    q_out, k_out, v_out,
    rows_buf, gain_buf, wq_buf, wkv_buf, stage, near_stage,
    x_sem, gain_sem, load_sem,
    part_send, part_recv, link_send, link_recv, side_send, side_recv, hand_send, hand_recv, last_send, last_recv,
    out_send, q_recv, kv_recv, relay_send, relay_recv, near_send, near_recv, pass_send, pass_recv,
    ready_sem, pair_sem,
    *, norm_tile, dot_tile, shift,
):
    n_rows, depth = rows_buf.shape
    heads = wq_hbm.shape[0]
    share = wk_hbm.shape[0]
    half = depth // 2
    pieces = 1 + heads

    group, member = lax.axis_index("dp"), lax.axis_index("tp")
    chip, core = member // 2, member % 2
    is_gate = core == GATE
    partner = (group, chip * 2 + (1 - core))
    across = (group, (1 - chip) * 2 + core)
    beside = (1 - group, member)

    def when(condition, act):
        pl.when(condition)(act)

    def signal(sem, device):
        pl.semaphore_signal(sem, inc=1, device_id=device, device_id_type=MESH)

    barrier = pltpu.get_barrier_semaphore()

    @pl.when(is_gate)
    def _():
        signal(barrier, across)
        when(group == 0, lambda: signal(barrier, beside))

    signal(barrier, partner)

    def kv_rows(owner):
        return pl.ds(pl.multiple_of(owner * 2 * share, 2 * share), 2 * share)

    k_load = pltpu.make_async_copy(wk_hbm, wkv_buf.at[0, pl.ds(pl.multiple_of(core * 2 * share, share), share)], load_sem.at[0])
    v_load = pltpu.make_async_copy(wv_hbm, wkv_buf.at[0, pl.ds(pl.multiple_of(core * 2 * share + share, share), share)], load_sem.at[1])
    q_loads = [pltpu.make_async_copy(wq_hbm.at[h], wq_buf.at[core, h], load_sem.at[2 + h]) for h in range(heads)]
    gain_load = pltpu.make_async_copy(gain_hbm, gain_buf, gain_sem)
    tiles = [pl.ds(i * norm_tile, norm_tile) for i in range(n_rows // norm_tile)]
    x_loads = [pltpu.make_async_copy(x_hbm.at[t], rows_buf.at[t], x_sem.at[i]) for i, t in enumerate(tiles)]
    k_load.start()
    v_load.start()
    for load in q_loads:
        load.start()

    pl.semaphore_wait(barrier, jnp.where(is_gate, 2 + group, 1))

    def remote(src, dst, send, recv, device):
        return pltpu.make_async_remote_copy(src_ref=src, dst_ref=dst, send_sem=send, recv_sem=recv, device_id=device, device_id_type=MESH)

    def piece(j, which, owner, depth_half=None):
        if depth_half is not None:
            extra = shift if (owner, j) == (0, heads) else 0
            cut = pl.ds(pl.multiple_of(depth_half * (half + extra), LANES), half - extra)
        if j == 0:
            return wkv_buf.at[which, kv_rows(owner)] if depth_half is None else wkv_buf.at[which, kv_rows(owner), cut]
        slot = wq_buf.at[which * 2 + owner, j - 1]
        return slot if depth_half is None else wq_buf.at[which * 2 + owner, j - 1, cut]

    part = [remote(piece(j, 0, core), piece(j, 0, core), part_send.at[j], part_recv.at[j], partner) for j in range(pieces)]
    link, side, hand, last = {}, {}, {}, {}
    for owner in range(2):
        for j in range(pieces):
            i = owner * pieces + j
            mine, theirs = piece(j, 1, owner, group), piece(j, 1, owner, 1 - group)
            link[owner, j] = remote(piece(j, 0, owner, group), mine, link_send.at[i], link_recv.at[i], across)
            side[owner, j] = remote(mine, mine, side_send.at[i], side_recv.at[i], beside)
            hand[owner, j] = remote(mine, mine, hand_send.at[i], hand_recv.at[i], partner)
            last[owner, j] = remote(theirs, theirs, last_send.at[i], last_recv.at[i], partner)
    extra = 2 * pieces
    middle = pl.ds(half - shift, 2 * shift)
    here, there = wq_buf.at[0, heads - 1, middle], wq_buf.at[2, heads - 1, middle]
    middle_link = remote(here, there, link_send.at[extra], link_recv.at[extra], across)
    middle_side = remote(there, there, side_send.at[extra], side_recv.at[extra], beside)
    middle_hand = remote(there, there, hand_send.at[extra], hand_recv.at[extra], partner)

    def block_of(owner, h):
        return 2 + owner * heads + h

    def rows_of(owner_chip, owner_core):
        return pl.ds(pl.multiple_of((owner_chip * 2 + owner_core) * n_rows, n_rows), n_rows)

    blocks = 2 + 2 * heads
    out = {}
    for r in range(2):
        rows = rows_of(chip, r)
        for i, ref in enumerate((k_out, v_out)):
            out[r, i] = remote(stage.at[r, i], ref.at[0, rows], out_send.at[r * blocks + i], kv_recv.at[r * 2 + i], across)
        for owner in range(2):
            for h in range(heads):
                b = block_of(owner, h)
                out[r, b] = remote(stage.at[r, b], q_out.at[h, rows], out_send.at[r * blocks + b], q_recv.at[r * heads + h],
                                   (group, (1 - chip) * 2 + owner))
    relay = [remote(stage.at[0, b], stage.at[0, b], relay_send.at[b], relay_recv.at[b], partner) for b in range(blocks)]
    passed = {}
    for r in range(2):
        rows = rows_of(1 - chip, r)
        for i, ref in enumerate((k_out, v_out)):
            passed[r, i] = remote(ref.at[0, rows], ref.at[0, rows], pass_send.at[r * 2 + i], pass_recv.at[r * 2 + i], partner)
    my_rows = rows_of(chip, core)
    near = [remote(ref.at[0, my_rows], ref.at[0, my_rows], near_send.at[i], near_recv.at[i], partner) for i, ref in enumerate((k_out, v_out))]
    near += [remote(near_stage.at[h], q_out.at[h, my_rows], near_send.at[2 + h], near_recv.at[2 + h], partner) for h in range(heads)]

    order = [(1, 0), (1, 1), (0, 0), (0, 1)] + [(owner, j) for j in range(2, pieces) for owner in (1, 0)]

    k_load.wait()
    v_load.wait()
    when(is_gate, link[order[0]].start)
    part[0].start()
    q_loads[0].wait()

    @pl.when(is_gate)
    def _():
        link[order[1]].start()
        signal(pair_sem, across)
        when(group == 1, lambda: signal(ready_sem, beside))

    gain_load.start()
    for load in x_loads:
        load.start()
    part[1].start()
    for j in range(2, pieces):
        q_loads[j - 1].wait()
        part[j].start()

    gain_load.wait()
    for load in x_loads:
        load.wait()
    chunks = depth // LANES
    sub = 64

    def norm_step(s, carry):
        here = pl.ds(pl.multiple_of(s * sub, sub), sub)
        total = jnp.zeros((sub, LANES), jnp.float32)
        for c in range(chunks):
            wide = rows_buf[here, c * LANES:(c + 1) * LANES].astype(jnp.float32)
            total = total + wide * wide
        scale = lax.rsqrt(jnp.sum(total, axis=-1, keepdims=True) / depth + EPSILON)
        for c in range(chunks):
            cols = slice(c * LANES, (c + 1) * LANES)
            wide = rows_buf[here, cols].astype(jnp.float32)
            rows_buf[here, cols] = (wide * scale * gain_buf[cols][None, :]).astype(jnp.bfloat16)
        return carry

    lax.fori_loop(0, n_rows // sub, norm_step, 0)

    for copy in part:
        copy.wait_recv()

    @pl.when(is_gate)
    def _():
        for key in order[2:]:
            link[key].start()
        when(group == 1, middle_link.start)
        pl.semaphore_wait(pair_sem, 1)
        when(group == 0, lambda: pl.semaphore_wait(ready_sem, 1))

    def over_tiles(step):
        lax.fori_loop(0, n_rows // dot_tile, lambda i, carry: (step(i * dot_tile), carry)[1], 0)

    def rows_at(start, base=0):
        return pl.ds(pl.multiple_of(base + start, dot_tile), dot_tile)

    def q_block(slot, h, store):
        def step(start):
            store(start, jnp.dot(rows_buf[rows_at(start), :], wq_buf[slot, h], preferred_element_type=jnp.float32).astype(jnp.bfloat16))
        over_tiles(step)

    def kv_block(which, store_k, store_v):
        def step(start):
            cut = [wkv_buf[which, i * share:(i + 1) * share, :] for i in (0, 2, 1, 3)]
            both = lax.dot_general(rows_buf[rows_at(start), :], jnp.concatenate(cut, axis=0), (((1,), (1,)), ((), ())),
                                   preferred_element_type=jnp.float32).astype(jnp.bfloat16)
            store_k(start, both[:, :LANES])
            store_v(start, both[:, LANES:])
        over_tiles(step)

    my_base = member * n_rows

    def own_q(h):
        def store(start, value):
            q_out[h, rows_at(start, my_base), :] = value
        q_block(core, h, store)

    def near_q(h):
        def store(start, value):
            near_stage[h, rows_at(start), :] = value
        q_block(1 - core, h, store)

    def far_q(owner, h):
        def store(start, value):
            stage[core, block_of(owner, h), rows_at(start), :] = value
        q_block(2 + owner, h, store)

    def own_kv():
        def store_k(start, value):
            k_out[0, rows_at(start, my_base), :] = value

        def store_v(start, value):
            v_out[0, rows_at(start, my_base), :] = value
        kv_block(0, store_k, store_v)

    def far_kv():
        def store_k(start, value):
            stage[core, 0, rows_at(start), :] = value

        def store_v(start, value):
            stage[core, 1, rows_at(start), :] = value
        kv_block(1, store_k, store_v)

    def send(b):
        when(is_gate, out[GATE, b].start)
        when(core != GATE, relay[b].start)

    def from_link(owner, j):
        @pl.when(is_gate)
        def _():
            link[owner, j].wait_recv()
            side[owner, j].start()
            hand[owner, j].start()

    def from_side(owner, j):
        @pl.when(is_gate)
        def _():
            side[owner, j].wait_recv()
            last[owner, j].start()

    def complete(owner, j):
        @pl.when(core != GATE)
        def _():
            hand[owner, j].wait_recv()
            last[owner, j].wait_recv()

    def from_middle():
        @pl.when(is_gate)
        def _():
            @pl.when(group == 1)
            def _():
                middle_link.wait_recv()
                middle_side.start()

            when(group == 0, middle_side.wait_recv)
            middle_hand.start()

    from_link(1, 0)
    own_kv()
    from_link(1, 1)
    own_q(0)
    near[0].start()
    near[1].start()
    from_side(1, 0)
    from_link(0, 0)
    own_q(1)
    from_side(1, 1)
    from_link(0, 1)
    complete(1, 1)
    far_q(1, 0)
    from_side(0, 0)
    from_link(1, 2)
    send(block_of(1, 0))
    complete(1, 0)
    complete(0, 0)
    far_kv()
    from_side(0, 1)
    from_link(0, 2)
    complete(0, 1)
    send(0)
    send(1)
    far_q(0, 0)
    from_side(1, 2)
    from_link(1, 3)
    send(block_of(0, 0))
    complete(1, 2)
    far_q(1, 1)
    from_side(0, 2)
    from_link(0, 3)
    send(block_of(1, 1))
    complete(0, 2)
    far_q(0, 1)
    from_side(1, 3)
    send(block_of(0, 1))
    complete(1, 3)
    far_q(1, 2)
    from_side(0, 3)
    from_middle()
    send(block_of(1, 2))
    complete(0, 3)
    when(core != GATE, middle_hand.wait_recv)
    far_q(0, 2)
    own_q(2)
    send(block_of(0, 2))
    for h in range(heads):
        near_q(h)
        if h:
            near[2 + h - 1].start()

    @pl.when(is_gate)
    def _():
        for b in range(blocks):
            relay[b].wait_recv()
            out[1 - GATE, b].start()

    near[2 + heads - 1].start()

    @pl.when(is_gate)
    def _():
        for r in (GATE, 1 - GATE):
            for i in range(2):
                out[r, i].wait_recv()
                passed[r, i].start()

    for copy in near:
        copy.wait()
    for copy in part:
        copy.wait_send()

    @pl.when(is_gate)
    def _():
        for copies in (link, side, hand, last, passed):
            for copy in copies.values():
                copy.wait_send()

        @pl.when(group == 1)
        def _():
            middle_link.wait_send()
            middle_side.wait_send()

        middle_hand.wait_send()

    @pl.when(core != GATE)
    def _():
        for copy in relay:
            copy.wait_send()
        for copy in passed.values():
            copy.wait_recv()

    for r in (GATE, 1 - GATE):
        for h in range(heads):
            out[r, block_of(0, h)].wait_recv()

    @pl.when(is_gate)
    def _():
        for copy in out.values():
            copy.wait_send()


def finish_kernel(q_ref, k_ref, v_ref, q_out, k_out, v_out, sems, *, cuts):
    copies = []
    for ref, out in ((q_ref, q_out), (k_ref, k_out), (v_ref, v_out)):
        rows = ref.shape[1] // cuts
        for h in range(ref.shape[0]):
            for cut in range(cuts):
                where = pl.ds(cut * rows, rows)
                copies.append(pltpu.make_async_copy(ref.at[h, where], out.at[h, where], sems.at[len(copies)]))
    for copy in copies:
        copy.start()
    for copy in copies:
        copy.wait()


def solution(mesh):
    def local_step(x_rows, norm_gain, w_q, w_k, w_v):
        n_rows, depth = x_rows.shape
        heads, width = w_q.shape[1:]
        share = w_k.shape[1]
        pieces = 1 + heads
        blocks = 2 + 2 * heads
        all_rows = mesh.shape["tp"] * n_rows
        dma = pltpu.SemaphoreType.DMA
        hbm = pl.BlockSpec(memory_space=pltpu.HBM)
        vmem = pl.BlockSpec(memory_space=pltpu.VMEM)
        inputs = (x_rows, norm_gain, w_q.transpose(1, 0, 2), w_k.T, w_v.T)
        results = tuple(jax.ShapeDtypeStruct((n, all_rows, width), jnp.bfloat16) for n in (heads, 1, 1))
        q, k, v = pl.pallas_call(
            functools.partial(qkv_kernel, norm_tile=n_rows // 4, dot_tile=256, shift=LANES),
            out_shape=results,
            in_specs=[hbm] * 5,
            out_specs=(vmem,) * 3,
            scratch_shapes=[
                pltpu.VMEM((n_rows, depth), jnp.bfloat16),
                pltpu.VMEM((depth,), jnp.float32),
                pltpu.VMEM((4, heads, depth, width), jnp.bfloat16),
                pltpu.VMEM((2, 4 * share, depth), jnp.bfloat16),
                pltpu.VMEM((2, blocks, n_rows, width), jnp.bfloat16),
                pltpu.VMEM((heads, n_rows, width), jnp.bfloat16),
                dma((4,)), dma(()), dma((2 + heads,)),
                dma((pieces,)), dma((pieces,)),
                *[dma((2 * pieces + 1,)) for _ in range(8)],
                dma((2 * blocks,)), dma((2 * heads,)), dma((4,)),
                dma((blocks,)), dma((blocks,)),
                dma((2 + heads,)), dma((2 + heads,)), dma((4,)), dma((4,)),
                pltpu.SemaphoreType.REGULAR, pltpu.SemaphoreType.REGULAR,
            ],
            compiler_params=pltpu.CompilerParams(collective_id=0, has_side_effects=True, vmem_limit_bytes=36 * 1024 * 1024),
            cost_estimate=pl.CostEstimate(flops=2 * n_rows * depth * 2048, bytes_accessed=16 * 1024 * 1024, transcendentals=0),
            name="qkv",
        )(*[pltpu.with_memory_space_constraint(a, pltpu.HBM) for a in inputs])
        cuts = 2
        q, k, v = pl.pallas_call(
            functools.partial(finish_kernel, cuts=cuts),
            out_shape=results,
            in_specs=[vmem] * 3,
            out_specs=(hbm,) * 3,
            scratch_shapes=[dma((cuts * (heads + 2),))],
            compiler_params=pltpu.CompilerParams(vmem_limit_bytes=16 * 1024 * 1024),
            name="finish",
        )(q, k, v)
        return q.transpose(1, 0, 2), k.transpose(1, 0, 2), v.transpose(1, 0, 2)

    return jax.shard_map(
        local_step, mesh=mesh,
        in_specs=(P(("dp", "tp"), None), P(None), P(None, "tp", None), P(None, "tp"), P(None, "tp")),
        out_specs=(P("dp", "tp", None), P("dp", "tp", None), P("dp", "tp", None)),
        check_vma=False,
    )
```

```python
import functools

import jax
import jax.numpy as jnp
from jax import lax
from jax.experimental import pallas as pl
from jax.experimental.pallas import tpu as pltpu
from jax.sharding import PartitionSpec as P

EPSILON = 1e-6
MESH = pl.DeviceIdType.MESH
LANES = 128
K_PIECE, V_PIECE, FIRST_HEAD = 0, 1, 2


def qkv_kernel(
    x_hbm, gain_hbm, wq_hbm, wk_hbm, wv_hbm,
    q_out, k_out, v_out,
    rows_buf, gain_buf, wq_buf, wkv_buf, q_stage, kv_stage,
    x_sem, gain_sem, load_sem,
    part_send, part_recv, link_send, link_recv, core_send, core_recv, side_send, side_recv, last_send, last_recv,
    middle_send, middle_recv, ready_sem, pair_sem, lent_buf, lent_sem,
    near_send, near_recv, far_send, far_recv, cross_send, cross_recv, pass_send, pass_recv,
    *, norm_tile, dot_tile, shift, lent,
):
    n_rows, depth = rows_buf.shape
    heads = wq_hbm.shape[0]
    share = wk_hbm.shape[0]
    half = depth // 2
    pieces = FIRST_HEAD + heads

    group, member = lax.axis_index("dp"), lax.axis_index("tp")
    chip, core = member // 2, member % 2
    partner = (group, chip * 2 + (1 - core))
    across = (group, (1 - chip) * 2 + core)
    across_other = (group, (1 - chip) * 2 + (1 - core))
    beside = (1 - group, member)

    barrier = pltpu.get_barrier_semaphore()
    for other in (across, partner):
        pl.semaphore_signal(barrier, inc=1, device_id=other, device_id_type=MESH)

    @pl.when(group == 0)
    def _():
        pl.semaphore_signal(barrier, inc=1, device_id=beside, device_id_type=MESH)

    sources = [wk_hbm, wv_hbm] + [wq_hbm.at[h] for h in range(heads)]

    last_head = pieces - 1
    middle = pl.ds(half - shift, 2 * shift)

    def piece_at(j, slot, depth_half=None):
        if j < FIRST_HEAD:
            rows = pl.ds(pl.multiple_of(j * 2 * share + core * share, share), share)
            if depth_half is None:
                return wkv_buf.at[slot // 2, rows]
            return wkv_buf.at[slot // 2, rows, pl.ds(pl.multiple_of(depth_half * half, half), half)]
        if depth_half is None:
            return wq_buf.at[slot, j - FIRST_HEAD]
        if j == last_head:
            start = pl.multiple_of(depth_half * (half + shift), 32)
            return wq_buf.at[slot, j - FIRST_HEAD, pl.ds(start, half - shift)]
        return wq_buf.at[slot, j - FIRST_HEAD, pl.ds(pl.multiple_of(depth_half * half, half), half)]

    loads = [pltpu.make_async_copy(sources[j], piece_at(j, 0), load_sem.at[j]) for j in range(pieces)]
    for load in loads[:FIRST_HEAD]:
        load.start()
    gain_load = pltpu.make_async_copy(gain_hbm, gain_buf, gain_sem)
    n_tiles = n_rows // norm_tile
    x_loads = [
        pltpu.make_async_copy(x_hbm.at[pl.ds(i * norm_tile, norm_tile)], rows_buf.at[pl.ds(i * norm_tile, norm_tile)], x_sem.at[i])
        for i in range(n_tiles)
    ]
    pl.semaphore_wait(barrier, 2 + group)

    def remote(src, dst, send, recv, device):
        return pltpu.make_async_remote_copy(src_ref=src, dst_ref=dst, send_sem=send, recv_sem=recv, device_id=device, device_id_type=MESH)

    part, link, hand, side, last = [], [], [], [], []
    for j in range(pieces):
        part.append(remote(piece_at(j, 0), piece_at(j, 0 if j < FIRST_HEAD else 1), part_send.at[j], part_recv.at[j], partner))
        link.append(remote(piece_at(j, 0, group), piece_at(j, 2, group), link_send.at[j], link_recv.at[j], across))
        arrived, other_half = piece_at(j, 2, group), piece_at(j, 2, 1 - group)
        hand.append(remote(arrived, piece_at(j, 2 if j < FIRST_HEAD else 3, group), core_send.at[j], core_recv.at[j], partner))
        side.append(remote(arrived, arrived, side_send.at[j], side_recv.at[j], beside))
        last.append(remote(other_half, piece_at(j, 2 if j < FIRST_HEAD else 3, 1 - group), last_send.at[j], last_recv.at[j], partner))

    def middle_at(slot):
        return wq_buf.at[slot, heads - 1, middle]

    middle_link = remote(middle_at(0), middle_at(2), middle_send.at[0], middle_recv.at[0], across)
    middle_side = remote(middle_at(2), middle_at(2), middle_send.at[1], middle_recv.at[1], beside)
    middle_hand = remote(middle_at(2), middle_at(3), middle_send.at[2], middle_recv.at[2], partner)

    my_rows = pl.ds(pl.multiple_of(member * n_rows, n_rows), n_rows)
    across_rows = pl.ds(pl.multiple_of(((1 - chip) * 2 + core) * n_rows, n_rows), n_rows)
    near = [remote(k_out.at[0, my_rows], k_out.at[0, my_rows], near_send.at[0], near_recv.at[0], partner),
            remote(v_out.at[0, my_rows], v_out.at[0, my_rows], near_send.at[1], near_recv.at[1], partner)]
    far = [remote(kv_stage.at[0], k_out.at[0, my_rows], far_send.at[0], far_recv.at[0], across),
           remote(kv_stage.at[1], v_out.at[0, my_rows], far_send.at[1], far_recv.at[1], across)]
    passed = [remote(k_out.at[0, across_rows], k_out.at[0, across_rows], pass_send.at[0], pass_recv.at[0], partner),
              remote(v_out.at[0, across_rows], v_out.at[0, across_rows], pass_send.at[1], pass_recv.at[1], partner)]
    cross = []
    for h in range(heads):
        near.append(remote(q_stage.at[0, h], q_out.at[h, my_rows], near_send.at[2 + h], near_recv.at[2 + h], partner))
        far.append(remote(q_stage.at[1, h], q_out.at[h, my_rows], far_send.at[2 + h], far_recv.at[2 + h], across))
        cross.append(remote(q_stage.at[2, h], q_out.at[h, my_rows], cross_send.at[h], cross_recv.at[h], across_other))

    last_h = heads - 1
    lent_rows, kept_rows = pl.ds(0, lent), pl.ds(lent, n_rows - lent)
    my_kept = pl.ds(pl.multiple_of(member * n_rows + lent, lent), n_rows - lent)
    partner_lent = pl.ds(pl.multiple_of((chip * 2 + 1 - core) * n_rows, n_rows), lent)
    lend = remote(q_stage.at[2, last_h, lent_rows], lent_buf, lent_sem.at[0], lent_sem.at[1], partner)
    cross_kept = remote(q_stage.at[2, last_h, kept_rows], q_out.at[last_h, my_kept], cross_send.at[last_h], cross_recv.at[last_h], across_other)
    cross_lent = remote(lent_buf, q_out.at[last_h, partner_lent], lent_sem.at[2], lent_sem.at[3], across)

    loads[0].wait()
    link[0].start()
    for load in loads[FIRST_HEAD:]:
        load.start()
    gain_load.start()
    for load in x_loads:
        load.start()
    for j in range(1, pieces):
        loads[j].wait()
        link[j].start()
    pl.semaphore_signal(pair_sem, inc=1, device_id=across, device_id_type=MESH)

    @pl.when(group == 1)
    def _():
        middle_link.start()
        pl.semaphore_signal(ready_sem, inc=1, device_id=beside, device_id_type=MESH)

    for copy in part:
        copy.start()

    gain_load.wait()
    chunks = depth // LANES
    sub = 64

    for i in range(n_tiles):
        x_loads[i].wait()

    def norm_step(s, carry):
        here = pl.ds(pl.multiple_of(s * sub, sub), sub)
        total = jnp.zeros((sub, LANES), jnp.float32)
        for c in range(chunks):
            wide = rows_buf[here, c * LANES:(c + 1) * LANES].astype(jnp.float32)
            total = total + wide * wide
        scale = lax.rsqrt(jnp.sum(total, axis=-1, keepdims=True) / depth + EPSILON)
        for c in range(chunks):
            cols = slice(c * LANES, (c + 1) * LANES)
            wide = rows_buf[here, cols].astype(jnp.float32)
            rows_buf[here, cols] = (wide * scale * gain_buf[cols][None, :]).astype(jnp.bfloat16)
        return carry

    lax.fori_loop(0, n_rows // sub, norm_step, 0)

    def over_tiles(step):
        lax.fori_loop(0, n_rows // dot_tile, lambda i, carry: (step(i * dot_tile), carry)[1], 0)

    def q_block(slot, h, store):
        def step(start):
            tile = rows_buf[pl.ds(pl.multiple_of(start, dot_tile), dot_tile), :]
            store(start, jnp.dot(tile, wq_buf[slot, h], preferred_element_type=jnp.float32).astype(jnp.bfloat16))
        over_tiles(step)

    def kv_block(which, store):
        def step(start):
            tile = rows_buf[pl.ds(pl.multiple_of(start, dot_tile), dot_tile), :]
            both = lax.dot_general(tile, wkv_buf[which], (((1,), (1,)), ((), ())), preferred_element_type=jnp.float32)
            store(start, both.astype(jnp.bfloat16))
        over_tiles(step)

    def rows_at(start):
        return pl.ds(pl.multiple_of(start, dot_tile), dot_tile)

    def own_rows_at(start):
        return pl.ds(pl.multiple_of(member * n_rows + start, dot_tile), dot_tile)

    def own_q(h):
        def store(start, value):
            q_out[h, own_rows_at(start), :] = value
        q_block(0, h, store)

    def staged_q(stage, slot, h):
        def store(start, value):
            q_stage[stage, h, rows_at(start), :] = value
        q_block(slot, h, store)

    def own_kv():
        def store(start, value):
            k_out[0, own_rows_at(start), :] = value[:, :LANES]
            v_out[0, own_rows_at(start), :] = value[:, LANES:]
        kv_block(0, store)

    def far_kv():
        def store(start, value):
            kv_stage[0, rows_at(start), :] = value[:, :LANES]
            kv_stage[1, rows_at(start), :] = value[:, LANES:]
        kv_block(1, store)

    def from_link(j):
        link[j].wait_recv()
        side[j].start()
        hand[j].start()

    def from_side(j):
        side[j].wait_recv()
        last[j].start()

    def from_middle():
        @pl.when(group == 1)
        def _():
            middle_link.wait_recv()
            middle_side.start()

        @pl.when(group == 0)
        def _():
            middle_side.wait_recv()

        middle_hand.start()

    def complete(j):
        hand[j].wait_recv()
        last[j].wait_recv()

    pl.semaphore_wait(pair_sem, 1)

    @pl.when(group == 0)
    def _():
        pl.semaphore_wait(ready_sem, 1)

    from_link(K_PIECE)
    from_link(V_PIECE)
    part[K_PIECE].wait_recv()
    part[V_PIECE].wait_recv()
    own_kv()
    from_side(K_PIECE)
    near[0].start()
    near[1].start()
    from_link(2)
    from_side(V_PIECE)
    complete(K_PIECE)
    complete(V_PIECE)
    far_kv()
    far[0].start()
    far[1].start()
    own_q(0)
    from_link(3)
    own_q(1)
    from_side(2)
    staged_q(1, 2, 0)
    from_link(4)
    complete(2)
    staged_q(2, 3, 0)
    far[2].start()
    from_side(3)
    staged_q(1, 2, 1)
    cross[0].start()
    complete(3)
    staged_q(2, 3, 1)
    far[3].start()
    from_side(4)
    from_middle()
    staged_q(1, 2, 2)
    cross[1].start()
    complete(4)
    middle_hand.wait_recv()
    staged_q(2, 3, 2)
    own_q(2)

    @pl.when(core == 0)
    def _():
        lend.start()
        far[FIRST_HEAD + last_h].start()
        cross_kept.start()

    @pl.when(core == 1)
    def _():
        cross[last_h].start()
        lend.wait_recv()
        cross_lent.start()
        far[FIRST_HEAD + last_h].start()

    for h in range(heads):
        part[FIRST_HEAD + h].wait_recv()
        staged_q(0, 1, h)
        if h:
            near[2 + h - 1].start()
    far[0].wait_recv()
    passed[0].start()
    far[1].wait_recv()
    passed[1].start()
    near[2 + heads - 1].start()

    for copy in part + link + hand + side + last + [middle_hand]:
        copy.wait_send()

    @pl.when(group == 1)
    def _():
        middle_link.wait_send()
        middle_side.wait_send()

    for copy in near:
        copy.wait()
    for copy in passed:
        copy.wait()
    for j, copy in enumerate(far):
        copy.wait_send()
        if j >= FIRST_HEAD:
            copy.wait_recv()
    for copy in cross[:last_h]:
        copy.wait()

    @pl.when(core == 0)
    def _():
        lend.wait_send()
        cross_kept.wait_send()
        cross[last_h].wait_recv()

    @pl.when(core == 1)
    def _():
        cross[last_h].wait_send()
        cross_lent.wait()
        cross_kept.wait_recv()


def finish_kernel(q_ref, k_ref, v_ref, q_out, k_out, v_out, sems, *, cuts):
    copies = []
    for ref, out in ((q_ref, q_out), (k_ref, k_out), (v_ref, v_out)):
        rows = ref.shape[1] // cuts
        for h in range(ref.shape[0]):
            for cut in range(cuts):
                where = pl.ds(cut * rows, rows)
                copies.append(pltpu.make_async_copy(ref.at[h, where], out.at[h, where], sems.at[len(copies)]))
    for copy in copies:
        copy.start()
    for copy in copies:
        copy.wait()


def solution(mesh):
    def local_step(x_rows, norm_gain, w_q, w_k, w_v):
        n_rows, depth = x_rows.shape
        heads, width = w_q.shape[1:]
        share = w_k.shape[1]
        members = mesh.shape["tp"]
        pieces = FIRST_HEAD + heads
        all_rows = members * n_rows
        dma = pltpu.SemaphoreType.DMA
        norm_tile = n_rows // 4
        lent = 256
        out_spec = pl.BlockSpec(memory_space=pltpu.VMEM)
        hbm = pl.BlockSpec(memory_space=pltpu.HBM)
        q, k, v = pl.pallas_call(
            functools.partial(qkv_kernel, norm_tile=norm_tile, dot_tile=256, shift=96, lent=lent),
            out_shape=(
                jax.ShapeDtypeStruct((heads, all_rows, width), jnp.bfloat16),
                jax.ShapeDtypeStruct((1, all_rows, width), jnp.bfloat16),
                jax.ShapeDtypeStruct((1, all_rows, width), jnp.bfloat16),
            ),
            in_specs=[hbm] * 5,
            out_specs=(out_spec,) * 3,
            scratch_shapes=[
                pltpu.VMEM((n_rows, depth), jnp.bfloat16),
                pltpu.VMEM((depth,), jnp.float32),
                pltpu.VMEM((4, heads, depth, width), jnp.bfloat16),
                pltpu.VMEM((2, 4 * share, depth), jnp.bfloat16),
                pltpu.VMEM((3, heads, n_rows, width), jnp.bfloat16),
                pltpu.VMEM((2, n_rows, width), jnp.bfloat16),
                dma((4,)), dma(()), dma((pieces,)),
                *[dma((pieces,)) for _ in range(10)],
                dma((3,)), dma((3,)), pltpu.SemaphoreType.REGULAR, pltpu.SemaphoreType.REGULAR,
                pltpu.VMEM((lent, width), jnp.bfloat16), dma((4,)),
                dma((pieces,)), dma((pieces,)), dma((pieces,)), dma((pieces,)),
                dma((heads,)), dma((heads,)), dma((2,)), dma((2,)),
            ],
            compiler_params=pltpu.CompilerParams(collective_id=0, has_side_effects=True, vmem_limit_bytes=36 * 1024 * 1024),
            cost_estimate=pl.CostEstimate(flops=2 * n_rows * depth * 2048, bytes_accessed=16 * 1024 * 1024, transcendentals=0),
            name="qkv",
        )(*[pltpu.with_memory_space_constraint(a, pltpu.HBM) for a in (x_rows, norm_gain, w_q.transpose(1, 0, 2), w_k.T, w_v.T)])
        cuts = 2
        vmem = pl.BlockSpec(memory_space=pltpu.VMEM)
        q, k, v = pl.pallas_call(
            functools.partial(finish_kernel, cuts=cuts),
            out_shape=tuple(jax.ShapeDtypeStruct(a.shape, a.dtype) for a in (q, k, v)),
            in_specs=[vmem] * 3,
            out_specs=(hbm,) * 3,
            scratch_shapes=[dma((cuts * (heads + 2),))],
            compiler_params=pltpu.CompilerParams(vmem_limit_bytes=16 * 1024 * 1024),
            name="finish",
        )(q, k, v)
        return q.transpose(1, 0, 2), k.transpose(1, 0, 2), v.transpose(1, 0, 2)

    return jax.shard_map(
        local_step, mesh=mesh,
        in_specs=(P(("dp", "tp"), None), P(None), P(None, "tp", None), P(None, "tp"), P(None, "tp")),
        out_specs=(P("dp", "tp", None), P("dp", "tp", None), P("dp", "tp", None)),
        check_vma=False,
    )
```

```python
import functools

import jax
import jax.numpy as jnp
from jax import lax
from jax.experimental import pallas as pl
from jax.experimental.pallas import tpu as pltpu
from jax.sharding import PartitionSpec as P

EPSILON = 1e-6
MESH = pl.DeviceIdType.MESH
LANES = 128
K_PIECE, V_PIECE, FIRST_HEAD = 0, 1, 2


def qkv_kernel(
    x_hbm, gain_hbm, wq_hbm, wk_hbm, wv_hbm,
    q_out, k_out, v_out, late_out,
    rows_buf, gain_buf, wq_buf, wkv_buf, q_stage, kv_stage,
    x_sem, gain_sem, load_sem,
    part_send, part_recv, link_send, link_recv, core_send, core_recv, side_send, side_recv, last_send, last_recv,
    middle_send, middle_recv, ready_sem, pair_sem,
    near_send, near_recv, far_send, far_recv, cross_send, cross_recv, pass_send, pass_recv,
    *, norm_tile, dot_tile, shift,
):
    n_rows, depth = rows_buf.shape
    heads = wq_hbm.shape[0]
    share = wk_hbm.shape[0]
    half = depth // 2
    pieces = FIRST_HEAD + heads

    group, member = lax.axis_index("dp"), lax.axis_index("tp")
    chip, core = member // 2, member % 2
    partner = (group, chip * 2 + (1 - core))
    across = (group, (1 - chip) * 2 + core)
    across_other = (group, (1 - chip) * 2 + (1 - core))
    beside = (1 - group, member)

    barrier = pltpu.get_barrier_semaphore()
    for other in (across, partner):
        pl.semaphore_signal(barrier, inc=1, device_id=other, device_id_type=MESH)

    @pl.when(group == 0)
    def _():
        pl.semaphore_signal(barrier, inc=1, device_id=beside, device_id_type=MESH)

    sources = [wk_hbm, wv_hbm] + [wq_hbm.at[h] for h in range(heads)]

    last_head = pieces - 1
    middle = pl.ds(half - shift, 2 * shift)

    def piece_at(j, slot, depth_half=None):
        if j < FIRST_HEAD:
            rows = pl.ds(pl.multiple_of(j * 2 * share + core * share, share), share)
            if depth_half is None:
                return wkv_buf.at[slot // 2, rows]
            return wkv_buf.at[slot // 2, rows, pl.ds(pl.multiple_of(depth_half * half, half), half)]
        if depth_half is None:
            return wq_buf.at[slot, j - FIRST_HEAD]
        if j == last_head:
            start = pl.multiple_of(depth_half * (half + shift), 16)
            return wq_buf.at[slot, j - FIRST_HEAD, pl.ds(start, half - shift)]
        return wq_buf.at[slot, j - FIRST_HEAD, pl.ds(pl.multiple_of(depth_half * half, half), half)]

    loads = [pltpu.make_async_copy(sources[j], piece_at(j, 0), load_sem.at[j]) for j in range(pieces)]
    for load in loads[:FIRST_HEAD]:
        load.start()
    gain_load = pltpu.make_async_copy(gain_hbm, gain_buf, gain_sem)
    n_tiles = n_rows // norm_tile
    x_loads = [
        pltpu.make_async_copy(x_hbm.at[pl.ds(i * norm_tile, norm_tile)], rows_buf.at[pl.ds(i * norm_tile, norm_tile)], x_sem.at[i])
        for i in range(n_tiles)
    ]
    pl.semaphore_wait(barrier, 2 + group)

    def remote(src, dst, send, recv, device):
        return pltpu.make_async_remote_copy(src_ref=src, dst_ref=dst, send_sem=send, recv_sem=recv, device_id=device, device_id_type=MESH)

    part, link, hand, side, last = [], [], [], [], []
    for j in range(pieces):
        part.append(remote(piece_at(j, 0), piece_at(j, 0 if j < FIRST_HEAD else 1), part_send.at[j], part_recv.at[j], partner))
        link.append(remote(piece_at(j, 0, group), piece_at(j, 2, group), link_send.at[j], link_recv.at[j], across))
        arrived, other_half = piece_at(j, 2, group), piece_at(j, 2, 1 - group)
        hand.append(remote(arrived, piece_at(j, 2 if j < FIRST_HEAD else 3, group), core_send.at[j], core_recv.at[j], partner))
        side.append(remote(arrived, arrived, side_send.at[j], side_recv.at[j], beside))
        last.append(remote(other_half, piece_at(j, 2 if j < FIRST_HEAD else 3, 1 - group), last_send.at[j], last_recv.at[j], partner))

    def middle_at(slot):
        return wq_buf.at[slot, heads - 1, middle]

    middle_link = remote(middle_at(0), middle_at(2), middle_send.at[0], middle_recv.at[0], across)
    middle_side = remote(middle_at(2), middle_at(2), middle_send.at[1], middle_recv.at[1], beside)
    middle_hand = remote(middle_at(2), middle_at(3), middle_send.at[2], middle_recv.at[2], partner)

    my_rows = pl.ds(pl.multiple_of(member * n_rows, n_rows), n_rows)
    across_rows = pl.ds(pl.multiple_of(((1 - chip) * 2 + core) * n_rows, n_rows), n_rows)
    near = [remote(k_out.at[0, my_rows], k_out.at[0, my_rows], near_send.at[0], near_recv.at[0], partner),
            remote(v_out.at[0, my_rows], v_out.at[0, my_rows], near_send.at[1], near_recv.at[1], partner)]
    far = [remote(kv_stage.at[0], k_out.at[0, my_rows], far_send.at[0], far_recv.at[0], across),
           remote(kv_stage.at[1], v_out.at[0, my_rows], far_send.at[1], far_recv.at[1], across)]
    passed = [remote(k_out.at[0, across_rows], k_out.at[0, across_rows], pass_send.at[0], pass_recv.at[0], partner),
              remote(v_out.at[0, across_rows], v_out.at[0, across_rows], pass_send.at[1], pass_recv.at[1], partner)]
    cross = []
    for h in range(heads):
        near.append(remote(q_stage.at[0, h], q_out.at[h, my_rows], near_send.at[2 + h], near_recv.at[2 + h], partner))
        far.append(remote(q_stage.at[1, 0] if h == 0 else late_out.at[h - 1], q_out.at[h, my_rows], far_send.at[2 + h], far_recv.at[2 + h], across))
        cross.append(remote(q_stage.at[2, h], q_out.at[h, my_rows], cross_send.at[h], cross_recv.at[h], across_other))

    loads[0].wait()
    link[0].start()
    for load in loads[FIRST_HEAD:]:
        load.start()
    gain_load.start()
    for load in x_loads:
        load.start()
    for j in range(1, pieces):
        loads[j].wait()
        link[j].start()
    pl.semaphore_signal(pair_sem, inc=1, device_id=across, device_id_type=MESH)

    @pl.when(group == 1)
    def _():
        middle_link.start()
        pl.semaphore_signal(ready_sem, inc=1, device_id=beside, device_id_type=MESH)

    for copy in part:
        copy.start()

    gain_load.wait()
    chunks = depth // LANES
    sub = 64

    for i in range(n_tiles):
        x_loads[i].wait()

    def norm_step(s, carry):
        here = pl.ds(pl.multiple_of(s * sub, sub), sub)
        total = jnp.zeros((sub, LANES), jnp.float32)
        for c in range(chunks):
            wide = rows_buf[here, c * LANES:(c + 1) * LANES].astype(jnp.float32)
            total = total + wide * wide
        scale = lax.rsqrt(jnp.sum(total, axis=-1, keepdims=True) / depth + EPSILON)
        for c in range(chunks):
            cols = slice(c * LANES, (c + 1) * LANES)
            wide = rows_buf[here, cols].astype(jnp.float32)
            rows_buf[here, cols] = (wide * scale * gain_buf[cols][None, :]).astype(jnp.bfloat16)
        return carry

    lax.fori_loop(0, n_rows // sub, norm_step, 0)

    def over_tiles(step):
        lax.fori_loop(0, n_rows // dot_tile, lambda i, carry: (step(i * dot_tile), carry)[1], 0)

    def q_block(slot, h, store):
        def step(start):
            tile = rows_buf[pl.ds(pl.multiple_of(start, dot_tile), dot_tile), :]
            store(start, jnp.dot(tile, wq_buf[slot, h], preferred_element_type=jnp.float32).astype(jnp.bfloat16))
        over_tiles(step)

    def kv_block(which, store):
        def step(start):
            tile = rows_buf[pl.ds(pl.multiple_of(start, dot_tile), dot_tile), :]
            both = lax.dot_general(tile, wkv_buf[which], (((1,), (1,)), ((), ())), preferred_element_type=jnp.float32)
            store(start, both.astype(jnp.bfloat16))
        over_tiles(step)

    def rows_at(start):
        return pl.ds(pl.multiple_of(start, dot_tile), dot_tile)

    def own_rows_at(start):
        return pl.ds(pl.multiple_of(member * n_rows + start, dot_tile), dot_tile)

    def own_q(h):
        def store(start, value):
            q_out[h, own_rows_at(start), :] = value
        q_block(0, h, store)

    def staged_q(stage, slot, h):
        def store(start, value):
            q_stage[stage, h, rows_at(start), :] = value
        q_block(slot, h, store)

    def late_q(h):
        def store(start, value):
            late_out[h - 1, rows_at(start), :] = value
        q_block(2, h, store)

    def own_kv():
        def store(start, value):
            k_out[0, own_rows_at(start), :] = value[:, :LANES]
            v_out[0, own_rows_at(start), :] = value[:, LANES:]
        kv_block(0, store)

    def far_kv():
        def store(start, value):
            kv_stage[0, rows_at(start), :] = value[:, :LANES]
            kv_stage[1, rows_at(start), :] = value[:, LANES:]
        kv_block(1, store)

    def from_link(j):
        link[j].wait_recv()
        side[j].start()
        hand[j].start()

    def from_side(j):
        side[j].wait_recv()
        last[j].start()

    def from_middle():
        @pl.when(group == 1)
        def _():
            middle_link.wait_recv()
            middle_side.start()

        @pl.when(group == 0)
        def _():
            middle_side.wait_recv()

        middle_hand.start()

    def complete(j):
        hand[j].wait_recv()
        last[j].wait_recv()

    pl.semaphore_wait(pair_sem, 1)

    @pl.when(group == 0)
    def _():
        pl.semaphore_wait(ready_sem, 1)

    from_link(K_PIECE)
    from_link(V_PIECE)
    part[K_PIECE].wait_recv()
    part[V_PIECE].wait_recv()
    own_kv()
    from_side(K_PIECE)
    near[0].start()
    near[1].start()
    from_link(2)
    from_side(V_PIECE)
    complete(K_PIECE)
    complete(V_PIECE)
    far_kv()
    far[0].start()
    far[1].start()
    own_q(0)
    from_link(3)
    own_q(1)
    from_side(2)
    staged_q(1, 2, 0)
    from_link(4)
    complete(2)
    staged_q(2, 3, 0)
    far[2].start()
    from_side(3)
    complete(3)
    staged_q(2, 3, 1)
    cross[0].start()
    late_q(1)
    from_side(4)
    from_middle()
    cross[1].start()
    complete(4)
    middle_hand.wait_recv()
    staged_q(2, 3, 2)
    late_q(2)
    cross[2].start()
    own_q(2)

    @pl.when(core == 0)
    def _():
        for copy in far[FIRST_HEAD + 1:]:
            copy.start()

    for h in range(heads):
        part[FIRST_HEAD + h].wait_recv()
        staged_q(0, 1, h)
        if h:
            near[2 + h - 1].start()
    far[0].wait_recv()
    passed[0].start()
    far[1].wait_recv()
    passed[1].start()
    near[2 + heads - 1].start()

    for copy in part + link + hand + side + last + [middle_hand]:
        copy.wait_send()

    @pl.when(group == 1)
    def _():
        middle_link.wait_send()
        middle_side.wait_send()

    for copy in near + passed + cross:
        copy.wait()
    for copy in far[:FIRST_HEAD]:
        copy.wait_send()
    far[FIRST_HEAD].wait()

    @pl.when(core == 0)
    def _():
        for copy in far[FIRST_HEAD + 1:]:
            copy.wait()


def finish_kernel(q_ref, k_ref, v_ref, q_out, k_out, v_out, sems):
    member = lax.axis_index("tp")
    chip, core = member // 2, member % 2
    n_rows = q_ref.shape[1] // 4
    here, there = [], []
    for ref, out in ((q_ref, q_out), (k_ref, k_out), (v_ref, v_out)):
        for h in range(ref.shape[0]):
            for cut in range(4):
                where = pl.ds(pl.multiple_of(((3 - 2 * chip + cut + 1) % 4) * n_rows, n_rows), n_rows)
                copy = pltpu.make_async_copy(ref.at[h, where], out.at[h, where], sems.at[len(here) + len(there)])
                (there if cut == 3 and ref is q_ref and h else here).append(copy)

    for copy in here:
        copy.start()

    @pl.when(core == 0)
    def _():
        for copy in there:
            copy.start()

    for copy in here:
        copy.wait()

    @pl.when(core == 0)
    def _():
        for copy in there:
            copy.wait()


def late_kernel(after_ref, late_out, late_in, send_sem, recv_sem):
    group, member = lax.axis_index("dp"), lax.axis_index("tp")

    @pl.when(member % 2 == 1)
    def _():
        across = (group, (member + 2) % 4)
        barrier = pltpu.get_barrier_semaphore()
        pl.semaphore_signal(barrier, inc=1, device_id=across, device_id_type=MESH)
        pl.semaphore_wait(barrier, 1)
        copies = [
            pltpu.make_async_remote_copy(src_ref=late_out.at[i], dst_ref=late_in.at[i], send_sem=send_sem.at[i], recv_sem=recv_sem.at[i],
                                         device_id=across, device_id_type=MESH)
            for i in range(late_out.shape[0])
        ]
        for copy in copies:
            copy.start()
        for copy in copies:
            copy.wait()


def patch_kernel(before_ref, late_ref, q_out, sems):
    member = lax.axis_index("tp")
    n_rows = late_ref.shape[1]

    @pl.when(member % 2 == 1)
    def _():
        where = pl.ds(pl.multiple_of(((member + 2) % 4) * n_rows, n_rows), n_rows)
        copies = [pltpu.make_async_copy(late_ref.at[i], q_out.at[1 + i, where], sems.at[i]) for i in range(late_ref.shape[0])]
        for copy in copies:
            copy.start()
        for copy in copies:
            copy.wait()


def solution(mesh):
    def local_step(x_rows, norm_gain, w_q, w_k, w_v):
        n_rows, depth = x_rows.shape
        heads, width = w_q.shape[1:]
        share = w_k.shape[1]
        members = mesh.shape["tp"]
        pieces = FIRST_HEAD + heads
        all_rows = members * n_rows
        dma = pltpu.SemaphoreType.DMA
        norm_tile = n_rows // 4
        vmem = pl.BlockSpec(memory_space=pltpu.VMEM)
        results = tuple(jax.ShapeDtypeStruct((n, all_rows, width), jnp.bfloat16) for n in (heads, 1, 1))
        hbm = pl.BlockSpec(memory_space=pltpu.HBM)
        late_shape = jax.ShapeDtypeStruct((heads - 1, n_rows, width), jnp.bfloat16)
        q, k, v, late = pl.pallas_call(
            functools.partial(qkv_kernel, norm_tile=norm_tile, dot_tile=256, shift=80),
            out_shape=results + (late_shape,),
            in_specs=[hbm] * 5,
            out_specs=(vmem,) * 4,
            scratch_shapes=[
                pltpu.VMEM((n_rows, depth), jnp.bfloat16),
                pltpu.VMEM((depth,), jnp.float32),
                pltpu.VMEM((4, heads, depth, width), jnp.bfloat16),
                pltpu.VMEM((2, 4 * share, depth), jnp.bfloat16),
                pltpu.VMEM((3, heads, n_rows, width), jnp.bfloat16),
                pltpu.VMEM((2, n_rows, width), jnp.bfloat16),
                dma((4,)), dma(()), dma((pieces,)),
                *[dma((pieces,)) for _ in range(10)],
                dma((3,)), dma((3,)), pltpu.SemaphoreType.REGULAR, pltpu.SemaphoreType.REGULAR,
                dma((pieces,)), dma((pieces,)), dma((pieces,)), dma((pieces,)),
                dma((heads,)), dma((heads,)), dma((2,)), dma((2,)),
            ],
            compiler_params=pltpu.CompilerParams(collective_id=0, has_side_effects=True, vmem_limit_bytes=36 * 1024 * 1024),
            cost_estimate=pl.CostEstimate(flops=2 * n_rows * depth * 2048, bytes_accessed=16 * 1024 * 1024, transcendentals=0),
            name="qkv",
        )(*[pltpu.with_memory_space_constraint(a, pltpu.HBM) for a in (x_rows, norm_gain, w_q.transpose(1, 0, 2), w_k.T, w_v.T)])
        q, k, v = pl.pallas_call(
            finish_kernel,
            out_shape=results,
            in_specs=[vmem] * 3,
            out_specs=(hbm,) * 3,
            scratch_shapes=[dma((4 * (heads + 2),))],
            compiler_params=pltpu.CompilerParams(vmem_limit_bytes=16 * 1024 * 1024),
            name="finish",
        )(q, k, v)
        late = pl.pallas_call(
            late_kernel,
            out_shape=late_shape,
            in_specs=[hbm, vmem],
            out_specs=vmem,
            scratch_shapes=[dma((heads - 1,)), dma((heads - 1,))],
            compiler_params=pltpu.CompilerParams(collective_id=1, has_side_effects=True, vmem_limit_bytes=16 * 1024 * 1024),
            name="late",
        )(pltpu.with_memory_space_constraint(q, pltpu.HBM), late)
        q = pl.pallas_call(
            patch_kernel,
            out_shape=results[0],
            in_specs=[hbm, vmem],
            out_specs=hbm,
            scratch_shapes=[dma((heads - 1,))],
            input_output_aliases={0: 0},
            compiler_params=pltpu.CompilerParams(vmem_limit_bytes=16 * 1024 * 1024),
            name="patch",
        )(q, late)
        return q.transpose(1, 0, 2), k.transpose(1, 0, 2), v.transpose(1, 0, 2)

    return jax.shard_map(
        local_step, mesh=mesh,
        in_specs=(P(("dp", "tp"), None), P(None), P(None, "tp", None), P(None, "tp"), P(None, "tp")),
        out_specs=(P("dp", "tp", None), P("dp", "tp", None), P("dp", "tp", None)),
        check_vma=False,
    )
```

```python
import functools

import jax
import jax.numpy as jnp
from jax import lax
from jax.experimental import pallas as pl
from jax.experimental.pallas import tpu as pltpu
from jax.sharding import PartitionSpec as P

EPSILON = 1e-6
MESH = pl.DeviceIdType.MESH
LANES = 128
K_PIECE, V_PIECE, FIRST_HEAD = 0, 1, 2


def qkv_kernel(
    x_hbm, gain_hbm, wq_hbm, wk_hbm, wv_hbm,
    q_out, k_out, v_out, late_out,
    rows_buf, gain_buf, wq_buf, wkv_buf, q_stage, kv_stage,
    x_sem, gain_sem, load_sem,
    part_send, part_recv, link_send, link_recv, core_send, core_recv, side_send, side_recv, last_send, last_recv,
    middle_send, middle_recv, ready_sem, pair_sem,
    near_send, near_recv, far_send, far_recv, cross_send, cross_recv, pass_send, pass_recv,
    *, norm_tile, dot_tile, shift,
):
    n_rows, depth = rows_buf.shape
    heads = wq_hbm.shape[0]
    share = wk_hbm.shape[0]
    half = depth // 2
    pieces = FIRST_HEAD + heads

    group, member = lax.axis_index("dp"), lax.axis_index("tp")
    chip, core = member // 2, member % 2
    partner = (group, chip * 2 + (1 - core))
    across = (group, (1 - chip) * 2 + core)
    across_other = (group, (1 - chip) * 2 + (1 - core))
    beside = (1 - group, member)

    sources = [wk_hbm, wv_hbm] + [wq_hbm.at[h] for h in range(heads)]

    last_head = pieces - 1
    middle = pl.ds(half - shift, 2 * shift)

    def piece_at(j, slot, depth_half=None):
        if j < FIRST_HEAD:
            rows = pl.ds(pl.multiple_of(j * 2 * share + core * share, share), share)
            if depth_half is None:
                return wkv_buf.at[slot // 2, rows]
            return wkv_buf.at[slot // 2, rows, pl.ds(pl.multiple_of(depth_half * half, half), half)]
        if depth_half is None:
            return wq_buf.at[slot, j - FIRST_HEAD]
        if j == last_head:
            start = pl.multiple_of(depth_half * (half + shift), 16)
            return wq_buf.at[slot, j - FIRST_HEAD, pl.ds(start, half - shift)]
        return wq_buf.at[slot, j - FIRST_HEAD, pl.ds(pl.multiple_of(depth_half * half, half), half)]

    firsts, rests = [], []
    for j in range(FIRST_HEAD):
        for copies, which, sem in ((firsts, group, j), (rests, 1 - group, pieces + j)):
            cols = pl.ds(pl.multiple_of(which * half, half), half)
            copies.append(pltpu.make_async_copy(sources[j].at[:, cols], piece_at(j, 0, which), load_sem.at[sem]))
    head_loads = [pltpu.make_async_copy(sources[j], piece_at(j, 0), load_sem.at[j]) for j in range(FIRST_HEAD, pieces)]
    for load in firsts:
        load.start()

    barrier = pltpu.get_barrier_semaphore()
    for other in (across, partner):
        pl.semaphore_signal(barrier, inc=1, device_id=other, device_id_type=MESH)

    @pl.when(group == 0)
    def _():
        pl.semaphore_signal(barrier, inc=1, device_id=beside, device_id_type=MESH)

    gain_load = pltpu.make_async_copy(gain_hbm, gain_buf, gain_sem)
    n_tiles = n_rows // norm_tile
    x_loads = [
        pltpu.make_async_copy(x_hbm.at[pl.ds(i * norm_tile, norm_tile)], rows_buf.at[pl.ds(i * norm_tile, norm_tile)], x_sem.at[i])
        for i in range(n_tiles)
    ]
    pl.semaphore_wait(barrier, 2 + group)

    def remote(src, dst, send, recv, device):
        return pltpu.make_async_remote_copy(src_ref=src, dst_ref=dst, send_sem=send, recv_sem=recv, device_id=device, device_id_type=MESH)

    part, link, hand, side, last = [], [], [], [], []
    for j in range(pieces):
        part.append(remote(piece_at(j, 0), piece_at(j, 0 if j < FIRST_HEAD else 1), part_send.at[j], part_recv.at[j], partner))
        link.append(remote(piece_at(j, 0, group), piece_at(j, 2, group), link_send.at[j], link_recv.at[j], across))
        arrived, other_half = piece_at(j, 2, group), piece_at(j, 2, 1 - group)
        hand.append(remote(arrived, piece_at(j, 2 if j < FIRST_HEAD else 3, group), core_send.at[j], core_recv.at[j], partner))
        side.append(remote(arrived, arrived, side_send.at[j], side_recv.at[j], beside))
        last.append(remote(other_half, piece_at(j, 2 if j < FIRST_HEAD else 3, 1 - group), last_send.at[j], last_recv.at[j], partner))

    def middle_at(slot):
        return wq_buf.at[slot, heads - 1, middle]

    middle_link = remote(middle_at(0), middle_at(2), middle_send.at[0], middle_recv.at[0], across)
    middle_side = remote(middle_at(2), middle_at(2), middle_send.at[1], middle_recv.at[1], beside)
    middle_hand = remote(middle_at(2), middle_at(3), middle_send.at[2], middle_recv.at[2], partner)

    my_rows = pl.ds(pl.multiple_of(member * n_rows, n_rows), n_rows)
    across_rows = pl.ds(pl.multiple_of(((1 - chip) * 2 + core) * n_rows, n_rows), n_rows)
    near = [remote(k_out.at[0, my_rows], k_out.at[0, my_rows], near_send.at[0], near_recv.at[0], partner),
            remote(v_out.at[0, my_rows], v_out.at[0, my_rows], near_send.at[1], near_recv.at[1], partner)]
    far = [remote(kv_stage.at[0], k_out.at[0, my_rows], far_send.at[0], far_recv.at[0], across),
           remote(kv_stage.at[1], v_out.at[0, my_rows], far_send.at[1], far_recv.at[1], across)]
    passed = [remote(k_out.at[0, across_rows], k_out.at[0, across_rows], pass_send.at[0], pass_recv.at[0], partner),
              remote(v_out.at[0, across_rows], v_out.at[0, across_rows], pass_send.at[1], pass_recv.at[1], partner)]
    cross = []
    for h in range(heads):
        near.append(remote(q_stage.at[0, h], q_out.at[h, my_rows], near_send.at[2 + h], near_recv.at[2 + h], partner))
        far.append(remote(q_stage.at[1, 0] if h == 0 else late_out.at[h - 1], q_out.at[h, my_rows], far_send.at[2 + h], far_recv.at[2 + h], across))
        cross.append(remote(q_stage.at[2, h], q_out.at[h, my_rows], cross_send.at[h], cross_recv.at[h], across_other))

    firsts[0].wait()
    link[0].start()
    for load in head_loads[:1] + rests + head_loads[1:] + [gain_load] + x_loads:
        load.start()
    firsts[1].wait()
    link[1].start()
    for j in range(FIRST_HEAD, pieces):
        head_loads[j - FIRST_HEAD].wait()
        link[j].start()
    for load in rests:
        load.wait()
    pl.semaphore_signal(pair_sem, inc=1, device_id=across, device_id_type=MESH)

    @pl.when(group == 1)
    def _():
        middle_link.start()
        pl.semaphore_signal(ready_sem, inc=1, device_id=beside, device_id_type=MESH)

    for copy in part:
        copy.start()

    gain_load.wait()
    chunks = depth // LANES
    sub = 64

    for i in range(n_tiles):
        x_loads[i].wait()

    def norm_step(s, carry):
        here = pl.ds(pl.multiple_of(s * sub, sub), sub)
        total = jnp.zeros((sub, LANES), jnp.float32)
        for c in range(chunks):
            wide = rows_buf[here, c * LANES:(c + 1) * LANES].astype(jnp.float32)
            total = total + wide * wide
        scale = lax.rsqrt(jnp.sum(total, axis=-1, keepdims=True) / depth + EPSILON)
        for c in range(chunks):
            cols = slice(c * LANES, (c + 1) * LANES)
            wide = rows_buf[here, cols].astype(jnp.float32)
            rows_buf[here, cols] = (wide * scale * gain_buf[cols][None, :]).astype(jnp.bfloat16)
        return carry

    lax.fori_loop(0, n_rows // sub, norm_step, 0)

    def over_tiles(step):
        lax.fori_loop(0, n_rows // dot_tile, lambda i, carry: (step(i * dot_tile), carry)[1], 0)

    def q_block(slot, h, store):
        def step(start):
            tile = rows_buf[pl.ds(pl.multiple_of(start, dot_tile), dot_tile), :]
            store(start, jnp.dot(tile, wq_buf[slot, h], preferred_element_type=jnp.float32).astype(jnp.bfloat16))
        over_tiles(step)

    def kv_block(which, store):
        def step(start):
            tile = rows_buf[pl.ds(pl.multiple_of(start, dot_tile), dot_tile), :]
            both = lax.dot_general(tile, wkv_buf[which], (((1,), (1,)), ((), ())), preferred_element_type=jnp.float32)
            store(start, both.astype(jnp.bfloat16))
        over_tiles(step)

    def rows_at(start):
        return pl.ds(pl.multiple_of(start, dot_tile), dot_tile)

    def own_rows_at(start):
        return pl.ds(pl.multiple_of(member * n_rows + start, dot_tile), dot_tile)

    def own_q(h):
        def store(start, value):
            q_out[h, own_rows_at(start), :] = value
        q_block(0, h, store)

    def staged_q(stage, slot, h):
        def store(start, value):
            q_stage[stage, h, rows_at(start), :] = value
        q_block(slot, h, store)

    def late_q(h):
        def store(start, value):
            late_out[h - 1, rows_at(start), :] = value
        q_block(2, h, store)

    def own_kv():
        def store(start, value):
            k_out[0, own_rows_at(start), :] = value[:, :LANES]
            v_out[0, own_rows_at(start), :] = value[:, LANES:]
        kv_block(0, store)

    def far_kv():
        def store(start, value):
            kv_stage[0, rows_at(start), :] = value[:, :LANES]
            kv_stage[1, rows_at(start), :] = value[:, LANES:]
        kv_block(1, store)

    def from_link(j):
        link[j].wait_recv()
        side[j].start()
        hand[j].start()

    def from_side(j):
        side[j].wait_recv()
        last[j].start()

    def from_middle():
        @pl.when(group == 1)
        def _():
            middle_link.wait_recv()
            middle_side.start()

        @pl.when(group == 0)
        def _():
            middle_side.wait_recv()

        middle_hand.start()

    def complete(j):
        hand[j].wait_recv()
        last[j].wait_recv()

    pl.semaphore_wait(pair_sem, 1)

    @pl.when(group == 0)
    def _():
        pl.semaphore_wait(ready_sem, 1)

    from_link(K_PIECE)
    from_link(V_PIECE)
    part[K_PIECE].wait_recv()
    part[V_PIECE].wait_recv()
    own_kv()
    from_side(K_PIECE)
    near[0].start()
    near[1].start()
    from_link(2)
    from_side(V_PIECE)
    complete(K_PIECE)
    complete(V_PIECE)
    far_kv()
    far[0].start()
    far[1].start()
    own_q(0)
    from_link(3)
    own_q(1)
    from_side(2)
    staged_q(1, 2, 0)
    from_link(4)
    complete(2)
    staged_q(2, 3, 0)
    far[2].start()
    from_side(3)
    complete(3)
    staged_q(2, 3, 1)
    cross[0].start()
    late_q(1)
    from_side(4)
    from_middle()
    cross[1].start()
    complete(4)
    middle_hand.wait_recv()
    staged_q(2, 3, 2)
    late_q(2)
    cross[2].start()
    own_q(2)

    @pl.when(core == 0)
    def _():
        for copy in far[FIRST_HEAD + 1:]:
            copy.start()

    for h in range(heads):
        part[FIRST_HEAD + h].wait_recv()
        staged_q(0, 1, h)
        if h:
            near[2 + h - 1].start()
    far[0].wait_recv()
    passed[0].start()
    far[1].wait_recv()
    passed[1].start()
    near[2 + heads - 1].start()

    for copy in part + link + hand + side + last + [middle_hand]:
        copy.wait_send()

    @pl.when(group == 1)
    def _():
        middle_link.wait_send()
        middle_side.wait_send()

    for copy in near + passed + cross:
        copy.wait()
    for copy in far[:FIRST_HEAD]:
        copy.wait_send()
    far[FIRST_HEAD].wait()

    @pl.when(core == 0)
    def _():
        for copy in far[FIRST_HEAD + 1:]:
            copy.wait()


def finish_kernel(q_ref, k_ref, v_ref, q_out, k_out, v_out, sems):
    member = lax.axis_index("tp")
    chip, core = member // 2, member % 2
    n_rows = q_ref.shape[1] // 4
    here, there = [], []
    for ref, out in ((q_ref, q_out), (k_ref, k_out), (v_ref, v_out)):
        for h in range(ref.shape[0]):
            for cut in range(4):
                where = pl.ds(pl.multiple_of(((3 - 2 * chip + cut + 1) % 4) * n_rows, n_rows), n_rows)
                copy = pltpu.make_async_copy(ref.at[h, where], out.at[h, where], sems.at[len(here) + len(there)])
                (there if cut == 3 and ref is q_ref and h else here).append(copy)

    for copy in here:
        copy.start()

    @pl.when(core == 0)
    def _():
        for copy in there:
            copy.start()

    for copy in here:
        copy.wait()

    @pl.when(core == 0)
    def _():
        for copy in there:
            copy.wait()


def late_kernel(after_ref, late_out, late_in, send_sem, recv_sem):
    group, member = lax.axis_index("dp"), lax.axis_index("tp")

    @pl.when(member % 2 == 1)
    def _():
        across = (group, (member + 2) % 4)
        barrier = pltpu.get_barrier_semaphore()
        pl.semaphore_signal(barrier, inc=1, device_id=across, device_id_type=MESH)
        pl.semaphore_wait(barrier, 1)
        copies = [
            pltpu.make_async_remote_copy(src_ref=late_out.at[i], dst_ref=late_in.at[i], send_sem=send_sem.at[i], recv_sem=recv_sem.at[i],
                                         device_id=across, device_id_type=MESH)
            for i in range(late_out.shape[0])
        ]
        for copy in copies:
            copy.start()
        for copy in copies:
            copy.wait()


def patch_kernel(before_ref, late_ref, q_out, sems):
    member = lax.axis_index("tp")
    n_rows = late_ref.shape[1]

    @pl.when(member % 2 == 1)
    def _():
        where = pl.ds(pl.multiple_of(((member + 2) % 4) * n_rows, n_rows), n_rows)
        copies = [pltpu.make_async_copy(late_ref.at[i], q_out.at[1 + i, where], sems.at[i]) for i in range(late_ref.shape[0])]
        for copy in copies:
            copy.start()
        for copy in copies:
            copy.wait()


def solution(mesh):
    def local_step(x_rows, norm_gain, w_q, w_k, w_v):
        n_rows, depth = x_rows.shape
        heads, width = w_q.shape[1:]
        share = w_k.shape[1]
        members = mesh.shape["tp"]
        pieces = FIRST_HEAD + heads
        all_rows = members * n_rows
        dma = pltpu.SemaphoreType.DMA
        norm_tile = n_rows // 4
        vmem = pl.BlockSpec(memory_space=pltpu.VMEM)
        results = tuple(jax.ShapeDtypeStruct((n, all_rows, width), jnp.bfloat16) for n in (heads, 1, 1))
        hbm = pl.BlockSpec(memory_space=pltpu.HBM)
        late_shape = jax.ShapeDtypeStruct((heads - 1, n_rows, width), jnp.bfloat16)
        q, k, v, late = pl.pallas_call(
            functools.partial(qkv_kernel, norm_tile=norm_tile, dot_tile=256, shift=80),
            out_shape=results + (late_shape,),
            in_specs=[hbm] * 5,
            out_specs=(vmem,) * 4,
            scratch_shapes=[
                pltpu.VMEM((n_rows, depth), jnp.bfloat16),
                pltpu.VMEM((depth,), jnp.float32),
                pltpu.VMEM((4, heads, depth, width), jnp.bfloat16),
                pltpu.VMEM((2, 4 * share, depth), jnp.bfloat16),
                pltpu.VMEM((3, heads, n_rows, width), jnp.bfloat16),
                pltpu.VMEM((2, n_rows, width), jnp.bfloat16),
                dma((4,)), dma(()), dma((pieces + FIRST_HEAD,)),
                *[dma((pieces,)) for _ in range(10)],
                dma((3,)), dma((3,)), pltpu.SemaphoreType.REGULAR, pltpu.SemaphoreType.REGULAR,
                dma((pieces,)), dma((pieces,)), dma((pieces,)), dma((pieces,)),
                dma((heads,)), dma((heads,)), dma((2,)), dma((2,)),
            ],
            compiler_params=pltpu.CompilerParams(collective_id=0, has_side_effects=True, vmem_limit_bytes=36 * 1024 * 1024),
            cost_estimate=pl.CostEstimate(flops=2 * n_rows * depth * 2048, bytes_accessed=16 * 1024 * 1024, transcendentals=0),
            name="qkv",
        )(*[pltpu.with_memory_space_constraint(a, pltpu.HBM) for a in (x_rows, norm_gain, w_q.transpose(1, 0, 2), w_k.T, w_v.T)])
        q, k, v = pl.pallas_call(
            finish_kernel,
            out_shape=results,
            in_specs=[vmem] * 3,
            out_specs=(hbm,) * 3,
            scratch_shapes=[dma((4 * (heads + 2),))],
            compiler_params=pltpu.CompilerParams(vmem_limit_bytes=16 * 1024 * 1024),
            name="finish",
        )(q, k, v)
        late = pl.pallas_call(
            late_kernel,
            out_shape=late_shape,
            in_specs=[hbm, vmem],
            out_specs=vmem,
            scratch_shapes=[dma((heads - 1,)), dma((heads - 1,))],
            compiler_params=pltpu.CompilerParams(collective_id=1, has_side_effects=True, vmem_limit_bytes=16 * 1024 * 1024),
            name="late",
        )(pltpu.with_memory_space_constraint(q, pltpu.HBM), late)
        q = pl.pallas_call(
            patch_kernel,
            out_shape=results[0],
            in_specs=[hbm, vmem],
            out_specs=hbm,
            scratch_shapes=[dma((heads - 1,))],
            input_output_aliases={0: 0},
            compiler_params=pltpu.CompilerParams(vmem_limit_bytes=16 * 1024 * 1024),
            name="patch",
        )(q, late)
        return q.transpose(1, 0, 2), k.transpose(1, 0, 2), v.transpose(1, 0, 2)

    return jax.shard_map(
        local_step, mesh=mesh,
        in_specs=(P(("dp", "tp"), None), P(None), P(None, "tp", None), P(None, "tp"), P(None, "tp")),
        out_specs=(P("dp", "tp", None), P("dp", "tp", None), P("dp", "tp", None)),
        check_vma=False,
    )
```

```python
import functools

import jax
import jax.numpy as jnp
from jax import lax
from jax.experimental import pallas as pl
from jax.experimental.pallas import tpu as pltpu
from jax.sharding import PartitionSpec as P

EPSILON = 1e-6
MESH = pl.DeviceIdType.MESH
LANES = 128
K_PIECE, V_PIECE, FIRST_HEAD = 0, 1, 2


def qkv_kernel(
    x_hbm, gain_hbm, wq_hbm, wk_hbm, wv_hbm,
    q_out, k_out, v_out, late_out,
    rows_buf, gain_buf, wq_buf, wkv_buf, q_stage, kv_stage,
    x_sem, gain_sem, load_sem,
    part_send, part_recv, link_send, link_recv, core_send, core_recv, side_send, side_recv, last_send, last_recv,
    middle_send, middle_recv, ready_sem, pair_sem,
    near_send, near_recv, far_send, far_recv, cross_send, cross_recv, pass_send, pass_recv,
    *, norm_tile, dot_tile, shift,
):
    n_rows, depth = rows_buf.shape
    heads = wq_hbm.shape[0]
    share = wk_hbm.shape[0]
    half = depth // 2
    pieces = FIRST_HEAD + heads

    group, member = lax.axis_index("dp"), lax.axis_index("tp")
    chip, core = member // 2, member % 2
    partner = (group, chip * 2 + (1 - core))
    across = (group, (1 - chip) * 2 + core)
    across_other = (group, (1 - chip) * 2 + (1 - core))
    beside = (1 - group, member)

    sources = [wk_hbm, wv_hbm] + [wq_hbm.at[h] for h in range(heads)]

    last_head = pieces - 1
    middle = pl.ds(half - shift, 2 * shift)

    def piece_at(j, slot, depth_half=None):
        if j < FIRST_HEAD:
            rows = pl.ds(pl.multiple_of(j * 2 * share + core * share, share), share)
            if depth_half is None:
                return wkv_buf.at[slot // 2, rows]
            return wkv_buf.at[slot // 2, rows, pl.ds(pl.multiple_of(depth_half * half, half), half)]
        if depth_half is None:
            return wq_buf.at[slot, j - FIRST_HEAD]
        if j == last_head:
            start = pl.multiple_of(depth_half * (half + shift), 16)
            return wq_buf.at[slot, j - FIRST_HEAD, pl.ds(start, half - shift)]
        return wq_buf.at[slot, j - FIRST_HEAD, pl.ds(pl.multiple_of(depth_half * half, half), half)]

    firsts, rests = [], []
    for j in range(FIRST_HEAD):
        for copies, which, sem in ((firsts, group, j), (rests, 1 - group, pieces + j)):
            cols = pl.ds(pl.multiple_of(which * half, half), half)
            copies.append(pltpu.make_async_copy(sources[j].at[:, cols], piece_at(j, 0, which), load_sem.at[sem]))
    head_loads = [pltpu.make_async_copy(sources[j], piece_at(j, 0), load_sem.at[j]) for j in range(FIRST_HEAD, pieces)]
    for load in firsts:
        load.start()

    barrier = pltpu.get_barrier_semaphore()
    for other in (across, partner):
        pl.semaphore_signal(barrier, inc=1, device_id=other, device_id_type=MESH)

    @pl.when(group == 0)
    def _():
        pl.semaphore_signal(barrier, inc=1, device_id=beside, device_id_type=MESH)

    gain_load = pltpu.make_async_copy(gain_hbm, gain_buf, gain_sem)
    n_tiles = n_rows // norm_tile
    x_loads = [
        pltpu.make_async_copy(x_hbm.at[pl.ds(i * norm_tile, norm_tile)], rows_buf.at[pl.ds(i * norm_tile, norm_tile)], x_sem.at[i])
        for i in range(n_tiles)
    ]
    pl.semaphore_wait(barrier, 2 + group)

    def remote(src, dst, send, recv, device):
        return pltpu.make_async_remote_copy(src_ref=src, dst_ref=dst, send_sem=send, recv_sem=recv, device_id=device, device_id_type=MESH)

    part, link, hand, side, last = [], [], [], [], []
    for j in range(pieces):
        part.append(remote(piece_at(j, 0), piece_at(j, 0 if j < FIRST_HEAD else 1), part_send.at[j], part_recv.at[j], partner))
        link.append(remote(piece_at(j, 0, group), piece_at(j, 2, group), link_send.at[j], link_recv.at[j], across))
        arrived, other_half = piece_at(j, 2, group), piece_at(j, 2, 1 - group)
        hand.append(remote(arrived, piece_at(j, 2 if j < FIRST_HEAD else 3, group), core_send.at[j], core_recv.at[j], partner))
        side.append(remote(arrived, arrived, side_send.at[j], side_recv.at[j], beside))
        last.append(remote(other_half, piece_at(j, 2 if j < FIRST_HEAD else 3, 1 - group), last_send.at[j], last_recv.at[j], partner))

    def middle_at(slot):
        return wq_buf.at[slot, heads - 1, middle]

    middle_link = remote(middle_at(0), middle_at(2), middle_send.at[0], middle_recv.at[0], across)
    middle_side = remote(middle_at(2), middle_at(2), middle_send.at[1], middle_recv.at[1], beside)
    middle_hand = remote(middle_at(2), middle_at(3), middle_send.at[2], middle_recv.at[2], partner)

    my_rows = pl.ds(pl.multiple_of(member * n_rows, n_rows), n_rows)
    across_rows = pl.ds(pl.multiple_of(((1 - chip) * 2 + core) * n_rows, n_rows), n_rows)
    near = [remote(k_out.at[0, my_rows], k_out.at[0, my_rows], near_send.at[0], near_recv.at[0], partner),
            remote(v_out.at[0, my_rows], v_out.at[0, my_rows], near_send.at[1], near_recv.at[1], partner)]
    far = [remote(kv_stage.at[0], k_out.at[0, my_rows], far_send.at[0], far_recv.at[0], across),
           remote(kv_stage.at[1], v_out.at[0, my_rows], far_send.at[1], far_recv.at[1], across)]
    passed = [remote(k_out.at[0, across_rows], k_out.at[0, across_rows], pass_send.at[0], pass_recv.at[0], partner),
              remote(v_out.at[0, across_rows], v_out.at[0, across_rows], pass_send.at[1], pass_recv.at[1], partner)]
    cross = []
    for h in range(heads):
        near.append(remote(q_stage.at[0, h], q_out.at[h, my_rows], near_send.at[2 + h], near_recv.at[2 + h], partner))
        far.append(remote(q_stage.at[1, 0] if h == 0 else late_out.at[h - 1], q_out.at[h, my_rows], far_send.at[2 + h], far_recv.at[2 + h], across))
        cross.append(remote(q_stage.at[2, h], q_out.at[h, my_rows], cross_send.at[h], cross_recv.at[h], across_other))

    firsts[0].wait()
    link[0].start()
    for load in head_loads[:1] + rests + head_loads[1:] + [gain_load] + x_loads:
        load.start()
    firsts[1].wait()
    link[1].start()
    for j in range(FIRST_HEAD, pieces):
        head_loads[j - FIRST_HEAD].wait()
        link[j].start()
    for load in rests:
        load.wait()
    pl.semaphore_signal(pair_sem, inc=1, device_id=across, device_id_type=MESH)

    @pl.when(group == 1)
    def _():
        middle_link.start()
        pl.semaphore_signal(ready_sem, inc=1, device_id=beside, device_id_type=MESH)

    for copy in part:
        copy.start()

    gain_load.wait()
    chunks = depth // LANES
    sub = 64

    for i in range(n_tiles):
        x_loads[i].wait()

    def norm_step(s, carry):
        here = pl.ds(pl.multiple_of(s * sub, sub), sub)
        total = jnp.zeros((sub, LANES), jnp.float32)
        for c in range(chunks):
            wide = rows_buf[here, c * LANES:(c + 1) * LANES].astype(jnp.float32)
            total = total + wide * wide
        scale = lax.rsqrt(jnp.sum(total, axis=-1, keepdims=True) / depth + EPSILON)
        for c in range(chunks):
            cols = slice(c * LANES, (c + 1) * LANES)
            wide = rows_buf[here, cols].astype(jnp.float32)
            rows_buf[here, cols] = (wide * scale * gain_buf[cols][None, :]).astype(jnp.bfloat16)
        return carry

    lax.fori_loop(0, n_rows // sub, norm_step, 0)

    def over_tiles(step):
        lax.fori_loop(0, n_rows // dot_tile, lambda i, carry: (step(i * dot_tile), carry)[1], 0)

    def q_block(slot, h, store):
        def step(start):
            tile = rows_buf[pl.ds(pl.multiple_of(start, dot_tile), dot_tile), :]
            store(start, jnp.dot(tile, wq_buf[slot, h], preferred_element_type=jnp.float32).astype(jnp.bfloat16))
        over_tiles(step)

    def kv_block(which, store):
        def step(start):
            tile = rows_buf[pl.ds(pl.multiple_of(start, dot_tile), dot_tile), :]
            both = lax.dot_general(tile, wkv_buf[which], (((1,), (1,)), ((), ())), preferred_element_type=jnp.float32)
            store(start, both.astype(jnp.bfloat16))
        over_tiles(step)

    def rows_at(start):
        return pl.ds(pl.multiple_of(start, dot_tile), dot_tile)

    def own_rows_at(start):
        return pl.ds(pl.multiple_of(member * n_rows + start, dot_tile), dot_tile)

    def own_q(h):
        def store(start, value):
            q_out[h, own_rows_at(start), :] = value
        q_block(0, h, store)

    def staged_q(stage, slot, h):
        def store(start, value):
            q_stage[stage, h, rows_at(start), :] = value
        q_block(slot, h, store)

    def late_q(h):
        def store(start, value):
            late_out[h - 1, rows_at(start), :] = value
        q_block(2, h, store)

    def own_kv():
        def store(start, value):
            k_out[0, own_rows_at(start), :] = value[:, :LANES]
            v_out[0, own_rows_at(start), :] = value[:, LANES:]
        kv_block(0, store)

    def far_kv():
        def store(start, value):
            kv_stage[0, rows_at(start), :] = value[:, :LANES]
            kv_stage[1, rows_at(start), :] = value[:, LANES:]
        kv_block(1, store)

    def from_link(j):
        link[j].wait_recv()
        side[j].start()
        hand[j].start()

    def from_side(j):
        side[j].wait_recv()
        last[j].start()

    def from_middle():
        @pl.when(group == 1)
        def _():
            middle_link.wait_recv()
            middle_side.start()

        @pl.when(group == 0)
        def _():
            middle_side.wait_recv()

        middle_hand.start()

    def complete(j):
        hand[j].wait_recv()
        last[j].wait_recv()

    pl.semaphore_wait(pair_sem, 1)

    @pl.when(group == 0)
    def _():
        pl.semaphore_wait(ready_sem, 1)

    from_link(K_PIECE)
    from_link(V_PIECE)
    part[K_PIECE].wait_recv()
    part[V_PIECE].wait_recv()
    own_kv()
    from_side(K_PIECE)
    near[0].start()
    near[1].start()
    from_link(2)
    from_side(V_PIECE)
    complete(K_PIECE)
    complete(V_PIECE)
    far_kv()
    far[0].start()
    far[1].start()
    own_q(0)
    from_link(3)
    own_q(1)
    from_side(2)
    staged_q(1, 2, 0)
    from_link(4)
    complete(2)
    staged_q(2, 3, 0)

    @pl.when(core == 1)
    def _():
        far[FIRST_HEAD].start()

    from_side(3)
    complete(3)
    staged_q(2, 3, 1)
    cross[0].start()
    late_q(1)
    from_side(4)
    from_middle()
    cross[1].start()
    complete(4)
    middle_hand.wait_recv()
    staged_q(2, 3, 2)
    late_q(2)
    cross[2].start()
    own_q(2)

    @pl.when(core == 0)
    def _():
        for copy in far[FIRST_HEAD:]:
            copy.start()

    for h in range(heads):
        part[FIRST_HEAD + h].wait_recv()
        staged_q(0, 1, h)
        if h:
            near[2 + h - 1].start()
    far[0].wait_recv()
    passed[0].start()
    far[1].wait_recv()
    passed[1].start()
    near[2 + heads - 1].start()

    for copy in part + link + hand + side + last + [middle_hand]:
        copy.wait_send()

    @pl.when(group == 1)
    def _():
        middle_link.wait_send()
        middle_side.wait_send()

    for copy in near + passed + cross:
        copy.wait()
    for copy in far[:FIRST_HEAD]:
        copy.wait_send()
    far[FIRST_HEAD].wait()

    @pl.when(core == 0)
    def _():
        for copy in far[FIRST_HEAD + 1:]:
            copy.wait()


def finish_kernel(q_ref, k_ref, v_ref, q_out, k_out, v_out, sems):
    member = lax.axis_index("tp")
    chip, core = member // 2, member % 2
    n_rows = q_ref.shape[1] // 4
    here, there = [], []
    for ref, out in ((q_ref, q_out), (k_ref, k_out), (v_ref, v_out)):
        for h in range(ref.shape[0]):
            for cut in range(4):
                where = pl.ds(pl.multiple_of(((3 - 2 * chip + cut + 1) % 4) * n_rows, n_rows), n_rows)
                copy = pltpu.make_async_copy(ref.at[h, where], out.at[h, where], sems.at[len(here) + len(there)])
                (there if cut == 3 and ref is q_ref and h else here).append(copy)

    for copy in here:
        copy.start()

    @pl.when(core == 0)
    def _():
        for copy in there:
            copy.start()

    for copy in here:
        copy.wait()

    @pl.when(core == 0)
    def _():
        for copy in there:
            copy.wait()


def late_kernel(after_ref, late_out, late_in, send_sem, recv_sem):
    group, member = lax.axis_index("dp"), lax.axis_index("tp")

    @pl.when(member % 2 == 1)
    def _():
        across = (group, (member + 2) % 4)
        barrier = pltpu.get_barrier_semaphore()
        pl.semaphore_signal(barrier, inc=1, device_id=across, device_id_type=MESH)
        pl.semaphore_wait(barrier, 1)
        copies = [
            pltpu.make_async_remote_copy(src_ref=late_out.at[i], dst_ref=late_in.at[i], send_sem=send_sem.at[i], recv_sem=recv_sem.at[i],
                                         device_id=across, device_id_type=MESH)
            for i in range(late_out.shape[0])
        ]
        for copy in copies:
            copy.start()
        for copy in copies:
            copy.wait()


def patch_kernel(before_ref, late_ref, q_out, sems):
    member = lax.axis_index("tp")
    n_rows = late_ref.shape[1]

    @pl.when(member % 2 == 1)
    def _():
        where = pl.ds(pl.multiple_of(((member + 2) % 4) * n_rows, n_rows), n_rows)
        copies = [pltpu.make_async_copy(late_ref.at[i], q_out.at[1 + i, where], sems.at[i]) for i in range(late_ref.shape[0])]
        for copy in copies:
            copy.start()
        for copy in copies:
            copy.wait()


def solution(mesh):
    def local_step(x_rows, norm_gain, w_q, w_k, w_v):
        n_rows, depth = x_rows.shape
        heads, width = w_q.shape[1:]
        share = w_k.shape[1]
        members = mesh.shape["tp"]
        pieces = FIRST_HEAD + heads
        all_rows = members * n_rows
        dma = pltpu.SemaphoreType.DMA
        norm_tile = n_rows // 4
        vmem = pl.BlockSpec(memory_space=pltpu.VMEM)
        results = tuple(jax.ShapeDtypeStruct((n, all_rows, width), jnp.bfloat16) for n in (heads, 1, 1))
        hbm = pl.BlockSpec(memory_space=pltpu.HBM)
        late_shape = jax.ShapeDtypeStruct((heads - 1, n_rows, width), jnp.bfloat16)
        q, k, v, late = pl.pallas_call(
            functools.partial(qkv_kernel, norm_tile=norm_tile, dot_tile=256, shift=80),
            out_shape=results + (late_shape,),
            in_specs=[hbm] * 5,
            out_specs=(vmem,) * 4,
            scratch_shapes=[
                pltpu.VMEM((n_rows, depth), jnp.bfloat16),
                pltpu.VMEM((depth,), jnp.float32),
                pltpu.VMEM((4, heads, depth, width), jnp.bfloat16),
                pltpu.VMEM((2, 4 * share, depth), jnp.bfloat16),
                pltpu.VMEM((3, heads, n_rows, width), jnp.bfloat16),
                pltpu.VMEM((2, n_rows, width), jnp.bfloat16),
                dma((4,)), dma(()), dma((pieces + FIRST_HEAD,)),
                *[dma((pieces,)) for _ in range(10)],
                dma((3,)), dma((3,)), pltpu.SemaphoreType.REGULAR, pltpu.SemaphoreType.REGULAR,
                dma((pieces,)), dma((pieces,)), dma((pieces,)), dma((pieces,)),
                dma((heads,)), dma((heads,)), dma((2,)), dma((2,)),
            ],
            compiler_params=pltpu.CompilerParams(collective_id=0, has_side_effects=True, vmem_limit_bytes=36 * 1024 * 1024),
            cost_estimate=pl.CostEstimate(flops=2 * n_rows * depth * 2048, bytes_accessed=16 * 1024 * 1024, transcendentals=0),
            name="qkv",
        )(*[pltpu.with_memory_space_constraint(a, pltpu.HBM) for a in (x_rows, norm_gain, w_q.transpose(1, 0, 2), w_k.T, w_v.T)])
        q, k, v = pl.pallas_call(
            finish_kernel,
            out_shape=results,
            in_specs=[vmem] * 3,
            out_specs=(hbm,) * 3,
            scratch_shapes=[dma((4 * (heads + 2),))],
            compiler_params=pltpu.CompilerParams(vmem_limit_bytes=16 * 1024 * 1024),
            name="finish",
        )(q, k, v)
        late = pl.pallas_call(
            late_kernel,
            out_shape=late_shape,
            in_specs=[hbm, vmem],
            out_specs=vmem,
            scratch_shapes=[dma((heads - 1,)), dma((heads - 1,))],
            compiler_params=pltpu.CompilerParams(collective_id=1, has_side_effects=True, vmem_limit_bytes=16 * 1024 * 1024),
            name="late",
        )(pltpu.with_memory_space_constraint(q, pltpu.HBM), late)
        q = pl.pallas_call(
            patch_kernel,
            out_shape=results[0],
            in_specs=[hbm, vmem],
            out_specs=hbm,
            scratch_shapes=[dma((heads - 1,))],
            input_output_aliases={0: 0},
            compiler_params=pltpu.CompilerParams(vmem_limit_bytes=16 * 1024 * 1024),
            name="patch",
        )(q, late)
        return q.transpose(1, 0, 2), k.transpose(1, 0, 2), v.transpose(1, 0, 2)

    return jax.shard_map(
        local_step, mesh=mesh,
        in_specs=(P(("dp", "tp"), None), P(None), P(None, "tp", None), P(None, "tp"), P(None, "tp")),
        out_specs=(P("dp", "tp", None), P("dp", "tp", None), P("dp", "tp", None)),
        check_vma=False,
    )
```

```python
import functools

import jax
import jax.numpy as jnp
from jax import lax
from jax.experimental import pallas as pl
from jax.experimental.pallas import tpu as pltpu
from jax.sharding import PartitionSpec as P

EPSILON = 1e-6
MESH = pl.DeviceIdType.MESH
LANES = 128
K_PIECE, V_PIECE, FIRST_HEAD = 0, 1, 2


def qkv_kernel(
    x_hbm, gain_hbm, wq_hbm, wk_hbm, wv_hbm,
    q_out, k_out, v_out, late_out,
    rows_buf, gain_buf, wq_buf, wkv_buf, q_stage, kv_stage,
    x_sem, gain_sem, load_sem,
    part_send, part_recv, link_send, link_recv, core_send, core_recv, side_send, side_recv, last_send, last_recv,
    middle_send, middle_recv, ready_sem, pair_sem, lent_buf, lent_sem, early_sem,
    near_send, near_recv, far_send, far_recv, cross_send, cross_recv, pass_send, pass_recv,
    *, norm_tile, dot_tile, shift, lent, early,
):
    n_rows, depth = rows_buf.shape
    heads = wq_hbm.shape[0]
    share = wk_hbm.shape[0]
    half = depth // 2
    pieces = FIRST_HEAD + heads

    group, member = lax.axis_index("dp"), lax.axis_index("tp")
    chip, core = member // 2, member % 2
    partner = (group, chip * 2 + (1 - core))
    across = (group, (1 - chip) * 2 + core)
    across_other = (group, (1 - chip) * 2 + (1 - core))
    beside = (1 - group, member)

    sources = [wk_hbm, wv_hbm] + [wq_hbm.at[h] for h in range(heads)]

    last_head = pieces - 1
    middle = pl.ds(half - shift, 2 * shift)

    def piece_at(j, slot, depth_half=None):
        if j < FIRST_HEAD:
            rows = pl.ds(pl.multiple_of(j * 2 * share + core * share, share), share)
            if depth_half is None:
                return wkv_buf.at[slot // 2, rows]
            return wkv_buf.at[slot // 2, rows, pl.ds(pl.multiple_of(depth_half * half, half), half)]
        if depth_half is None:
            return wq_buf.at[slot, j - FIRST_HEAD]
        if j == last_head:
            start = pl.multiple_of(depth_half * (half + shift), 8)
            return wq_buf.at[slot, j - FIRST_HEAD, pl.ds(start, half - shift)]
        return wq_buf.at[slot, j - FIRST_HEAD, pl.ds(pl.multiple_of(depth_half * half, half), half)]

    firsts, rests = [], []
    for j in range(FIRST_HEAD):
        for copies, which, sem in ((firsts, group, j), (rests, 1 - group, pieces + j)):
            cols = pl.ds(pl.multiple_of(which * half, half), half)
            copies.append(pltpu.make_async_copy(sources[j].at[:, cols], piece_at(j, 0, which), load_sem.at[sem]))
    head_loads = [pltpu.make_async_copy(sources[j], piece_at(j, 0), load_sem.at[j]) for j in range(FIRST_HEAD, pieces)]
    for load in firsts:
        load.start()

    barrier = pltpu.get_barrier_semaphore()
    for other in (across, partner):
        pl.semaphore_signal(barrier, inc=1, device_id=other, device_id_type=MESH)

    @pl.when(group == 0)
    def _():
        pl.semaphore_signal(barrier, inc=1, device_id=beside, device_id_type=MESH)

    gain_load = pltpu.make_async_copy(gain_hbm, gain_buf, gain_sem)
    n_tiles = n_rows // norm_tile
    x_loads = [
        pltpu.make_async_copy(x_hbm.at[pl.ds(i * norm_tile, norm_tile)], rows_buf.at[pl.ds(i * norm_tile, norm_tile)], x_sem.at[i])
        for i in range(n_tiles)
    ]
    pl.semaphore_wait(barrier, 2 + group)

    def remote(src, dst, send, recv, device):
        return pltpu.make_async_remote_copy(src_ref=src, dst_ref=dst, send_sem=send, recv_sem=recv, device_id=device, device_id_type=MESH)

    part, link, hand, side, last = [], [], [], [], []
    for j in range(pieces):
        part.append(remote(piece_at(j, 0), piece_at(j, 0 if j < FIRST_HEAD else 1), part_send.at[j], part_recv.at[j], partner))
        link.append(remote(piece_at(j, 0, group), piece_at(j, 2, group), link_send.at[j], link_recv.at[j], across))
        arrived, other_half = piece_at(j, 2, group), piece_at(j, 2, 1 - group)
        hand.append(remote(arrived, piece_at(j, 2 if j < FIRST_HEAD else 3, group), core_send.at[j], core_recv.at[j], partner))
        side.append(remote(arrived, arrived, side_send.at[j], side_recv.at[j], beside))
        last.append(remote(other_half, piece_at(j, 2 if j < FIRST_HEAD else 3, 1 - group), last_send.at[j], last_recv.at[j], partner))

    def middle_at(slot):
        return wq_buf.at[slot, heads - 1, middle]

    middle_link = remote(middle_at(0), middle_at(2), middle_send.at[0], middle_recv.at[0], across)
    middle_side = remote(middle_at(2), middle_at(2), middle_send.at[1], middle_recv.at[1], beside)
    middle_hand = remote(middle_at(2), middle_at(3), middle_send.at[2], middle_recv.at[2], partner)

    my_rows = pl.ds(pl.multiple_of(member * n_rows, n_rows), n_rows)
    across_rows = pl.ds(pl.multiple_of(((1 - chip) * 2 + core) * n_rows, n_rows), n_rows)
    near = [remote(k_out.at[0, my_rows], k_out.at[0, my_rows], near_send.at[0], near_recv.at[0], partner),
            remote(v_out.at[0, my_rows], v_out.at[0, my_rows], near_send.at[1], near_recv.at[1], partner)]
    far = [remote(kv_stage.at[0], k_out.at[0, my_rows], far_send.at[0], far_recv.at[0], across),
           remote(kv_stage.at[1], v_out.at[0, my_rows], far_send.at[1], far_recv.at[1], across)]
    passed = [remote(k_out.at[0, across_rows], k_out.at[0, across_rows], pass_send.at[0], pass_recv.at[0], partner),
              remote(v_out.at[0, across_rows], v_out.at[0, across_rows], pass_send.at[1], pass_recv.at[1], partner)]
    cross = []
    for h in range(heads):
        near.append(remote(q_stage.at[0, h], q_out.at[h, my_rows], near_send.at[2 + h], near_recv.at[2 + h], partner))
        far.append(remote(q_stage.at[1, 0] if h == 0 else late_out.at[h - 1], q_out.at[h, my_rows], far_send.at[2 + h], far_recv.at[2 + h], across))
        cross.append(remote(q_stage.at[2, h], q_out.at[h, my_rows], cross_send.at[h], cross_recv.at[h], across_other))

    last_h = heads - 1
    lent_rows, kept_rows = pl.ds(0, lent), pl.ds(lent, n_rows - lent)
    my_kept = pl.ds(pl.multiple_of(member * n_rows + lent, lent), n_rows - lent)
    partner_lent = pl.ds(pl.multiple_of((chip * 2 + 1 - core) * n_rows, n_rows), lent)
    lend = remote(q_stage.at[2, last_h, lent_rows], lent_buf, lent_sem.at[0], lent_sem.at[1], partner)
    cross_kept = remote(q_stage.at[2, last_h, kept_rows], q_out.at[last_h, my_kept], cross_send.at[last_h], cross_recv.at[last_h], across_other)
    cross_lent = remote(lent_buf, q_out.at[last_h, partner_lent], lent_sem.at[2], lent_sem.at[3], across)
    my_early = pl.ds(pl.multiple_of(member * n_rows, n_rows), early)
    early_far = remote(late_out.at[0, pl.ds(0, early)], q_out.at[1, my_early], early_sem.at[0], early_sem.at[1], across)

    firsts[0].wait()
    link[0].start()
    for load in head_loads[:1] + rests + head_loads[1:] + [gain_load] + x_loads:
        load.start()
    firsts[1].wait()
    link[1].start()
    for j in range(FIRST_HEAD, pieces):
        head_loads[j - FIRST_HEAD].wait()
        link[j].start()
    for load in rests:
        load.wait()
    pl.semaphore_signal(pair_sem, inc=1, device_id=across, device_id_type=MESH)

    @pl.when(group == 1)
    def _():
        middle_link.start()
        pl.semaphore_signal(ready_sem, inc=1, device_id=beside, device_id_type=MESH)

    for copy in part:
        copy.start()

    gain_load.wait()
    chunks = depth // LANES
    sub = 64

    for i in range(n_tiles):
        x_loads[i].wait()

    def norm_step(s, carry):
        here = pl.ds(pl.multiple_of(s * sub, sub), sub)
        total = jnp.zeros((sub, LANES), jnp.float32)
        for c in range(chunks):
            wide = rows_buf[here, c * LANES:(c + 1) * LANES].astype(jnp.float32)
            total = total + wide * wide
        scale = lax.rsqrt(jnp.sum(total, axis=-1, keepdims=True) / depth + EPSILON)
        for c in range(chunks):
            cols = slice(c * LANES, (c + 1) * LANES)
            wide = rows_buf[here, cols].astype(jnp.float32)
            rows_buf[here, cols] = (wide * scale * gain_buf[cols][None, :]).astype(jnp.bfloat16)
        return carry

    lax.fori_loop(0, n_rows // sub, norm_step, 0)

    def over_tiles(step):
        lax.fori_loop(0, n_rows // dot_tile, lambda i, carry: (step(i * dot_tile), carry)[1], 0)

    def q_block(slot, h, store):
        def step(start):
            tile = rows_buf[pl.ds(pl.multiple_of(start, dot_tile), dot_tile), :]
            store(start, jnp.dot(tile, wq_buf[slot, h], preferred_element_type=jnp.float32).astype(jnp.bfloat16))
        over_tiles(step)

    def kv_block(which, store):
        def step(start):
            tile = rows_buf[pl.ds(pl.multiple_of(start, dot_tile), dot_tile), :]
            both = lax.dot_general(tile, wkv_buf[which], (((1,), (1,)), ((), ())), preferred_element_type=jnp.float32)
            store(start, both.astype(jnp.bfloat16))
        over_tiles(step)

    def rows_at(start):
        return pl.ds(pl.multiple_of(start, dot_tile), dot_tile)

    def own_rows_at(start):
        return pl.ds(pl.multiple_of(member * n_rows + start, dot_tile), dot_tile)

    def when(condition, act):
        pl.when(condition)(act)

    def own_q(h):
        def store(start, value):
            q_out[h, own_rows_at(start), :] = value
        q_block(0, h, store)

    def staged_q(stage, slot, h):
        def store(start, value):
            q_stage[stage, h, rows_at(start), :] = value
        q_block(slot, h, store)

    def late_q(h):
        def store(start, value):
            late_out[h - 1, rows_at(start), :] = value
        q_block(2, h, store)

    def own_kv():
        def store(start, value):
            k_out[0, own_rows_at(start), :] = value[:, :LANES]
            v_out[0, own_rows_at(start), :] = value[:, LANES:]
        kv_block(0, store)

    def far_kv():
        def store(start, value):
            kv_stage[0, rows_at(start), :] = value[:, :LANES]
            kv_stage[1, rows_at(start), :] = value[:, LANES:]
        kv_block(1, store)

    def from_link(j):
        link[j].wait_recv()
        side[j].start()
        hand[j].start()

    def from_side(j):
        side[j].wait_recv()
        last[j].start()

    def from_middle():
        @pl.when(group == 1)
        def _():
            middle_link.wait_recv()
            middle_side.start()

        @pl.when(group == 0)
        def _():
            middle_side.wait_recv()

        middle_hand.start()

    def complete(j):
        hand[j].wait_recv()
        last[j].wait_recv()

    pl.semaphore_wait(pair_sem, 1)

    @pl.when(group == 0)
    def _():
        pl.semaphore_wait(ready_sem, 1)

    from_link(K_PIECE)
    from_link(V_PIECE)
    part[K_PIECE].wait_recv()
    part[V_PIECE].wait_recv()
    own_kv()
    from_side(K_PIECE)
    near[0].start()
    near[1].start()
    from_link(2)
    from_side(V_PIECE)
    complete(K_PIECE)
    complete(V_PIECE)
    far_kv()
    far[0].start()
    far[1].start()
    own_q(0)
    from_link(3)
    own_q(1)
    from_side(2)
    staged_q(1, 2, 0)
    from_link(4)
    complete(2)
    staged_q(2, 3, 0)

    @pl.when(core == 1)
    def _():
        far[FIRST_HEAD].start()

    from_side(3)
    complete(3)
    staged_q(2, 3, 1)
    cross[0].start()
    late_q(1)
    from_side(4)
    from_middle()
    cross[1].start()
    complete(4)
    middle_hand.wait_recv()
    staged_q(2, 3, 2)
    late_q(2)
    when(core == 0, lend.start)
    own_q(2)

    @pl.when(core == 1)
    def _():
        lend.wait_recv()
        cross_lent.start()
        early_far.start()
        cross[last_h].start()

    @pl.when(core == 0)
    def _():
        cross_kept.start()
        for copy in far[FIRST_HEAD:]:
            copy.start()

    for h in range(heads):
        part[FIRST_HEAD + h].wait_recv()
        staged_q(0, 1, h)
        if h:
            near[2 + h - 1].start()
    far[0].wait_recv()
    passed[0].start()
    far[1].wait_recv()
    passed[1].start()
    near[2 + heads - 1].start()

    for copy in part + link + hand + side + last + [middle_hand]:
        copy.wait_send()

    @pl.when(group == 1)
    def _():
        middle_link.wait_send()
        middle_side.wait_send()

    for copy in near + passed + cross[:last_h]:
        copy.wait()
    for copy in far[:FIRST_HEAD]:
        copy.wait_send()
    far[FIRST_HEAD].wait()

    @pl.when(core == 0)
    def _():
        for copy in far[FIRST_HEAD + 1:]:
            copy.wait()
        lend.wait_send()
        cross_kept.wait_send()
        cross[last_h].wait_recv()

    @pl.when(core == 1)
    def _():
        cross[last_h].wait_send()
        early_far.wait()
        cross_lent.wait()
        cross_kept.wait_recv()


def finish_kernel(q_ref, k_ref, v_ref, q_out, k_out, v_out, sems, *, early):
    member = lax.axis_index("tp")
    chip, core = member // 2, member % 2
    n_rows = q_ref.shape[1] // 4
    here, there = [], []
    for ref, out in ((q_ref, q_out), (k_ref, k_out), (v_ref, v_out)):
        for h in range(ref.shape[0]):
            for cut in range(4):
                where = pl.ds(pl.multiple_of(((3 - 2 * chip + cut + 1) % 4) * n_rows, n_rows), n_rows)
                copy = pltpu.make_async_copy(ref.at[h, where], out.at[h, where], sems.at[len(here) + len(there)])
                (there if cut == 3 and ref is q_ref and h else here).append(copy)

    for copy in here:
        copy.start()

    early_rows = pl.ds(pl.multiple_of((3 - 2 * chip) * n_rows, n_rows), early)
    early_copy = pltpu.make_async_copy(q_ref.at[1, early_rows], q_out.at[1, early_rows], sems.at[len(here) + len(there)])

    @pl.when(core == 1)
    def _():
        early_copy.start()

    @pl.when(core == 0)
    def _():
        for copy in there:
            copy.start()

    for copy in here:
        copy.wait()

    @pl.when(core == 1)
    def _():
        early_copy.wait()

    @pl.when(core == 0)
    def _():
        for copy in there:
            copy.wait()


def late_cut(early, n_rows, i):
    return pl.ds(early, n_rows - early) if i == 0 else pl.ds(0, n_rows)


def late_kernel(after_ref, late_out, late_in, send_sem, recv_sem, *, early):
    group, member = lax.axis_index("dp"), lax.axis_index("tp")

    @pl.when(member % 2 == 1)
    def _():
        across = (group, (member + 2) % 4)
        barrier = pltpu.get_barrier_semaphore()
        pl.semaphore_signal(barrier, inc=1, device_id=across, device_id_type=MESH)
        pl.semaphore_wait(barrier, 1)
        copies = [
            pltpu.make_async_remote_copy(src_ref=late_out.at[i, cut], dst_ref=late_in.at[i, cut], send_sem=send_sem.at[i],
                                         recv_sem=recv_sem.at[i], device_id=across, device_id_type=MESH)
            for i, cut in enumerate(late_cut(early, late_out.shape[1], i) for i in range(late_out.shape[0]))
        ]
        for copy in copies:
            copy.start()
        for copy in copies:
            copy.wait()


def patch_kernel(before_ref, late_ref, q_out, sems, *, early):
    member = lax.axis_index("tp")
    n_rows = late_ref.shape[1]

    @pl.when(member % 2 == 1)
    def _():
        base = ((member + 2) % 4) * n_rows
        copies = []
        for i in range(late_ref.shape[0]):
            cut = late_cut(early, n_rows, i)
            where = pl.ds(pl.multiple_of(base + cut.start, early), cut.size)
            copies.append(pltpu.make_async_copy(late_ref.at[i, cut], q_out.at[1 + i, where], sems.at[i]))
        for copy in copies:
            copy.start()
        for copy in copies:
            copy.wait()


def solution(mesh):
    def local_step(x_rows, norm_gain, w_q, w_k, w_v):
        n_rows, depth = x_rows.shape
        heads, width = w_q.shape[1:]
        share = w_k.shape[1]
        members = mesh.shape["tp"]
        pieces = FIRST_HEAD + heads
        all_rows = members * n_rows
        dma = pltpu.SemaphoreType.DMA
        norm_tile = n_rows // 4
        shift, lent, early = 72, 128, 512
        vmem = pl.BlockSpec(memory_space=pltpu.VMEM)
        results = tuple(jax.ShapeDtypeStruct((n, all_rows, width), jnp.bfloat16) for n in (heads, 1, 1))
        hbm = pl.BlockSpec(memory_space=pltpu.HBM)
        late_shape = jax.ShapeDtypeStruct((heads - 1, n_rows, width), jnp.bfloat16)
        q, k, v, late = pl.pallas_call(
            functools.partial(qkv_kernel, norm_tile=norm_tile, dot_tile=256, shift=shift, lent=lent, early=early),
            out_shape=results + (late_shape,),
            in_specs=[hbm] * 5,
            out_specs=(vmem,) * 4,
            scratch_shapes=[
                pltpu.VMEM((n_rows, depth), jnp.bfloat16),
                pltpu.VMEM((depth,), jnp.float32),
                pltpu.VMEM((4, heads, depth, width), jnp.bfloat16),
                pltpu.VMEM((2, 4 * share, depth), jnp.bfloat16),
                pltpu.VMEM((3, heads, n_rows, width), jnp.bfloat16),
                pltpu.VMEM((2, n_rows, width), jnp.bfloat16),
                dma((4,)), dma(()), dma((pieces + FIRST_HEAD,)),
                *[dma((pieces,)) for _ in range(10)],
                dma((3,)), dma((3,)), pltpu.SemaphoreType.REGULAR, pltpu.SemaphoreType.REGULAR,
                pltpu.VMEM((lent, width), jnp.bfloat16), dma((4,)), dma((2,)),
                dma((pieces,)), dma((pieces,)), dma((pieces,)), dma((pieces,)),
                dma((heads,)), dma((heads,)), dma((2,)), dma((2,)),
            ],
            compiler_params=pltpu.CompilerParams(collective_id=0, has_side_effects=True, vmem_limit_bytes=36 * 1024 * 1024),
            cost_estimate=pl.CostEstimate(flops=2 * n_rows * depth * 2048, bytes_accessed=16 * 1024 * 1024, transcendentals=0),
            name="qkv",
        )(*[pltpu.with_memory_space_constraint(a, pltpu.HBM) for a in (x_rows, norm_gain, w_q.transpose(1, 0, 2), w_k.T, w_v.T)])
        q, k, v = pl.pallas_call(
            functools.partial(finish_kernel, early=early),
            out_shape=results,
            in_specs=[vmem] * 3,
            out_specs=(hbm,) * 3,
            scratch_shapes=[dma((4 * (heads + 2) + 1,))],
            compiler_params=pltpu.CompilerParams(vmem_limit_bytes=16 * 1024 * 1024),
            name="finish",
        )(q, k, v)
        late = pl.pallas_call(
            functools.partial(late_kernel, early=early),
            out_shape=late_shape,
            in_specs=[hbm, vmem],
            out_specs=vmem,
            scratch_shapes=[dma((heads - 1,)), dma((heads - 1,))],
            compiler_params=pltpu.CompilerParams(collective_id=1, has_side_effects=True, vmem_limit_bytes=16 * 1024 * 1024),
            name="late",
        )(pltpu.with_memory_space_constraint(q, pltpu.HBM), late)
        q = pl.pallas_call(
            functools.partial(patch_kernel, early=early),
            out_shape=results[0],
            in_specs=[hbm, vmem],
            out_specs=hbm,
            scratch_shapes=[dma((heads - 1,))],
            input_output_aliases={0: 0},
            compiler_params=pltpu.CompilerParams(vmem_limit_bytes=16 * 1024 * 1024),
            name="patch",
        )(q, late)
        return q.transpose(1, 0, 2), k.transpose(1, 0, 2), v.transpose(1, 0, 2)

    return jax.shard_map(
        local_step, mesh=mesh,
        in_specs=(P(("dp", "tp"), None), P(None), P(None, "tp", None), P(None, "tp"), P(None, "tp")),
        out_specs=(P("dp", "tp", None), P("dp", "tp", None), P("dp", "tp", None)),
        check_vma=False,
    )
```

```python
import functools

import jax
import jax.numpy as jnp
from jax import lax
from jax.experimental import pallas as pl
from jax.experimental.pallas import tpu as pltpu
from jax.sharding import PartitionSpec as P

EPSILON = 1e-6
MESH = pl.DeviceIdType.MESH
LANES = 128
K_PIECE, V_PIECE, FIRST_HEAD = 0, 1, 2


def qkv_kernel(
    x_hbm, gain_hbm, wq_hbm, wk_hbm, wv_hbm,
    q_out, k_out, v_out, late_out,
    rows_buf, gain_buf, wq_buf, wkv_buf, q_stage, kv_stage,
    x_sem, gain_sem, load_sem,
    part_send, part_recv, link_send, link_recv, core_send, core_recv, side_send, side_recv, last_send, last_recv,
    middle_send, middle_recv, ready_sem, pair_sem, lent_buf, lent_sem, early_sem,
    near_send, near_recv, far_send, far_recv, cross_send, cross_recv, pass_send, pass_recv,
    *, norm_tile, dot_tile, shift, lent, early,
):
    n_rows, depth = rows_buf.shape
    heads = wq_hbm.shape[0]
    share = wk_hbm.shape[0]
    half = depth // 2
    pieces = FIRST_HEAD + heads

    group, member = lax.axis_index("dp"), lax.axis_index("tp")
    chip, core = member // 2, member % 2
    partner = (group, chip * 2 + (1 - core))
    across = (group, (1 - chip) * 2 + core)
    across_other = (group, (1 - chip) * 2 + (1 - core))
    beside = (1 - group, member)

    sources = [wk_hbm, wv_hbm] + [wq_hbm.at[h] for h in range(heads)]

    last_head = pieces - 1
    middle = pl.ds(half - shift, 2 * shift)

    def piece_at(j, slot, depth_half=None):
        if j < FIRST_HEAD:
            rows = pl.ds(pl.multiple_of(j * 2 * share + core * share, share), share)
            if depth_half is None:
                return wkv_buf.at[slot // 2, rows]
            return wkv_buf.at[slot // 2, rows, pl.ds(pl.multiple_of(depth_half * half, half), half)]
        if depth_half is None:
            return wq_buf.at[slot, j - FIRST_HEAD]
        if j == last_head:
            start = pl.multiple_of(depth_half * (half + shift), 8)
            return wq_buf.at[slot, j - FIRST_HEAD, pl.ds(start, half - shift)]
        return wq_buf.at[slot, j - FIRST_HEAD, pl.ds(pl.multiple_of(depth_half * half, half), half)]

    firsts, rests = [], []
    for j in range(FIRST_HEAD):
        for copies, which, sem in ((firsts, group, j), (rests, 1 - group, pieces + j)):
            cols = pl.ds(pl.multiple_of(which * half, half), half)
            copies.append(pltpu.make_async_copy(sources[j].at[:, cols], piece_at(j, 0, which), load_sem.at[sem]))
    head_loads = [pltpu.make_async_copy(sources[j], piece_at(j, 0), load_sem.at[j]) for j in range(FIRST_HEAD, pieces)]
    for load in firsts:
        load.start()

    barrier = pltpu.get_barrier_semaphore()
    for other in (across, partner):
        pl.semaphore_signal(barrier, inc=1, device_id=other, device_id_type=MESH)

    @pl.when(group == 0)
    def _():
        pl.semaphore_signal(barrier, inc=1, device_id=beside, device_id_type=MESH)

    gain_load = pltpu.make_async_copy(gain_hbm, gain_buf, gain_sem)
    n_tiles = n_rows // norm_tile
    x_loads = [
        pltpu.make_async_copy(x_hbm.at[pl.ds(i * norm_tile, norm_tile)], rows_buf.at[pl.ds(i * norm_tile, norm_tile)], x_sem.at[i])
        for i in range(n_tiles)
    ]
    for load in head_loads[:1] + rests + head_loads[1:] + [gain_load] + x_loads:
        load.start()
    pl.semaphore_wait(barrier, 2 + group)

    def remote(src, dst, send, recv, device):
        return pltpu.make_async_remote_copy(src_ref=src, dst_ref=dst, send_sem=send, recv_sem=recv, device_id=device, device_id_type=MESH)

    part, link, hand, side, last = [], [], [], [], []
    for j in range(pieces):
        part.append(remote(piece_at(j, 0), piece_at(j, 0 if j < FIRST_HEAD else 1), part_send.at[j], part_recv.at[j], partner))
        link.append(remote(piece_at(j, 0, group), piece_at(j, 2, group), link_send.at[j], link_recv.at[j], across))
        arrived, other_half = piece_at(j, 2, group), piece_at(j, 2, 1 - group)
        hand.append(remote(arrived, piece_at(j, 2 if j < FIRST_HEAD else 3, group), core_send.at[j], core_recv.at[j], partner))
        side.append(remote(arrived, arrived, side_send.at[j], side_recv.at[j], beside))
        last.append(remote(other_half, piece_at(j, 2 if j < FIRST_HEAD else 3, 1 - group), last_send.at[j], last_recv.at[j], partner))

    def middle_at(slot):
        return wq_buf.at[slot, heads - 1, middle]

    middle_link = remote(middle_at(0), middle_at(2), middle_send.at[0], middle_recv.at[0], across)
    middle_side = remote(middle_at(2), middle_at(2), middle_send.at[1], middle_recv.at[1], beside)
    middle_hand = remote(middle_at(2), middle_at(3), middle_send.at[2], middle_recv.at[2], partner)

    my_rows = pl.ds(pl.multiple_of(member * n_rows, n_rows), n_rows)
    across_rows = pl.ds(pl.multiple_of(((1 - chip) * 2 + core) * n_rows, n_rows), n_rows)
    near = [remote(k_out.at[0, my_rows], k_out.at[0, my_rows], near_send.at[0], near_recv.at[0], partner),
            remote(v_out.at[0, my_rows], v_out.at[0, my_rows], near_send.at[1], near_recv.at[1], partner)]
    far = [remote(kv_stage.at[0], k_out.at[0, my_rows], far_send.at[0], far_recv.at[0], across),
           remote(kv_stage.at[1], v_out.at[0, my_rows], far_send.at[1], far_recv.at[1], across)]
    passed = [remote(k_out.at[0, across_rows], k_out.at[0, across_rows], pass_send.at[0], pass_recv.at[0], partner),
              remote(v_out.at[0, across_rows], v_out.at[0, across_rows], pass_send.at[1], pass_recv.at[1], partner)]
    cross = []
    for h in range(heads):
        near.append(remote(q_stage.at[0, h], q_out.at[h, my_rows], near_send.at[2 + h], near_recv.at[2 + h], partner))
        far.append(remote(q_stage.at[1, 0] if h == 0 else late_out.at[h - 1], q_out.at[h, my_rows], far_send.at[2 + h], far_recv.at[2 + h], across))
        cross.append(remote(q_stage.at[2, h], q_out.at[h, my_rows], cross_send.at[h], cross_recv.at[h], across_other))

    last_h = heads - 1
    lent_rows, kept_rows = pl.ds(0, lent), pl.ds(lent, n_rows - lent)
    my_kept = pl.ds(pl.multiple_of(member * n_rows + lent, lent), n_rows - lent)
    partner_lent = pl.ds(pl.multiple_of((chip * 2 + 1 - core) * n_rows, n_rows), lent)
    lend = remote(q_stage.at[2, last_h, lent_rows], lent_buf, lent_sem.at[0], lent_sem.at[1], partner)
    cross_kept = remote(q_stage.at[2, last_h, kept_rows], q_out.at[last_h, my_kept], cross_send.at[last_h], cross_recv.at[last_h], across_other)
    cross_lent = remote(lent_buf, q_out.at[last_h, partner_lent], lent_sem.at[2], lent_sem.at[3], across)
    my_early = pl.ds(pl.multiple_of(member * n_rows, n_rows), early)
    early_far = remote(late_out.at[0, pl.ds(0, early)], q_out.at[1, my_early], early_sem.at[0], early_sem.at[1], across)

    firsts[0].wait()
    link[0].start()
    firsts[1].wait()
    link[1].start()
    for j in range(FIRST_HEAD, pieces):
        head_loads[j - FIRST_HEAD].wait()
        link[j].start()
    for load in rests:
        load.wait()
    pl.semaphore_signal(pair_sem, inc=1, device_id=across, device_id_type=MESH)

    @pl.when(group == 1)
    def _():
        middle_link.start()
        pl.semaphore_signal(ready_sem, inc=1, device_id=beside, device_id_type=MESH)

    for copy in part:
        copy.start()

    gain_load.wait()
    chunks = depth // LANES
    sub = 64

    for i in range(n_tiles):
        x_loads[i].wait()

    def norm_step(s, carry):
        here = pl.ds(pl.multiple_of(s * sub, sub), sub)
        total = jnp.zeros((sub, LANES), jnp.float32)
        for c in range(chunks):
            wide = rows_buf[here, c * LANES:(c + 1) * LANES].astype(jnp.float32)
            total = total + wide * wide
        scale = lax.rsqrt(jnp.sum(total, axis=-1, keepdims=True) / depth + EPSILON)
        for c in range(chunks):
            cols = slice(c * LANES, (c + 1) * LANES)
            wide = rows_buf[here, cols].astype(jnp.float32)
            rows_buf[here, cols] = (wide * scale * gain_buf[cols][None, :]).astype(jnp.bfloat16)
        return carry

    lax.fori_loop(0, n_rows // sub, norm_step, 0)

    def over_tiles(step):
        lax.fori_loop(0, n_rows // dot_tile, lambda i, carry: (step(i * dot_tile), carry)[1], 0)

    def q_block(slot, h, store):
        def step(start):
            tile = rows_buf[pl.ds(pl.multiple_of(start, dot_tile), dot_tile), :]
            store(start, jnp.dot(tile, wq_buf[slot, h], preferred_element_type=jnp.float32).astype(jnp.bfloat16))
        over_tiles(step)

    def kv_block(which, store):
        def step(start):
            tile = rows_buf[pl.ds(pl.multiple_of(start, dot_tile), dot_tile), :]
            both = lax.dot_general(tile, wkv_buf[which], (((1,), (1,)), ((), ())), preferred_element_type=jnp.float32)
            store(start, both.astype(jnp.bfloat16))
        over_tiles(step)

    def rows_at(start):
        return pl.ds(pl.multiple_of(start, dot_tile), dot_tile)

    def own_rows_at(start):
        return pl.ds(pl.multiple_of(member * n_rows + start, dot_tile), dot_tile)

    def when(condition, act):
        pl.when(condition)(act)

    def own_q(h):
        def store(start, value):
            q_out[h, own_rows_at(start), :] = value
        q_block(0, h, store)

    def staged_q(stage, slot, h):
        def store(start, value):
            q_stage[stage, h, rows_at(start), :] = value
        q_block(slot, h, store)

    def late_q(h):
        def store(start, value):
            late_out[h - 1, rows_at(start), :] = value
        q_block(2, h, store)

    def own_kv():
        def store(start, value):
            k_out[0, own_rows_at(start), :] = value[:, :LANES]
            v_out[0, own_rows_at(start), :] = value[:, LANES:]
        kv_block(0, store)

    def far_kv():
        def store(start, value):
            kv_stage[0, rows_at(start), :] = value[:, :LANES]
            kv_stage[1, rows_at(start), :] = value[:, LANES:]
        kv_block(1, store)

    def from_link(j):
        link[j].wait_recv()
        side[j].start()
        hand[j].start()

    def from_side(j):
        side[j].wait_recv()
        last[j].start()

    def from_middle():
        @pl.when(group == 1)
        def _():
            middle_link.wait_recv()
            middle_side.start()

        @pl.when(group == 0)
        def _():
            middle_side.wait_recv()

        middle_hand.start()

    def complete(j):
        hand[j].wait_recv()
        last[j].wait_recv()

    pl.semaphore_wait(pair_sem, 1)

    @pl.when(group == 0)
    def _():
        pl.semaphore_wait(ready_sem, 1)

    from_link(K_PIECE)
    from_link(V_PIECE)
    part[K_PIECE].wait_recv()
    part[V_PIECE].wait_recv()
    own_kv()
    from_side(K_PIECE)
    near[0].start()
    near[1].start()
    from_link(2)
    from_side(V_PIECE)
    complete(K_PIECE)
    complete(V_PIECE)
    far_kv()
    far[0].start()
    far[1].start()
    own_q(0)
    from_link(3)
    own_q(1)
    from_side(2)
    staged_q(1, 2, 0)
    from_link(4)
    complete(2)
    staged_q(2, 3, 0)

    @pl.when(core == 1)
    def _():
        far[FIRST_HEAD].start()

    from_side(3)
    complete(3)
    staged_q(2, 3, 1)
    cross[0].start()
    late_q(1)
    from_side(4)
    from_middle()
    cross[1].start()
    complete(4)
    middle_hand.wait_recv()
    staged_q(2, 3, 2)
    late_q(2)
    when(core == 0, lend.start)
    own_q(2)

    @pl.when(core == 1)
    def _():
        lend.wait_recv()
        cross_lent.start()
        early_far.start()
        cross[last_h].start()

    @pl.when(core == 0)
    def _():
        cross_kept.start()
        for copy in far[FIRST_HEAD:]:
            copy.start()

    for h in range(heads):
        part[FIRST_HEAD + h].wait_recv()
        staged_q(0, 1, h)
        if h:
            near[2 + h - 1].start()
    far[0].wait_recv()
    passed[0].start()
    far[1].wait_recv()
    passed[1].start()
    near[2 + heads - 1].start()

    for copy in part + link + hand + side + last + [middle_hand]:
        copy.wait_send()

    @pl.when(group == 1)
    def _():
        middle_link.wait_send()
        middle_side.wait_send()

    for copy in near + passed + cross[:last_h]:
        copy.wait()
    for copy in far[:FIRST_HEAD]:
        copy.wait_send()
    far[FIRST_HEAD].wait()

    @pl.when(core == 0)
    def _():
        for copy in far[FIRST_HEAD + 1:]:
            copy.wait()
        lend.wait_send()
        cross_kept.wait_send()
        cross[last_h].wait_recv()

    @pl.when(core == 1)
    def _():
        cross[last_h].wait_send()
        early_far.wait()
        cross_lent.wait()
        cross_kept.wait_recv()


def finish_kernel(q_ref, k_ref, v_ref, q_out, k_out, v_out, sems, *, early):
    member = lax.axis_index("tp")
    chip, core = member // 2, member % 2
    n_rows = q_ref.shape[1] // 4
    here, there = [], []
    for ref, out in ((q_ref, q_out), (k_ref, k_out), (v_ref, v_out)):
        for h in range(ref.shape[0]):
            for cut in range(4):
                where = pl.ds(pl.multiple_of(((3 - 2 * chip + cut + 1) % 4) * n_rows, n_rows), n_rows)
                copy = pltpu.make_async_copy(ref.at[h, where], out.at[h, where], sems.at[len(here) + len(there)])
                (there if cut == 3 and ref is q_ref and h else here).append(copy)

    for copy in here:
        copy.start()

    early_rows = pl.ds(pl.multiple_of((3 - 2 * chip) * n_rows, n_rows), early)
    early_copy = pltpu.make_async_copy(q_ref.at[1, early_rows], q_out.at[1, early_rows], sems.at[len(here) + len(there)])

    @pl.when(core == 1)
    def _():
        early_copy.start()

    @pl.when(core == 0)
    def _():
        for copy in there:
            copy.start()

    for copy in here:
        copy.wait()

    @pl.when(core == 1)
    def _():
        early_copy.wait()

    @pl.when(core == 0)
    def _():
        for copy in there:
            copy.wait()


def late_cut(early, n_rows, i):
    return pl.ds(early, n_rows - early) if i == 0 else pl.ds(0, n_rows)


def late_kernel(after_ref, late_out, late_in, send_sem, recv_sem, *, early):
    group, member = lax.axis_index("dp"), lax.axis_index("tp")

    @pl.when(member % 2 == 1)
    def _():
        across = (group, (member + 2) % 4)
        barrier = pltpu.get_barrier_semaphore()
        pl.semaphore_signal(barrier, inc=1, device_id=across, device_id_type=MESH)
        pl.semaphore_wait(barrier, 1)
        copies = [
            pltpu.make_async_remote_copy(src_ref=late_out.at[i, cut], dst_ref=late_in.at[i, cut], send_sem=send_sem.at[i],
                                         recv_sem=recv_sem.at[i], device_id=across, device_id_type=MESH)
            for i, cut in enumerate(late_cut(early, late_out.shape[1], i) for i in range(late_out.shape[0]))
        ]
        for copy in copies:
            copy.start()
        for copy in copies:
            copy.wait()


def patch_kernel(before_ref, late_ref, q_out, sems, *, early):
    member = lax.axis_index("tp")
    n_rows = late_ref.shape[1]

    @pl.when(member % 2 == 1)
    def _():
        base = ((member + 2) % 4) * n_rows
        copies = []
        for i in range(late_ref.shape[0]):
            cut = late_cut(early, n_rows, i)
            where = pl.ds(pl.multiple_of(base + cut.start, early), cut.size)
            copies.append(pltpu.make_async_copy(late_ref.at[i, cut], q_out.at[1 + i, where], sems.at[i]))
        for copy in copies:
            copy.start()
        for copy in copies:
            copy.wait()


def solution(mesh):
    def local_step(x_rows, norm_gain, w_q, w_k, w_v):
        n_rows, depth = x_rows.shape
        heads, width = w_q.shape[1:]
        share = w_k.shape[1]
        members = mesh.shape["tp"]
        pieces = FIRST_HEAD + heads
        all_rows = members * n_rows
        dma = pltpu.SemaphoreType.DMA
        norm_tile = n_rows // 4
        shift, lent, early = 72, 128, 512
        vmem = pl.BlockSpec(memory_space=pltpu.VMEM)
        results = tuple(jax.ShapeDtypeStruct((n, all_rows, width), jnp.bfloat16) for n in (heads, 1, 1))
        hbm = pl.BlockSpec(memory_space=pltpu.HBM)
        late_shape = jax.ShapeDtypeStruct((heads - 1, n_rows, width), jnp.bfloat16)
        q, k, v, late = pl.pallas_call(
            functools.partial(qkv_kernel, norm_tile=norm_tile, dot_tile=256, shift=shift, lent=lent, early=early),
            out_shape=results + (late_shape,),
            in_specs=[hbm] * 5,
            out_specs=(vmem,) * 4,
            scratch_shapes=[
                pltpu.VMEM((n_rows, depth), jnp.bfloat16),
                pltpu.VMEM((depth,), jnp.float32),
                pltpu.VMEM((4, heads, depth, width), jnp.bfloat16),
                pltpu.VMEM((2, 4 * share, depth), jnp.bfloat16),
                pltpu.VMEM((3, heads, n_rows, width), jnp.bfloat16),
                pltpu.VMEM((2, n_rows, width), jnp.bfloat16),
                dma((4,)), dma(()), dma((pieces + FIRST_HEAD,)),
                *[dma((pieces,)) for _ in range(10)],
                dma((3,)), dma((3,)), pltpu.SemaphoreType.REGULAR, pltpu.SemaphoreType.REGULAR,
                pltpu.VMEM((lent, width), jnp.bfloat16), dma((4,)), dma((2,)),
                dma((pieces,)), dma((pieces,)), dma((pieces,)), dma((pieces,)),
                dma((heads,)), dma((heads,)), dma((2,)), dma((2,)),
            ],
            compiler_params=pltpu.CompilerParams(collective_id=0, has_side_effects=True, vmem_limit_bytes=36 * 1024 * 1024),
            cost_estimate=pl.CostEstimate(flops=2 * n_rows * depth * 2048, bytes_accessed=16 * 1024 * 1024, transcendentals=0),
            name="qkv",
        )(*[pltpu.with_memory_space_constraint(a, pltpu.HBM) for a in (x_rows, norm_gain, w_q.transpose(1, 0, 2), w_k.T, w_v.T)])
        q, k, v = pl.pallas_call(
            functools.partial(finish_kernel, early=early),
            out_shape=results,
            in_specs=[vmem] * 3,
            out_specs=(hbm,) * 3,
            scratch_shapes=[dma((4 * (heads + 2) + 1,))],
            compiler_params=pltpu.CompilerParams(vmem_limit_bytes=16 * 1024 * 1024),
            name="finish",
        )(q, k, v)
        late = pl.pallas_call(
            functools.partial(late_kernel, early=early),
            out_shape=late_shape,
            in_specs=[hbm, vmem],
            out_specs=vmem,
            scratch_shapes=[dma((heads - 1,)), dma((heads - 1,))],
            compiler_params=pltpu.CompilerParams(collective_id=1, has_side_effects=True, vmem_limit_bytes=16 * 1024 * 1024),
            name="late",
        )(pltpu.with_memory_space_constraint(q, pltpu.HBM), late)
        q = pl.pallas_call(
            functools.partial(patch_kernel, early=early),
            out_shape=results[0],
            in_specs=[hbm, vmem],
            out_specs=hbm,
            scratch_shapes=[dma((heads - 1,))],
            input_output_aliases={0: 0},
            compiler_params=pltpu.CompilerParams(vmem_limit_bytes=16 * 1024 * 1024),
            name="patch",
        )(q, late)
        return q.transpose(1, 0, 2), k.transpose(1, 0, 2), v.transpose(1, 0, 2)

    return jax.shard_map(
        local_step, mesh=mesh,
        in_specs=(P(("dp", "tp"), None), P(None), P(None, "tp", None), P(None, "tp"), P(None, "tp")),
        out_specs=(P("dp", "tp", None), P("dp", "tp", None), P("dp", "tp", None)),
        check_vma=False,
    )
```

```python
import functools

import jax
import jax.numpy as jnp
from jax import lax
from jax.experimental import pallas as pl
from jax.experimental.pallas import tpu as pltpu
from jax.sharding import PartitionSpec as P

EPSILON = 1e-6
MESH = pl.DeviceIdType.MESH
LANES = 128
K_PIECE, V_PIECE, FIRST_HEAD = 0, 1, 2


def qkv_kernel(
    x_hbm, gain_hbm, wq_hbm, wk_hbm, wv_hbm,
    q_out, k_out, v_out, late_out,
    rows_buf, gain_buf, wq_buf, wkv_buf, q_stage, kv_stage,
    x_sem, gain_sem, load_sem,
    part_send, part_recv, link_send, link_recv, core_send, core_recv, side_send, side_recv, last_send, last_recv,
    middle_send, middle_recv, ready_sem, pair_sem, lent_buf, lent_sem, early_sem,
    near_send, near_recv, far_send, far_recv, cross_send, cross_recv, pass_send, pass_recv,
    *, norm_tile, dot_tile, shift, lent, early,
):
    n_rows, depth = rows_buf.shape
    heads = wq_hbm.shape[0]
    share = wk_hbm.shape[0]
    half = depth // 2
    pieces = FIRST_HEAD + heads

    group, member = lax.axis_index("dp"), lax.axis_index("tp")
    chip, core = member // 2, member % 2
    partner = (group, chip * 2 + (1 - core))
    across = (group, (1 - chip) * 2 + core)
    across_other = (group, (1 - chip) * 2 + (1 - core))
    beside = (1 - group, member)

    sources = [wk_hbm, wv_hbm] + [wq_hbm.at[h] for h in range(heads)]

    last_head = pieces - 1
    middle = pl.ds(half - shift, 2 * shift)

    def piece_at(j, slot, depth_half=None):
        if j < FIRST_HEAD:
            rows = pl.ds(pl.multiple_of(j * 2 * share + core * share, share), share)
            if depth_half is None:
                return wkv_buf.at[slot // 2, rows]
            return wkv_buf.at[slot // 2, rows, pl.ds(pl.multiple_of(depth_half * half, half), half)]
        if depth_half is None:
            return wq_buf.at[slot, j - FIRST_HEAD]
        if j == last_head:
            start = pl.multiple_of(depth_half * (half + shift), 8)
            return wq_buf.at[slot, j - FIRST_HEAD, pl.ds(start, half - shift)]
        return wq_buf.at[slot, j - FIRST_HEAD, pl.ds(pl.multiple_of(depth_half * half, half), half)]

    firsts, rests = [], []
    for j in range(FIRST_HEAD):
        for copies, which, sem in ((firsts, group, j), (rests, 1 - group, pieces + j)):
            cols = pl.ds(pl.multiple_of(which * half, half), half)
            copies.append(pltpu.make_async_copy(sources[j].at[:, cols], piece_at(j, 0, which), load_sem.at[sem]))
    head_loads = [pltpu.make_async_copy(sources[j], piece_at(j, 0), load_sem.at[j]) for j in range(FIRST_HEAD, pieces)]
    for load in firsts:
        load.start()

    barrier = pltpu.get_barrier_semaphore()
    for other in (across, partner):
        pl.semaphore_signal(barrier, inc=1, device_id=other, device_id_type=MESH)

    @pl.when(group == 0)
    def _():
        pl.semaphore_signal(barrier, inc=1, device_id=beside, device_id_type=MESH)

    gain_load = pltpu.make_async_copy(gain_hbm, gain_buf, gain_sem)
    n_tiles = n_rows // norm_tile
    x_loads = [
        pltpu.make_async_copy(x_hbm.at[pl.ds(i * norm_tile, norm_tile)], rows_buf.at[pl.ds(i * norm_tile, norm_tile)], x_sem.at[i])
        for i in range(n_tiles)
    ]
    for load in head_loads[:1] + rests + head_loads[1:] + [gain_load] + x_loads:
        load.start()
    pl.semaphore_wait(barrier, 2 + group)

    def remote(src, dst, send, recv, device):
        return pltpu.make_async_remote_copy(src_ref=src, dst_ref=dst, send_sem=send, recv_sem=recv, device_id=device, device_id_type=MESH)

    part, link, hand, side, last = [], [], [], [], []
    for j in range(pieces):
        part.append(remote(piece_at(j, 0), piece_at(j, 0 if j < FIRST_HEAD else 1), part_send.at[j], part_recv.at[j], partner))
        link.append(remote(piece_at(j, 0, group), piece_at(j, 2, group), link_send.at[j], link_recv.at[j], across))
        arrived, other_half = piece_at(j, 2, group), piece_at(j, 2, 1 - group)
        hand.append(remote(arrived, piece_at(j, 2 if j < FIRST_HEAD else 3, group), core_send.at[j], core_recv.at[j], partner))
        side.append(remote(arrived, arrived, side_send.at[j], side_recv.at[j], beside))
        last.append(remote(other_half, piece_at(j, 2 if j < FIRST_HEAD else 3, 1 - group), last_send.at[j], last_recv.at[j], partner))

    def middle_at(slot):
        return wq_buf.at[slot, heads - 1, middle]

    middle_link = remote(middle_at(0), middle_at(2), middle_send.at[0], middle_recv.at[0], across)
    middle_side = remote(middle_at(2), middle_at(2), middle_send.at[1], middle_recv.at[1], beside)
    middle_hand = remote(middle_at(2), middle_at(3), middle_send.at[2], middle_recv.at[2], partner)

    my_rows = pl.ds(pl.multiple_of(member * n_rows, n_rows), n_rows)
    across_rows = pl.ds(pl.multiple_of(((1 - chip) * 2 + core) * n_rows, n_rows), n_rows)
    near = [remote(k_out.at[0, my_rows], k_out.at[0, my_rows], near_send.at[0], near_recv.at[0], partner),
            remote(v_out.at[0, my_rows], v_out.at[0, my_rows], near_send.at[1], near_recv.at[1], partner)]
    far = [remote(kv_stage.at[0], k_out.at[0, my_rows], far_send.at[0], far_recv.at[0], across),
           remote(kv_stage.at[1], v_out.at[0, my_rows], far_send.at[1], far_recv.at[1], across)]
    passed = [remote(k_out.at[0, across_rows], k_out.at[0, across_rows], pass_send.at[0], pass_recv.at[0], partner),
              remote(v_out.at[0, across_rows], v_out.at[0, across_rows], pass_send.at[1], pass_recv.at[1], partner)]
    cross = []
    for h in range(heads):
        near.append(remote(q_stage.at[0, h], q_out.at[h, my_rows], near_send.at[2 + h], near_recv.at[2 + h], partner))
        far.append(remote(q_stage.at[1, 0] if h == 0 else late_out.at[h - 1], q_out.at[h, my_rows], far_send.at[2 + h], far_recv.at[2 + h], across))
        cross.append(remote(q_stage.at[2, h], q_out.at[h, my_rows], cross_send.at[h], cross_recv.at[h], across_other))

    last_h = heads - 1
    lent_rows, kept_rows = pl.ds(0, lent), pl.ds(lent, n_rows - lent)
    my_kept = pl.ds(pl.multiple_of(member * n_rows + lent, lent), n_rows - lent)
    partner_lent = pl.ds(pl.multiple_of((chip * 2 + 1 - core) * n_rows, n_rows), lent)
    lend = remote(q_stage.at[2, last_h, lent_rows], lent_buf, lent_sem.at[0], lent_sem.at[1], partner)
    cross_kept = remote(q_stage.at[2, last_h, kept_rows], q_out.at[last_h, my_kept], cross_send.at[last_h], cross_recv.at[last_h], across_other)
    cross_lent = remote(lent_buf, q_out.at[last_h, partner_lent], lent_sem.at[2], lent_sem.at[3], across)
    my_early = pl.ds(pl.multiple_of(member * n_rows, n_rows), early)
    early_far = remote(late_out.at[0, pl.ds(0, early)], q_out.at[1, my_early], early_sem.at[0], early_sem.at[1], across)

    firsts[0].wait()
    link[0].start()
    firsts[1].wait()
    link[1].start()
    pl.semaphore_signal(pair_sem, inc=1, device_id=across, device_id_type=MESH)

    @pl.when(group == 1)
    def _():
        pl.semaphore_signal(ready_sem, inc=1, device_id=beside, device_id_type=MESH)

    pl.semaphore_wait(pair_sem, 1)
    for j in range(FIRST_HEAD, pieces):
        head_loads[j - FIRST_HEAD].wait()
        link[j].start()
    for load in rests:
        load.wait()

    @pl.when(group == 1)
    def _():
        middle_link.start()

    for copy in part:
        copy.start()

    chunks = depth // LANES
    sub = 64

    def norm_step(s, carry):
        here = pl.ds(pl.multiple_of(s * sub, sub), sub)
        total = jnp.zeros((sub, LANES), jnp.float32)
        for c in range(chunks):
            wide = rows_buf[here, c * LANES:(c + 1) * LANES].astype(jnp.float32)
            total = total + wide * wide
        scale = lax.rsqrt(jnp.sum(total, axis=-1, keepdims=True) / depth + EPSILON)
        for c in range(chunks):
            cols = slice(c * LANES, (c + 1) * LANES)
            wide = rows_buf[here, cols].astype(jnp.float32)
            rows_buf[here, cols] = (wide * scale * gain_buf[cols][None, :]).astype(jnp.bfloat16)
        return carry

    def normalize():
        gain_load.wait()
        for load in x_loads:
            load.wait()
        lax.fori_loop(0, n_rows // sub, norm_step, 0)

    def over_tiles(step):
        lax.fori_loop(0, n_rows // dot_tile, lambda i, carry: (step(i * dot_tile), carry)[1], 0)

    def q_block(slot, h, store):
        def step(start):
            tile = rows_buf[pl.ds(pl.multiple_of(start, dot_tile), dot_tile), :]
            store(start, jnp.dot(tile, wq_buf[slot, h], preferred_element_type=jnp.float32).astype(jnp.bfloat16))
        over_tiles(step)

    def kv_block(which, store):
        def step(start):
            tile = rows_buf[pl.ds(pl.multiple_of(start, dot_tile), dot_tile), :]
            both = lax.dot_general(tile, wkv_buf[which], (((1,), (1,)), ((), ())), preferred_element_type=jnp.float32)
            store(start, both.astype(jnp.bfloat16))
        over_tiles(step)

    def rows_at(start):
        return pl.ds(pl.multiple_of(start, dot_tile), dot_tile)

    def own_rows_at(start):
        return pl.ds(pl.multiple_of(member * n_rows + start, dot_tile), dot_tile)

    def when(condition, act):
        pl.when(condition)(act)

    def own_q(h):
        def store(start, value):
            q_out[h, own_rows_at(start), :] = value
        q_block(0, h, store)

    def staged_q(stage, slot, h):
        def store(start, value):
            q_stage[stage, h, rows_at(start), :] = value
        q_block(slot, h, store)

    def late_q(h):
        def store(start, value):
            late_out[h - 1, rows_at(start), :] = value
        q_block(2, h, store)

    def own_kv():
        def store(start, value):
            k_out[0, own_rows_at(start), :] = value[:, :LANES]
            v_out[0, own_rows_at(start), :] = value[:, LANES:]
        kv_block(0, store)

    def far_kv():
        def store(start, value):
            kv_stage[0, rows_at(start), :] = value[:, :LANES]
            kv_stage[1, rows_at(start), :] = value[:, LANES:]
        kv_block(1, store)

    def from_link(j):
        link[j].wait_recv()
        side[j].start()
        hand[j].start()

    def from_side(j):
        side[j].wait_recv()
        last[j].start()

    def from_middle():
        @pl.when(group == 1)
        def _():
            middle_link.wait_recv()
            middle_side.start()

        @pl.when(group == 0)
        def _():
            middle_side.wait_recv()

        middle_hand.start()

    def complete(j):
        hand[j].wait_recv()
        last[j].wait_recv()

    @pl.when(group == 0)
    def _():
        pl.semaphore_wait(ready_sem, 1)

    from_link(K_PIECE)
    normalize()
    from_link(V_PIECE)
    part[K_PIECE].wait_recv()
    part[V_PIECE].wait_recv()
    own_kv()
    from_side(K_PIECE)
    near[0].start()
    near[1].start()
    from_link(2)
    from_side(V_PIECE)
    complete(K_PIECE)
    complete(V_PIECE)
    far_kv()
    far[0].start()
    far[1].start()
    own_q(0)
    from_link(3)
    own_q(1)
    from_side(2)
    staged_q(1, 2, 0)
    from_link(4)
    complete(2)
    staged_q(2, 3, 0)

    @pl.when(core == 1)
    def _():
        far[FIRST_HEAD].start()

    from_side(3)
    complete(3)
    staged_q(2, 3, 1)
    cross[0].start()
    late_q(1)
    from_side(4)
    from_middle()
    cross[1].start()
    complete(4)
    middle_hand.wait_recv()
    staged_q(2, 3, 2)
    late_q(2)
    when(core == 0, lend.start)
    own_q(2)

    @pl.when(core == 1)
    def _():
        lend.wait_recv()
        cross_lent.start()
        early_far.start()
        cross[last_h].start()

    @pl.when(core == 0)
    def _():
        cross_kept.start()
        for copy in far[FIRST_HEAD:]:
            copy.start()

    for h in range(heads):
        part[FIRST_HEAD + h].wait_recv()
        staged_q(0, 1, h)
        if h:
            near[2 + h - 1].start()
    far[0].wait_recv()
    passed[0].start()
    far[1].wait_recv()
    passed[1].start()
    near[2 + heads - 1].start()

    for copy in part + link + hand + side + last + [middle_hand]:
        copy.wait_send()

    @pl.when(group == 1)
    def _():
        middle_link.wait_send()
        middle_side.wait_send()

    for copy in near + passed + cross[:last_h]:
        copy.wait()
    for copy in far[:FIRST_HEAD]:
        copy.wait_send()
    far[FIRST_HEAD].wait()

    @pl.when(core == 0)
    def _():
        for copy in far[FIRST_HEAD + 1:]:
            copy.wait()
        lend.wait_send()
        cross_kept.wait_send()
        cross[last_h].wait_recv()

    @pl.when(core == 1)
    def _():
        cross[last_h].wait_send()
        early_far.wait()
        cross_lent.wait()
        cross_kept.wait_recv()


def finish_kernel(q_ref, k_ref, v_ref, q_out, k_out, v_out, sems, *, early):
    member = lax.axis_index("tp")
    chip, core = member // 2, member % 2
    n_rows = q_ref.shape[1] // 4
    here, there = [], []
    for ref, out in ((q_ref, q_out), (k_ref, k_out), (v_ref, v_out)):
        for h in range(ref.shape[0]):
            for cut in range(4):
                where = pl.ds(pl.multiple_of(((3 - 2 * chip + cut + 1) % 4) * n_rows, n_rows), n_rows)
                copy = pltpu.make_async_copy(ref.at[h, where], out.at[h, where], sems.at[len(here) + len(there)])
                (there if cut == 3 and ref is q_ref and h else here).append(copy)

    for copy in here:
        copy.start()

    early_rows = pl.ds(pl.multiple_of((3 - 2 * chip) * n_rows, n_rows), early)
    early_copy = pltpu.make_async_copy(q_ref.at[1, early_rows], q_out.at[1, early_rows], sems.at[len(here) + len(there)])

    @pl.when(core == 1)
    def _():
        early_copy.start()

    @pl.when(core == 0)
    def _():
        for copy in there:
            copy.start()

    for copy in here:
        copy.wait()

    @pl.when(core == 1)
    def _():
        early_copy.wait()

    @pl.when(core == 0)
    def _():
        for copy in there:
            copy.wait()


def late_cut(early, n_rows, i):
    return pl.ds(early, n_rows - early) if i == 0 else pl.ds(0, n_rows)


def late_kernel(after_ref, late_out, late_in, send_sem, recv_sem, *, early):
    group, member = lax.axis_index("dp"), lax.axis_index("tp")

    @pl.when(member % 2 == 1)
    def _():
        across = (group, (member + 2) % 4)
        barrier = pltpu.get_barrier_semaphore()
        pl.semaphore_signal(barrier, inc=1, device_id=across, device_id_type=MESH)
        pl.semaphore_wait(barrier, 1)
        copies = [
            pltpu.make_async_remote_copy(src_ref=late_out.at[i, cut], dst_ref=late_in.at[i, cut], send_sem=send_sem.at[i],
                                         recv_sem=recv_sem.at[i], device_id=across, device_id_type=MESH)
            for i, cut in enumerate(late_cut(early, late_out.shape[1], i) for i in range(late_out.shape[0]))
        ]
        for copy in copies:
            copy.start()
        for copy in copies:
            copy.wait()


def patch_kernel(before_ref, late_ref, q_out, sems, *, early):
    member = lax.axis_index("tp")
    n_rows = late_ref.shape[1]

    @pl.when(member % 2 == 1)
    def _():
        base = ((member + 2) % 4) * n_rows
        copies = []
        for i in range(late_ref.shape[0]):
            cut = late_cut(early, n_rows, i)
            where = pl.ds(pl.multiple_of(base + cut.start, early), cut.size)
            copies.append(pltpu.make_async_copy(late_ref.at[i, cut], q_out.at[1 + i, where], sems.at[i]))
        for copy in copies:
            copy.start()
        for copy in copies:
            copy.wait()


def solution(mesh):
    def local_step(x_rows, norm_gain, w_q, w_k, w_v):
        n_rows, depth = x_rows.shape
        heads, width = w_q.shape[1:]
        share = w_k.shape[1]
        members = mesh.shape["tp"]
        pieces = FIRST_HEAD + heads
        all_rows = members * n_rows
        dma = pltpu.SemaphoreType.DMA
        norm_tile = n_rows // 4
        shift, lent, early = 72, 128, 512
        vmem = pl.BlockSpec(memory_space=pltpu.VMEM)
        results = tuple(jax.ShapeDtypeStruct((n, all_rows, width), jnp.bfloat16) for n in (heads, 1, 1))
        hbm = pl.BlockSpec(memory_space=pltpu.HBM)
        late_shape = jax.ShapeDtypeStruct((heads - 1, n_rows, width), jnp.bfloat16)
        q, k, v, late = pl.pallas_call(
            functools.partial(qkv_kernel, norm_tile=norm_tile, dot_tile=256, shift=shift, lent=lent, early=early),
            out_shape=results + (late_shape,),
            in_specs=[hbm] * 5,
            out_specs=(vmem,) * 4,
            scratch_shapes=[
                pltpu.VMEM((n_rows, depth), jnp.bfloat16),
                pltpu.VMEM((depth,), jnp.float32),
                pltpu.VMEM((4, heads, depth, width), jnp.bfloat16),
                pltpu.VMEM((2, 4 * share, depth), jnp.bfloat16),
                pltpu.VMEM((3, heads, n_rows, width), jnp.bfloat16),
                pltpu.VMEM((2, n_rows, width), jnp.bfloat16),
                dma((4,)), dma(()), dma((pieces + FIRST_HEAD,)),
                *[dma((pieces,)) for _ in range(10)],
                dma((3,)), dma((3,)), pltpu.SemaphoreType.REGULAR, pltpu.SemaphoreType.REGULAR,
                pltpu.VMEM((lent, width), jnp.bfloat16), dma((4,)), dma((2,)),
                dma((pieces,)), dma((pieces,)), dma((pieces,)), dma((pieces,)),
                dma((heads,)), dma((heads,)), dma((2,)), dma((2,)),
            ],
            compiler_params=pltpu.CompilerParams(collective_id=0, has_side_effects=True, vmem_limit_bytes=36 * 1024 * 1024),
            cost_estimate=pl.CostEstimate(flops=2 * n_rows * depth * 2048, bytes_accessed=16 * 1024 * 1024, transcendentals=0),
            name="qkv",
        )(*[pltpu.with_memory_space_constraint(a, pltpu.HBM) for a in (x_rows, norm_gain, w_q.transpose(1, 0, 2), w_k.T, w_v.T)])
        q, k, v = pl.pallas_call(
            functools.partial(finish_kernel, early=early),
            out_shape=results,
            in_specs=[vmem] * 3,
            out_specs=(hbm,) * 3,
            scratch_shapes=[dma((4 * (heads + 2) + 1,))],
            compiler_params=pltpu.CompilerParams(vmem_limit_bytes=16 * 1024 * 1024),
            name="finish",
        )(q, k, v)
        late = pl.pallas_call(
            functools.partial(late_kernel, early=early),
            out_shape=late_shape,
            in_specs=[hbm, vmem],
            out_specs=vmem,
            scratch_shapes=[dma((heads - 1,)), dma((heads - 1,))],
            compiler_params=pltpu.CompilerParams(collective_id=1, has_side_effects=True, vmem_limit_bytes=16 * 1024 * 1024),
            name="late",
        )(pltpu.with_memory_space_constraint(q, pltpu.HBM), late)
        q = pl.pallas_call(
            functools.partial(patch_kernel, early=early),
            out_shape=results[0],
            in_specs=[hbm, vmem],
            out_specs=hbm,
            scratch_shapes=[dma((heads - 1,))],
            input_output_aliases={0: 0},
            compiler_params=pltpu.CompilerParams(vmem_limit_bytes=16 * 1024 * 1024),
            name="patch",
        )(q, late)
        return q.transpose(1, 0, 2), k.transpose(1, 0, 2), v.transpose(1, 0, 2)

    return jax.shard_map(
        local_step, mesh=mesh,
        in_specs=(P(("dp", "tp"), None), P(None), P(None, "tp", None), P(None, "tp"), P(None, "tp")),
        out_specs=(P("dp", "tp", None), P("dp", "tp", None), P("dp", "tp", None)),
        check_vma=False,
    )
```

```python
import functools

import jax
import jax.numpy as jnp
from jax import lax
from jax.experimental import pallas as pl
from jax.experimental.pallas import tpu as pltpu
from jax.sharding import PartitionSpec as P

EPSILON = 1e-6
MESH = pl.DeviceIdType.MESH
LANES = 128
K_PIECE, V_PIECE, FIRST_HEAD = 0, 1, 2


def qkv_kernel(
    x_hbm, gain_hbm, wq_hbm, wk_hbm, wv_hbm,
    q_out, k_out, v_out, late_out,
    rows_buf, gain_buf, wq_buf, wkv_buf, q_stage, kv_stage,
    x_sem, gain_sem, load_sem,
    part_send, part_recv, link_send, link_recv, core_send, core_recv, side_send, side_recv, last_send, last_recv,
    middle_send, middle_recv, ready_sem, pair_sem, mate_sem, lent_buf, lent_sem, early_sem,
    near_send, near_recv, far_send, far_recv, cross_send, cross_recv, pass_send, pass_recv,
    *, norm_tile, dot_tile, shift, lent, early,
):
    n_rows, depth = rows_buf.shape
    heads = wq_hbm.shape[0]
    share = wk_hbm.shape[0]
    half = depth // 2
    pieces = FIRST_HEAD + heads

    group, member = lax.axis_index("dp"), lax.axis_index("tp")
    chip, core = member // 2, member % 2
    partner = (group, chip * 2 + (1 - core))
    across = (group, (1 - chip) * 2 + core)
    across_other = (group, (1 - chip) * 2 + (1 - core))
    beside = (1 - group, member)

    sources = [wk_hbm, wv_hbm] + [wq_hbm.at[h] for h in range(heads)]

    last_head = pieces - 1
    middle = pl.ds(half - shift, 2 * shift)

    def piece_at(j, slot, depth_half=None):
        if j < FIRST_HEAD:
            rows = pl.ds(pl.multiple_of(j * 2 * share + core * share, share), share)
            if depth_half is None:
                return wkv_buf.at[slot // 2, rows]
            return wkv_buf.at[slot // 2, rows, pl.ds(pl.multiple_of(depth_half * half, half), half)]
        if depth_half is None:
            return wq_buf.at[slot, j - FIRST_HEAD]
        if j == last_head:
            start = pl.multiple_of(depth_half * (half + shift), 8)
            return wq_buf.at[slot, j - FIRST_HEAD, pl.ds(start, half - shift)]
        return wq_buf.at[slot, j - FIRST_HEAD, pl.ds(pl.multiple_of(depth_half * half, half), half)]

    barrier = pltpu.get_barrier_semaphore()

    def signal(sem, device):
        pl.semaphore_signal(sem, inc=1, device_id=device, device_id_type=MESH)

    def when(condition, act):
        pl.when(condition)(act)

    signal(barrier, across)
    when(core == 1, lambda: signal(barrier, partner))
    when(group == 0, lambda: signal(barrier, beside))
    pl.semaphore_wait(barrier, 2 + group - core)

    loads = [pltpu.make_async_copy(sources[j], piece_at(j, 0), load_sem.at[j]) for j in range(pieces)]
    gain_load = pltpu.make_async_copy(gain_hbm, gain_buf, gain_sem)
    n_tiles = n_rows // norm_tile
    x_loads = [
        pltpu.make_async_copy(x_hbm.at[pl.ds(i * norm_tile, norm_tile)], rows_buf.at[pl.ds(i * norm_tile, norm_tile)], x_sem.at[i])
        for i in range(n_tiles)
    ]

    def remote(src, dst, send, recv, device):
        return pltpu.make_async_remote_copy(src_ref=src, dst_ref=dst, send_sem=send, recv_sem=recv, device_id=device, device_id_type=MESH)

    part, link, hand, side, last = [], [], [], [], []
    for j in range(pieces):
        part.append(remote(piece_at(j, 0), piece_at(j, 0 if j < FIRST_HEAD else 1), part_send.at[j], part_recv.at[j], partner))
        sent = sources[j].at[:, pl.ds(pl.multiple_of(group * half, half), half)] if j < FIRST_HEAD else piece_at(j, 0, group)
        link.append(remote(sent, piece_at(j, 2, group), link_send.at[j], link_recv.at[j], across))
        arrived, other_half = piece_at(j, 2, group), piece_at(j, 2, 1 - group)
        hand.append(remote(arrived, piece_at(j, 2 if j < FIRST_HEAD else 3, group), core_send.at[j], core_recv.at[j], partner))
        side.append(remote(arrived, arrived, side_send.at[j], side_recv.at[j], beside))
        last.append(remote(other_half, piece_at(j, 2 if j < FIRST_HEAD else 3, 1 - group), last_send.at[j], last_recv.at[j], partner))

    def middle_at(slot, part_of=None):
        if part_of is None:
            return wq_buf.at[slot, heads - 1, middle]
        return wq_buf.at[slot, heads - 1, pl.ds(pl.multiple_of(half - shift + part_of * shift, 8), shift)]

    def middle_copy(i, source_slot, slot, device, part_of=None):
        return remote(middle_at(source_slot, part_of), middle_at(slot, part_of), middle_send.at[i], middle_recv.at[i], device)

    middle_link = middle_copy(0, 0, 2, across)
    middle_side = middle_copy(1, 2, 2, beside)
    middle_hand = middle_copy(2, 2, 3, partner)
    half_link = middle_copy(3, 0, 2, across, group)
    half_side = middle_copy(4, 2, 2, beside, group)
    half_hand = middle_copy(5, 2, 3, partner, group)
    half_last = middle_copy(6, 2, 3, partner, 1 - group)

    my_rows = pl.ds(pl.multiple_of(member * n_rows, n_rows), n_rows)
    across_rows = pl.ds(pl.multiple_of(((1 - chip) * 2 + core) * n_rows, n_rows), n_rows)
    near = [remote(k_out.at[0, my_rows], k_out.at[0, my_rows], near_send.at[0], near_recv.at[0], partner),
            remote(v_out.at[0, my_rows], v_out.at[0, my_rows], near_send.at[1], near_recv.at[1], partner)]
    far = [remote(kv_stage.at[0], k_out.at[0, my_rows], far_send.at[0], far_recv.at[0], across),
           remote(kv_stage.at[1], v_out.at[0, my_rows], far_send.at[1], far_recv.at[1], across)]
    passed = [remote(k_out.at[0, across_rows], k_out.at[0, across_rows], pass_send.at[0], pass_recv.at[0], partner),
              remote(v_out.at[0, across_rows], v_out.at[0, across_rows], pass_send.at[1], pass_recv.at[1], partner)]
    cross = []
    for h in range(heads):
        near.append(remote(q_stage.at[0, h], q_out.at[h, my_rows], near_send.at[2 + h], near_recv.at[2 + h], partner))
        far.append(remote(q_stage.at[1, 0] if h == 0 else late_out.at[h - 1], q_out.at[h, my_rows], far_send.at[2 + h], far_recv.at[2 + h], across))
        cross.append(remote(q_stage.at[2, h], q_out.at[h, my_rows], cross_send.at[h], cross_recv.at[h], across_other))

    last_h = heads - 1
    lent_rows, kept_rows = pl.ds(0, lent), pl.ds(lent, n_rows - lent)
    my_kept = pl.ds(pl.multiple_of(member * n_rows + lent, lent), n_rows - lent)
    partner_lent = pl.ds(pl.multiple_of((chip * 2 + 1 - core) * n_rows, n_rows), lent)
    lend = remote(q_stage.at[2, last_h, lent_rows], lent_buf, lent_sem.at[0], lent_sem.at[1], partner)
    cross_kept = remote(q_stage.at[2, last_h, kept_rows], q_out.at[last_h, my_kept], cross_send.at[last_h], cross_recv.at[last_h], across_other)
    cross_lent = remote(lent_buf, q_out.at[last_h, partner_lent], lent_sem.at[2], lent_sem.at[3], across)
    my_early = pl.ds(pl.multiple_of(member * n_rows, n_rows), early)
    early_far = remote(late_out.at[0, pl.ds(0, early)], q_out.at[1, my_early], early_sem.at[0], early_sem.at[1], across)

    for j in range(FIRST_HEAD):
        link[j].start()
    for load in loads + [gain_load] + x_loads:
        load.start()

    when(core == 0, lambda: signal(mate_sem, partner))
    when(core == 1, lambda: pl.semaphore_wait(mate_sem, 1))
    signal(pair_sem, across)
    when(group == 1, lambda: signal(ready_sem, beside))
    pl.semaphore_wait(pair_sem, 1)
    for j in range(pieces):
        loads[j].wait()
        if j >= FIRST_HEAD:
            link[j].start()
    when(chip == 0, half_link.start)
    when((chip == 1) & (group == 1), middle_link.start)
    for copy in part:
        copy.start()

    chunks = depth // LANES
    sub = 64

    def norm_step(s, carry):
        here = pl.ds(pl.multiple_of(s * sub, sub), sub)
        total = jnp.zeros((sub, LANES), jnp.float32)
        for c in range(chunks):
            wide = rows_buf[here, c * LANES:(c + 1) * LANES].astype(jnp.float32)
            total = total + wide * wide
        scale = lax.rsqrt(jnp.sum(total, axis=-1, keepdims=True) / depth + EPSILON)
        for c in range(chunks):
            cols = slice(c * LANES, (c + 1) * LANES)
            wide = rows_buf[here, cols].astype(jnp.float32)
            rows_buf[here, cols] = (wide * scale * gain_buf[cols][None, :]).astype(jnp.bfloat16)
        return carry

    def normalize():
        gain_load.wait()
        for load in x_loads:
            load.wait()
        lax.fori_loop(0, n_rows // sub, norm_step, 0)

    def over_tiles(step):
        lax.fori_loop(0, n_rows // dot_tile, lambda i, carry: (step(i * dot_tile), carry)[1], 0)

    def q_block(slot, h, store):
        def step(start):
            tile = rows_buf[pl.ds(pl.multiple_of(start, dot_tile), dot_tile), :]
            store(start, jnp.dot(tile, wq_buf[slot, h], preferred_element_type=jnp.float32).astype(jnp.bfloat16))
        over_tiles(step)

    def kv_block(which, store):
        def step(start):
            tile = rows_buf[pl.ds(pl.multiple_of(start, dot_tile), dot_tile), :]
            both = lax.dot_general(tile, wkv_buf[which], (((1,), (1,)), ((), ())), preferred_element_type=jnp.float32)
            store(start, both.astype(jnp.bfloat16))
        over_tiles(step)

    def rows_at(start):
        return pl.ds(pl.multiple_of(start, dot_tile), dot_tile)

    def own_rows_at(start):
        return pl.ds(pl.multiple_of(member * n_rows + start, dot_tile), dot_tile)

    def own_q(h):
        def store(start, value):
            q_out[h, own_rows_at(start), :] = value
        q_block(0, h, store)

    def staged_q(stage, slot, h):
        def store(start, value):
            q_stage[stage, h, rows_at(start), :] = value
        q_block(slot, h, store)

    def late_q(h):
        def store(start, value):
            late_out[h - 1, rows_at(start), :] = value
        q_block(2, h, store)

    def own_kv():
        def store(start, value):
            k_out[0, own_rows_at(start), :] = value[:, :LANES]
            v_out[0, own_rows_at(start), :] = value[:, LANES:]
        kv_block(0, store)

    def far_kv():
        def store(start, value):
            kv_stage[0, rows_at(start), :] = value[:, :LANES]
            kv_stage[1, rows_at(start), :] = value[:, LANES:]
        kv_block(1, store)

    def from_link(j):
        link[j].wait_recv()
        side[j].start()
        hand[j].start()

    def from_side(j):
        side[j].wait_recv()
        last[j].start()

    def from_middle():
        @pl.when(chip == 0)
        def _():
            @pl.when(group == 1)
            def _():
                middle_link.wait_recv()
                middle_side.start()

            when(group == 0, middle_side.wait_recv)
            middle_hand.start()

        @pl.when(chip == 1)
        def _():
            half_link.wait_recv()
            half_side.start()
            half_hand.start()
            half_side.wait_recv()
            half_last.start()

    def complete_middle():
        when(chip == 0, middle_hand.wait_recv)

        @pl.when(chip == 1)
        def _():
            half_hand.wait_recv()
            half_last.wait_recv()

    def complete(j):
        hand[j].wait_recv()
        last[j].wait_recv()

    @pl.when(group == 0)
    def _():
        pl.semaphore_wait(ready_sem, 1)

    from_link(K_PIECE)
    normalize()
    from_link(V_PIECE)
    part[K_PIECE].wait_recv()
    part[V_PIECE].wait_recv()
    own_kv()
    from_side(K_PIECE)
    near[0].start()
    near[1].start()
    from_link(2)
    from_side(V_PIECE)
    complete(K_PIECE)
    complete(V_PIECE)
    far_kv()
    far[0].start()
    far[1].start()
    own_q(0)
    from_link(3)
    own_q(1)
    from_side(2)
    staged_q(1, 2, 0)
    from_link(4)
    complete(2)
    staged_q(2, 3, 0)

    @pl.when(core == 1)
    def _():
        far[FIRST_HEAD].start()

    from_side(3)
    complete(3)
    staged_q(2, 3, 1)
    cross[0].start()
    late_q(1)
    from_side(4)
    from_middle()
    cross[1].start()
    complete(4)
    complete_middle()
    staged_q(2, 3, 2)
    late_q(2)
    when(core == 0, lend.start)
    own_q(2)

    @pl.when(core == 1)
    def _():
        lend.wait_recv()
        cross_lent.start()
        early_far.start()
        cross[last_h].start()

    @pl.when(core == 0)
    def _():
        cross_kept.start()
        for copy in far[FIRST_HEAD:]:
            copy.start()

    for h in range(heads):
        part[FIRST_HEAD + h].wait_recv()
        staged_q(0, 1, h)
        if h:
            near[2 + h - 1].start()
    far[0].wait_recv()
    passed[0].start()
    far[1].wait_recv()
    passed[1].start()
    near[2 + heads - 1].start()

    for copy in part + link + hand + side + last:
        copy.wait_send()

    @pl.when(chip == 0)
    def _():
        half_link.wait_send()
        middle_hand.wait_send()
        when(group == 1, middle_side.wait_send)

    @pl.when(chip == 1)
    def _():
        when(group == 1, middle_link.wait_send)
        for copy in (half_side, half_hand, half_last):
            copy.wait_send()

    for copy in near + passed + cross[:last_h]:
        copy.wait()
    for copy in far[:FIRST_HEAD]:
        copy.wait_send()
    far[FIRST_HEAD].wait()

    @pl.when(core == 0)
    def _():
        for copy in far[FIRST_HEAD + 1:]:
            copy.wait()
        lend.wait_send()
        cross_kept.wait_send()
        cross[last_h].wait_recv()

    @pl.when(core == 1)
    def _():
        cross[last_h].wait_send()
        early_far.wait()
        cross_lent.wait()
        cross_kept.wait_recv()


def finish_kernel(q_ref, k_ref, v_ref, q_out, k_out, v_out, sems, *, early):
    member = lax.axis_index("tp")
    chip, core = member // 2, member % 2
    n_rows = q_ref.shape[1] // 4
    here, there = [], []
    for ref, out in ((q_ref, q_out), (k_ref, k_out), (v_ref, v_out)):
        for h in range(ref.shape[0]):
            for cut in range(4):
                where = pl.ds(pl.multiple_of(((3 - 2 * chip + cut + 1) % 4) * n_rows, n_rows), n_rows)
                copy = pltpu.make_async_copy(ref.at[h, where], out.at[h, where], sems.at[len(here) + len(there)])
                (there if cut == 3 and ref is q_ref and h else here).append(copy)

    for copy in here:
        copy.start()

    early_rows = pl.ds(pl.multiple_of((3 - 2 * chip) * n_rows, n_rows), early)
    early_copy = pltpu.make_async_copy(q_ref.at[1, early_rows], q_out.at[1, early_rows], sems.at[len(here) + len(there)])

    @pl.when(core == 1)
    def _():
        early_copy.start()

    @pl.when(core == 0)
    def _():
        for copy in there:
            copy.start()

    for copy in here:
        copy.wait()

    @pl.when(core == 1)
    def _():
        early_copy.wait()

    @pl.when(core == 0)
    def _():
        for copy in there:
            copy.wait()


def late_cut(early, n_rows, i):
    return pl.ds(early, n_rows - early) if i == 0 else pl.ds(0, n_rows)


def late_kernel(after_ref, late_out, late_in, send_sem, recv_sem, *, early):
    group, member = lax.axis_index("dp"), lax.axis_index("tp")

    @pl.when(member % 2 == 1)
    def _():
        across = (group, (member + 2) % 4)
        barrier = pltpu.get_barrier_semaphore()
        pl.semaphore_signal(barrier, inc=1, device_id=across, device_id_type=MESH)
        pl.semaphore_wait(barrier, 1)
        copies = [
            pltpu.make_async_remote_copy(src_ref=late_out.at[i, cut], dst_ref=late_in.at[i, cut], send_sem=send_sem.at[i],
                                         recv_sem=recv_sem.at[i], device_id=across, device_id_type=MESH)
            for i, cut in enumerate(late_cut(early, late_out.shape[1], i) for i in range(late_out.shape[0]))
        ]
        for copy in copies:
            copy.start()
        for copy in copies:
            copy.wait()


def patch_kernel(before_ref, late_ref, q_out, sems, *, early):
    member = lax.axis_index("tp")
    n_rows = late_ref.shape[1]

    @pl.when(member % 2 == 1)
    def _():
        base = ((member + 2) % 4) * n_rows
        copies = []
        for i in range(late_ref.shape[0]):
            cut = late_cut(early, n_rows, i)
            where = pl.ds(pl.multiple_of(base + cut.start, early), cut.size)
            copies.append(pltpu.make_async_copy(late_ref.at[i, cut], q_out.at[1 + i, where], sems.at[i]))
        for copy in copies:
            copy.start()
        for copy in copies:
            copy.wait()


def solution(mesh):
    def local_step(x_rows, norm_gain, w_q, w_k, w_v):
        n_rows, depth = x_rows.shape
        heads, width = w_q.shape[1:]
        share = w_k.shape[1]
        members = mesh.shape["tp"]
        pieces = FIRST_HEAD + heads
        all_rows = members * n_rows
        dma = pltpu.SemaphoreType.DMA
        norm_tile = n_rows // 4
        shift, lent, early = 56, 128, 512
        vmem = pl.BlockSpec(memory_space=pltpu.VMEM)
        results = tuple(jax.ShapeDtypeStruct((n, all_rows, width), jnp.bfloat16) for n in (heads, 1, 1))
        hbm = pl.BlockSpec(memory_space=pltpu.HBM)
        late_shape = jax.ShapeDtypeStruct((heads - 1, n_rows, width), jnp.bfloat16)
        q, k, v, late = pl.pallas_call(
            functools.partial(qkv_kernel, norm_tile=norm_tile, dot_tile=256, shift=shift, lent=lent, early=early),
            out_shape=results + (late_shape,),
            in_specs=[hbm] * 5,
            out_specs=(vmem,) * 4,
            scratch_shapes=[
                pltpu.VMEM((n_rows, depth), jnp.bfloat16),
                pltpu.VMEM((depth,), jnp.float32),
                pltpu.VMEM((4, heads, depth, width), jnp.bfloat16),
                pltpu.VMEM((2, 4 * share, depth), jnp.bfloat16),
                pltpu.VMEM((3, heads, n_rows, width), jnp.bfloat16),
                pltpu.VMEM((2, n_rows, width), jnp.bfloat16),
                dma((4,)), dma(()), dma((pieces,)),
                *[dma((pieces,)) for _ in range(10)],
                dma((7,)), dma((7,)), pltpu.SemaphoreType.REGULAR, pltpu.SemaphoreType.REGULAR, pltpu.SemaphoreType.REGULAR,
                pltpu.VMEM((lent, width), jnp.bfloat16), dma((4,)), dma((2,)),
                dma((pieces,)), dma((pieces,)), dma((pieces,)), dma((pieces,)),
                dma((heads,)), dma((heads,)), dma((2,)), dma((2,)),
            ],
            compiler_params=pltpu.CompilerParams(collective_id=0, has_side_effects=True, vmem_limit_bytes=36 * 1024 * 1024),
            cost_estimate=pl.CostEstimate(flops=2 * n_rows * depth * 2048, bytes_accessed=16 * 1024 * 1024, transcendentals=0),
            name="qkv",
        )(*[pltpu.with_memory_space_constraint(a, pltpu.HBM) for a in (x_rows, norm_gain, w_q.transpose(1, 0, 2), w_k.T, w_v.T)])
        q, k, v = pl.pallas_call(
            functools.partial(finish_kernel, early=early),
            out_shape=results,
            in_specs=[vmem] * 3,
            out_specs=(hbm,) * 3,
            scratch_shapes=[dma((4 * (heads + 2) + 1,))],
            compiler_params=pltpu.CompilerParams(vmem_limit_bytes=16 * 1024 * 1024),
            name="finish",
        )(q, k, v)
        late = pl.pallas_call(
            functools.partial(late_kernel, early=early),
            out_shape=late_shape,
            in_specs=[hbm, vmem],
            out_specs=vmem,
            scratch_shapes=[dma((heads - 1,)), dma((heads - 1,))],
            compiler_params=pltpu.CompilerParams(collective_id=1, has_side_effects=True, vmem_limit_bytes=16 * 1024 * 1024),
            name="late",
        )(pltpu.with_memory_space_constraint(q, pltpu.HBM), late)
        q = pl.pallas_call(
            functools.partial(patch_kernel, early=early),
            out_shape=results[0],
            in_specs=[hbm, vmem],
            out_specs=hbm,
            scratch_shapes=[dma((heads - 1,))],
            input_output_aliases={0: 0},
            compiler_params=pltpu.CompilerParams(vmem_limit_bytes=16 * 1024 * 1024),
            name="patch",
        )(q, late)
        return q.transpose(1, 0, 2), k.transpose(1, 0, 2), v.transpose(1, 0, 2)

    return jax.shard_map(
        local_step, mesh=mesh,
        in_specs=(P(("dp", "tp"), None), P(None), P(None, "tp", None), P(None, "tp"), P(None, "tp")),
        out_specs=(P("dp", "tp", None), P("dp", "tp", None), P("dp", "tp", None)),
        check_vma=False,
    )
```

```python
import functools

import jax
import jax.numpy as jnp
from jax import lax
from jax.experimental import pallas as pl
from jax.experimental.pallas import tpu as pltpu
from jax.sharding import PartitionSpec as P

EPSILON = 1e-6
MESH = pl.DeviceIdType.MESH
LANES = 128
K_PIECE, V_PIECE, FIRST_HEAD = 0, 1, 2


def qkv_kernel(
    x_hbm, gain_hbm, wq_hbm, wk_hbm, wv_hbm,
    q_out, k_out, v_out, late_out,
    rows_buf, gain_buf, wq_buf, wkv_buf, q_stage, kv_stage,
    x_sem, gain_sem, load_sem,
    part_send, part_recv, link_send, link_recv, core_send, core_recv, side_send, side_recv, last_send, last_recv,
    middle_send, middle_recv, ready_sem, pair_sem, mate_sem, lent_buf, lent_sem, early_sem,
    near_send, near_recv, far_send, far_recv, cross_send, cross_recv, pass_send, pass_recv,
    *, norm_tile, dot_tile, shift, lent, early,
):
    n_rows, depth = rows_buf.shape
    heads = wq_hbm.shape[0]
    share = wk_hbm.shape[0]
    half = depth // 2
    pieces = FIRST_HEAD + heads

    group, member = lax.axis_index("dp"), lax.axis_index("tp")
    chip, core = member // 2, member % 2
    partner = (group, chip * 2 + (1 - core))
    across = (group, (1 - chip) * 2 + core)
    across_other = (group, (1 - chip) * 2 + (1 - core))
    beside = (1 - group, member)

    sources = [wk_hbm, wv_hbm] + [wq_hbm.at[h] for h in range(heads)]

    last_head = pieces - 1
    middle = pl.ds(half - shift, 2 * shift)

    def piece_at(j, slot, depth_half=None):
        if j < FIRST_HEAD:
            rows = pl.ds(pl.multiple_of(j * 2 * share + core * share, share), share)
            if depth_half is None:
                return wkv_buf.at[slot // 2, rows]
            return wkv_buf.at[slot // 2, rows, pl.ds(pl.multiple_of(depth_half * half, half), half)]
        if depth_half is None:
            return wq_buf.at[slot, j - FIRST_HEAD]
        if j == last_head:
            start = pl.multiple_of(depth_half * (half + shift), 8)
            return wq_buf.at[slot, j - FIRST_HEAD, pl.ds(start, half - shift)]
        return wq_buf.at[slot, j - FIRST_HEAD, pl.ds(pl.multiple_of(depth_half * half, half), half)]

    barrier = pltpu.get_barrier_semaphore()

    def signal(sem, device):
        pl.semaphore_signal(sem, inc=1, device_id=device, device_id_type=MESH)

    def when(condition, act):
        pl.when(condition)(act)

    signal(barrier, across)
    when(core == 1, lambda: signal(barrier, partner))
    when(group == 0, lambda: signal(barrier, beside))
    pl.semaphore_wait(barrier, 2 + group - core)

    loads = [pltpu.make_async_copy(sources[j], piece_at(j, 0), load_sem.at[j]) for j in range(pieces)]
    gain_load = pltpu.make_async_copy(gain_hbm, gain_buf, gain_sem)
    n_tiles = n_rows // norm_tile
    x_loads = [
        pltpu.make_async_copy(x_hbm.at[pl.ds(i * norm_tile, norm_tile)], rows_buf.at[pl.ds(i * norm_tile, norm_tile)], x_sem.at[i])
        for i in range(n_tiles)
    ]

    def remote(src, dst, send, recv, device):
        return pltpu.make_async_remote_copy(src_ref=src, dst_ref=dst, send_sem=send, recv_sem=recv, device_id=device, device_id_type=MESH)

    part, link, hand, side, last = [], [], [], [], []
    for j in range(pieces):
        part.append(remote(piece_at(j, 0), piece_at(j, 0 if j < FIRST_HEAD else 1), part_send.at[j], part_recv.at[j], partner))
        sent = sources[j].at[:, pl.ds(pl.multiple_of(group * half, half), half)] if j < FIRST_HEAD else piece_at(j, 0, group)
        link.append(remote(sent, piece_at(j, 2, group), link_send.at[j], link_recv.at[j], across))
        arrived, other_half = piece_at(j, 2, group), piece_at(j, 2, 1 - group)
        hand.append(remote(arrived, piece_at(j, 2 if j < FIRST_HEAD else 3, group), core_send.at[j], core_recv.at[j], partner))
        side.append(remote(arrived, arrived, side_send.at[j], side_recv.at[j], beside))
        last.append(remote(other_half, piece_at(j, 2 if j < FIRST_HEAD else 3, 1 - group), last_send.at[j], last_recv.at[j], partner))

    def middle_at(slot, part_of=None):
        if part_of is None:
            return wq_buf.at[slot, heads - 1, middle]
        return wq_buf.at[slot, heads - 1, pl.ds(pl.multiple_of(half - shift + part_of * shift, 8), shift)]

    def middle_copy(i, source_slot, slot, device, part_of=None):
        return remote(middle_at(source_slot, part_of), middle_at(slot, part_of), middle_send.at[i], middle_recv.at[i], device)

    middle_link = middle_copy(0, 0, 2, across)
    middle_side = middle_copy(1, 2, 2, beside)
    middle_hand = middle_copy(2, 2, 3, partner)
    half_link = middle_copy(3, 0, 2, across, group)
    half_side = middle_copy(4, 2, 2, beside, group)
    half_hand = middle_copy(5, 2, 3, partner, group)
    half_last = middle_copy(6, 2, 3, partner, 1 - group)

    my_rows = pl.ds(pl.multiple_of(member * n_rows, n_rows), n_rows)
    across_rows = pl.ds(pl.multiple_of(((1 - chip) * 2 + core) * n_rows, n_rows), n_rows)
    near = [remote(k_out.at[0, my_rows], k_out.at[0, my_rows], near_send.at[0], near_recv.at[0], partner),
            remote(v_out.at[0, my_rows], v_out.at[0, my_rows], near_send.at[1], near_recv.at[1], partner)]
    far = [remote(kv_stage.at[0], k_out.at[0, my_rows], far_send.at[0], far_recv.at[0], across),
           remote(kv_stage.at[1], v_out.at[0, my_rows], far_send.at[1], far_recv.at[1], across)]
    passed = [remote(k_out.at[0, across_rows], k_out.at[0, across_rows], pass_send.at[0], pass_recv.at[0], partner),
              remote(v_out.at[0, across_rows], v_out.at[0, across_rows], pass_send.at[1], pass_recv.at[1], partner)]
    cross = []
    for h in range(heads):
        near.append(remote(q_stage.at[0, h], q_out.at[h, my_rows], near_send.at[2 + h], near_recv.at[2 + h], partner))
        far.append(remote(q_stage.at[1, 0] if h == 0 else late_out.at[h - 1], q_out.at[h, my_rows], far_send.at[2 + h], far_recv.at[2 + h], across))
        cross.append(remote(q_stage.at[2, h], q_out.at[h, my_rows], cross_send.at[h], cross_recv.at[h], across_other))

    last_h = heads - 1
    lent_rows, kept_rows = pl.ds(0, lent), pl.ds(lent, n_rows - lent)
    my_kept = pl.ds(pl.multiple_of(member * n_rows + lent, lent), n_rows - lent)
    partner_lent = pl.ds(pl.multiple_of((chip * 2 + 1 - core) * n_rows, n_rows), lent)
    lend = remote(q_stage.at[2, last_h, lent_rows], lent_buf, lent_sem.at[0], lent_sem.at[1], partner)
    cross_kept = remote(q_stage.at[2, last_h, kept_rows], q_out.at[last_h, my_kept], cross_send.at[last_h], cross_recv.at[last_h], across_other)
    cross_lent = remote(lent_buf, q_out.at[last_h, partner_lent], lent_sem.at[2], lent_sem.at[3], across)
    my_early = pl.ds(pl.multiple_of(member * n_rows, n_rows), early)
    early_far = remote(late_out.at[0, pl.ds(0, early)], q_out.at[1, my_early], early_sem.at[0], early_sem.at[1], across)

    for j in range(FIRST_HEAD):
        link[j].start()
    for load in loads + [gain_load] + x_loads:
        load.start()

    when(core == 0, lambda: signal(mate_sem, partner))
    when(core == 1, lambda: pl.semaphore_wait(mate_sem, 1))
    signal(pair_sem, across)
    when(group == 1, lambda: signal(ready_sem, beside))
    pl.semaphore_wait(pair_sem, 1)
    for j in range(pieces):
        loads[j].wait()
        if j >= FIRST_HEAD:
            link[j].start()
    when(chip == 0, half_link.start)
    when((chip == 1) & (group == 1), middle_link.start)
    for copy in part:
        copy.start()

    chunks = depth // LANES
    sub = 64

    def norm_step(s, carry):
        here = pl.ds(pl.multiple_of(s * sub, sub), sub)
        total = jnp.zeros((sub, LANES), jnp.float32)
        for c in range(chunks):
            wide = rows_buf[here, c * LANES:(c + 1) * LANES].astype(jnp.float32)
            total = total + wide * wide
        scale = lax.rsqrt(jnp.sum(total, axis=-1, keepdims=True) / depth + EPSILON)
        for c in range(chunks):
            cols = slice(c * LANES, (c + 1) * LANES)
            wide = rows_buf[here, cols].astype(jnp.float32)
            rows_buf[here, cols] = (wide * scale * gain_buf[cols][None, :]).astype(jnp.bfloat16)
        return carry

    def normalize():
        gain_load.wait()
        for load in x_loads:
            load.wait()
        lax.fori_loop(0, n_rows // sub, norm_step, 0)

    def over_tiles(step):
        lax.fori_loop(0, n_rows // dot_tile, lambda i, carry: (step(i * dot_tile), carry)[1], 0)

    def q_block(slot, h, store):
        def step(start):
            tile = rows_buf[pl.ds(pl.multiple_of(start, dot_tile), dot_tile), :]
            store(start, jnp.dot(tile, wq_buf[slot, h], preferred_element_type=jnp.float32).astype(jnp.bfloat16))
        over_tiles(step)

    def kv_block(which, store):
        def step(start):
            tile = rows_buf[pl.ds(pl.multiple_of(start, dot_tile), dot_tile), :]
            both = lax.dot_general(tile, wkv_buf[which], (((1,), (1,)), ((), ())), preferred_element_type=jnp.float32)
            store(start, both.astype(jnp.bfloat16))
        over_tiles(step)

    def rows_at(start):
        return pl.ds(pl.multiple_of(start, dot_tile), dot_tile)

    def own_rows_at(start):
        return pl.ds(pl.multiple_of(member * n_rows + start, dot_tile), dot_tile)

    def own_q(h):
        def store(start, value):
            q_out[h, own_rows_at(start), :] = value
        q_block(0, h, store)

    def staged_q(stage, slot, h):
        def store(start, value):
            q_stage[stage, h, rows_at(start), :] = value
        q_block(slot, h, store)

    def late_q(h):
        def store(start, value):
            late_out[h - 1, rows_at(start), :] = value
        q_block(2, h, store)

    def own_kv():
        def store(start, value):
            k_out[0, own_rows_at(start), :] = value[:, :LANES]
            v_out[0, own_rows_at(start), :] = value[:, LANES:]
        kv_block(0, store)

    def far_kv():
        def store(start, value):
            kv_stage[0, rows_at(start), :] = value[:, :LANES]
            kv_stage[1, rows_at(start), :] = value[:, LANES:]
        kv_block(1, store)

    def from_link(j):
        link[j].wait_recv()
        side[j].start()
        hand[j].start()

    def from_side(j):
        side[j].wait_recv()
        last[j].start()

    def from_middle():
        @pl.when(chip == 0)
        def _():
            @pl.when(group == 1)
            def _():
                middle_link.wait_recv()
                middle_side.start()

            when(group == 0, middle_side.wait_recv)
            middle_hand.start()

        @pl.when(chip == 1)
        def _():
            half_link.wait_recv()
            half_side.start()
            half_hand.start()
            half_side.wait_recv()
            half_last.start()

    def complete_middle():
        when(chip == 0, middle_hand.wait_recv)

        @pl.when(chip == 1)
        def _():
            half_hand.wait_recv()
            half_last.wait_recv()

    def complete(j):
        hand[j].wait_recv()
        last[j].wait_recv()

    @pl.when(group == 0)
    def _():
        pl.semaphore_wait(ready_sem, 1)

    from_link(K_PIECE)
    normalize()
    from_link(V_PIECE)
    part[K_PIECE].wait_recv()
    part[V_PIECE].wait_recv()
    own_kv()
    from_side(K_PIECE)
    near[0].start()
    near[1].start()
    from_link(2)
    from_side(V_PIECE)
    complete(K_PIECE)
    complete(V_PIECE)
    far_kv()
    far[0].start()
    far[1].start()
    own_q(0)
    from_link(3)
    own_q(1)
    from_side(2)
    staged_q(1, 2, 0)
    from_link(4)
    complete(2)
    staged_q(2, 3, 0)

    @pl.when(core == 1)
    def _():
        far[FIRST_HEAD].start()

    from_side(3)
    complete(3)
    staged_q(2, 3, 1)
    cross[0].start()
    late_q(1)
    from_side(4)
    from_middle()
    cross[1].start()
    complete(4)
    complete_middle()
    staged_q(2, 3, 2)
    late_q(2)
    when(core == 0, lend.start)
    own_q(2)

    @pl.when(core == 1)
    def _():
        lend.wait_recv()
        cross_lent.start()
        early_far.start()
        cross[last_h].start()

    @pl.when(core == 0)
    def _():
        cross_kept.start()
        for copy in far[FIRST_HEAD:]:
            copy.start()

    for h in range(heads):
        part[FIRST_HEAD + h].wait_recv()
        staged_q(0, 1, h)
        if h:
            near[2 + h - 1].start()
    far[0].wait_recv()
    passed[0].start()
    far[1].wait_recv()
    passed[1].start()
    near[2 + heads - 1].start()

    for copy in part + link + hand + side + last:
        copy.wait_send()

    @pl.when(chip == 0)
    def _():
        half_link.wait_send()
        middle_hand.wait_send()
        when(group == 1, middle_side.wait_send)

    @pl.when(chip == 1)
    def _():
        when(group == 1, middle_link.wait_send)
        for copy in (half_side, half_hand, half_last):
            copy.wait_send()

    for copy in near + passed + cross[:last_h]:
        copy.wait()
    for copy in far[:FIRST_HEAD]:
        copy.wait_send()
    far[FIRST_HEAD].wait()

    @pl.when(core == 0)
    def _():
        for copy in far[FIRST_HEAD + 1:]:
            copy.wait()
        lend.wait_send()
        cross_kept.wait_send()
        cross[last_h].wait_recv()

    @pl.when(core == 1)
    def _():
        cross[last_h].wait_send()
        early_far.wait()
        cross_lent.wait()
        cross_kept.wait_recv()


def finish_kernel(q_ref, k_ref, v_ref, q_out, k_out, v_out, sems, *, early):
    member = lax.axis_index("tp")
    chip, core = member // 2, member % 2
    n_rows = q_ref.shape[1] // 4
    here, there = [], []
    for ref, out in ((q_ref, q_out), (k_ref, k_out), (v_ref, v_out)):
        for h in range(ref.shape[0]):
            for cut in range(4):
                where = pl.ds(pl.multiple_of(((3 - 2 * chip + cut + 1) % 4) * n_rows, n_rows), n_rows)
                copy = pltpu.make_async_copy(ref.at[h, where], out.at[h, where], sems.at[len(here) + len(there)])
                (there if cut == 3 and ref is q_ref and h else here).append(copy)

    for copy in here:
        copy.start()

    early_rows = pl.ds(pl.multiple_of((3 - 2 * chip) * n_rows, n_rows), early)
    early_copy = pltpu.make_async_copy(q_ref.at[1, early_rows], q_out.at[1, early_rows], sems.at[len(here) + len(there)])

    @pl.when(core == 1)
    def _():
        early_copy.start()

    @pl.when(core == 0)
    def _():
        for copy in there:
            copy.start()

    for copy in here:
        copy.wait()

    @pl.when(core == 1)
    def _():
        early_copy.wait()

    @pl.when(core == 0)
    def _():
        for copy in there:
            copy.wait()


def late_cut(early, n_rows, i):
    return pl.ds(early, n_rows - early) if i == 0 else pl.ds(0, n_rows)


def late_kernel(after_ref, late_out, late_in, send_sem, recv_sem, *, early):
    group, member = lax.axis_index("dp"), lax.axis_index("tp")

    @pl.when(member % 2 == 1)
    def _():
        across = (group, (member + 2) % 4)
        barrier = pltpu.get_barrier_semaphore()
        pl.semaphore_signal(barrier, inc=1, device_id=across, device_id_type=MESH)
        pl.semaphore_wait(barrier, 1)
        copies = [
            pltpu.make_async_remote_copy(src_ref=late_out.at[i, cut], dst_ref=late_in.at[i, cut], send_sem=send_sem.at[i],
                                         recv_sem=recv_sem.at[i], device_id=across, device_id_type=MESH)
            for i, cut in enumerate(late_cut(early, late_out.shape[1], i) for i in range(late_out.shape[0]))
        ]
        for copy in copies:
            copy.start()
        for copy in copies:
            copy.wait()


def patch_kernel(before_ref, late_ref, q_out, sems, *, early):
    member = lax.axis_index("tp")
    n_rows = late_ref.shape[1]

    @pl.when(member % 2 == 1)
    def _():
        base = ((member + 2) % 4) * n_rows
        copies = []
        for i in range(late_ref.shape[0]):
            cut = late_cut(early, n_rows, i)
            where = pl.ds(pl.multiple_of(base + cut.start, early), cut.size)
            copies.append(pltpu.make_async_copy(late_ref.at[i, cut], q_out.at[1 + i, where], sems.at[i]))
        for copy in copies:
            copy.start()
        for copy in copies:
            copy.wait()


def solution(mesh):
    def local_step(x_rows, norm_gain, w_q, w_k, w_v):
        n_rows, depth = x_rows.shape
        heads, width = w_q.shape[1:]
        share = w_k.shape[1]
        members = mesh.shape["tp"]
        pieces = FIRST_HEAD + heads
        all_rows = members * n_rows
        dma = pltpu.SemaphoreType.DMA
        norm_tile = n_rows // 4
        shift, lent, early = 56, 128, 256
        vmem = pl.BlockSpec(memory_space=pltpu.VMEM)
        results = tuple(jax.ShapeDtypeStruct((n, all_rows, width), jnp.bfloat16) for n in (heads, 1, 1))
        hbm = pl.BlockSpec(memory_space=pltpu.HBM)
        late_shape = jax.ShapeDtypeStruct((heads - 1, n_rows, width), jnp.bfloat16)
        q, k, v, late = pl.pallas_call(
            functools.partial(qkv_kernel, norm_tile=norm_tile, dot_tile=256, shift=shift, lent=lent, early=early),
            out_shape=results + (late_shape,),
            in_specs=[hbm] * 5,
            out_specs=(vmem,) * 4,
            scratch_shapes=[
                pltpu.VMEM((n_rows, depth), jnp.bfloat16),
                pltpu.VMEM((depth,), jnp.float32),
                pltpu.VMEM((4, heads, depth, width), jnp.bfloat16),
                pltpu.VMEM((2, 4 * share, depth), jnp.bfloat16),
                pltpu.VMEM((3, heads, n_rows, width), jnp.bfloat16),
                pltpu.VMEM((2, n_rows, width), jnp.bfloat16),
                dma((4,)), dma(()), dma((pieces,)),
                *[dma((pieces,)) for _ in range(10)],
                dma((7,)), dma((7,)), pltpu.SemaphoreType.REGULAR, pltpu.SemaphoreType.REGULAR, pltpu.SemaphoreType.REGULAR,
                pltpu.VMEM((lent, width), jnp.bfloat16), dma((4,)), dma((2,)),
                dma((pieces,)), dma((pieces,)), dma((pieces,)), dma((pieces,)),
                dma((heads,)), dma((heads,)), dma((2,)), dma((2,)),
            ],
            compiler_params=pltpu.CompilerParams(collective_id=0, has_side_effects=True, vmem_limit_bytes=36 * 1024 * 1024),
            cost_estimate=pl.CostEstimate(flops=2 * n_rows * depth * 2048, bytes_accessed=16 * 1024 * 1024, transcendentals=0),
            name="qkv",
        )(*[pltpu.with_memory_space_constraint(a, pltpu.HBM) for a in (x_rows, norm_gain, w_q.transpose(1, 0, 2), w_k.T, w_v.T)])
        q, k, v = pl.pallas_call(
            functools.partial(finish_kernel, early=early),
            out_shape=results,
            in_specs=[vmem] * 3,
            out_specs=(hbm,) * 3,
            scratch_shapes=[dma((4 * (heads + 2) + 1,))],
            compiler_params=pltpu.CompilerParams(vmem_limit_bytes=16 * 1024 * 1024),
            name="finish",
        )(q, k, v)
        late = pl.pallas_call(
            functools.partial(late_kernel, early=early),
            out_shape=late_shape,
            in_specs=[hbm, vmem],
            out_specs=vmem,
            scratch_shapes=[dma((heads - 1,)), dma((heads - 1,))],
            compiler_params=pltpu.CompilerParams(collective_id=1, has_side_effects=True, vmem_limit_bytes=16 * 1024 * 1024),
            name="late",
        )(pltpu.with_memory_space_constraint(q, pltpu.HBM), late)
        q = pl.pallas_call(
            functools.partial(patch_kernel, early=early),
            out_shape=results[0],
            in_specs=[hbm, vmem],
            out_specs=hbm,
            scratch_shapes=[dma((heads - 1,))],
            input_output_aliases={0: 0},
            compiler_params=pltpu.CompilerParams(vmem_limit_bytes=16 * 1024 * 1024),
            name="patch",
        )(q, late)
        return q.transpose(1, 0, 2), k.transpose(1, 0, 2), v.transpose(1, 0, 2)

    return jax.shard_map(
        local_step, mesh=mesh,
        in_specs=(P(("dp", "tp"), None), P(None), P(None, "tp", None), P(None, "tp"), P(None, "tp")),
        out_specs=(P("dp", "tp", None), P("dp", "tp", None), P("dp", "tp", None)),
        check_vma=False,
    )
```

```python
import functools

import jax
import jax.numpy as jnp
from jax import lax
from jax.experimental import pallas as pl
from jax.experimental.pallas import tpu as pltpu
from jax.sharding import PartitionSpec as P

EPSILON = 1e-6
MESH = pl.DeviceIdType.MESH
LANES = 128
K_PIECE, V_PIECE, FIRST_HEAD = 0, 1, 2


def qkv_kernel(
    x_hbm, gain_hbm, wq_hbm, wk_hbm, wv_hbm,
    q_out, k_out, v_out, late_out,
    rows_buf, gain_buf, wq_buf, wkv_buf, q_stage, kv_stage,
    x_sem, gain_sem, load_sem,
    part_send, part_recv, link_send, link_recv, core_send, core_recv, side_send, side_recv, last_send, last_recv,
    middle_send, middle_recv, ready_sem, pair_sem, mate_sem, lent_buf, lent_sem, early_sem,
    near_send, near_recv, far_send, far_recv, cross_send, cross_recv, pass_send, pass_recv,
    *, norm_tile, dot_tile, shift, lent, early,
):
    n_rows, depth = rows_buf.shape
    heads = wq_hbm.shape[0]
    share = wk_hbm.shape[0]
    half = depth // 2
    pieces = FIRST_HEAD + heads

    group, member = lax.axis_index("dp"), lax.axis_index("tp")
    chip, core = member // 2, member % 2
    partner = (group, chip * 2 + (1 - core))
    across = (group, (1 - chip) * 2 + core)
    across_other = (group, (1 - chip) * 2 + (1 - core))
    beside = (1 - group, member)

    sources = [wk_hbm, wv_hbm] + [wq_hbm.at[h] for h in range(heads)]

    last_head = pieces - 1
    middle = pl.ds(half - shift, 2 * shift)

    def piece_at(j, slot, depth_half=None):
        if j < FIRST_HEAD:
            rows = pl.ds(pl.multiple_of(j * 2 * share + core * share, share), share)
            if depth_half is None:
                return wkv_buf.at[slot // 2, rows]
            return wkv_buf.at[slot // 2, rows, pl.ds(pl.multiple_of(depth_half * half, half), half)]
        if depth_half is None:
            return wq_buf.at[slot, j - FIRST_HEAD]
        if j == last_head:
            start = pl.multiple_of(depth_half * (half + shift), 8)
            return wq_buf.at[slot, j - FIRST_HEAD, pl.ds(start, half - shift)]
        return wq_buf.at[slot, j - FIRST_HEAD, pl.ds(pl.multiple_of(depth_half * half, half), half)]

    barrier = pltpu.get_barrier_semaphore()

    def signal(sem, device):
        pl.semaphore_signal(sem, inc=1, device_id=device, device_id_type=MESH)

    def when(condition, act):
        pl.when(condition)(act)

    signal(barrier, across)
    when(core == 1, lambda: signal(barrier, partner))
    when(group == 0, lambda: signal(barrier, beside))
    pl.semaphore_wait(barrier, 2 + group - core)

    loads = [pltpu.make_async_copy(sources[j], piece_at(j, 0), load_sem.at[j]) for j in range(pieces)]
    gain_load = pltpu.make_async_copy(gain_hbm, gain_buf, gain_sem)
    n_tiles = n_rows // norm_tile
    x_loads = [
        pltpu.make_async_copy(x_hbm.at[pl.ds(i * norm_tile, norm_tile)], rows_buf.at[pl.ds(i * norm_tile, norm_tile)], x_sem.at[i])
        for i in range(n_tiles)
    ]

    def remote(src, dst, send, recv, device):
        return pltpu.make_async_remote_copy(src_ref=src, dst_ref=dst, send_sem=send, recv_sem=recv, device_id=device, device_id_type=MESH)

    part, link, hand, side, last = [], [], [], [], []
    for j in range(pieces):
        part.append(remote(piece_at(j, 0), piece_at(j, 0 if j < FIRST_HEAD else 1), part_send.at[j], part_recv.at[j], partner))
        sent = sources[j].at[:, pl.ds(pl.multiple_of(group * half, half), half)] if j < FIRST_HEAD else piece_at(j, 0, group)
        link.append(remote(sent, piece_at(j, 2, group), link_send.at[j], link_recv.at[j], across))
        arrived, other_half = piece_at(j, 2, group), piece_at(j, 2, 1 - group)
        hand.append(remote(arrived, piece_at(j, 2 if j < FIRST_HEAD else 3, group), core_send.at[j], core_recv.at[j], partner))
        side.append(remote(arrived, arrived, side_send.at[j], side_recv.at[j], beside))
        last.append(remote(other_half, piece_at(j, 2 if j < FIRST_HEAD else 3, 1 - group), last_send.at[j], last_recv.at[j], partner))

    def middle_at(slot, part_of=None):
        if part_of is None:
            return wq_buf.at[slot, heads - 1, middle]
        return wq_buf.at[slot, heads - 1, pl.ds(pl.multiple_of(half - shift + part_of * shift, 8), shift)]

    def middle_copy(i, source_slot, slot, device, part_of=None):
        return remote(middle_at(source_slot, part_of), middle_at(slot, part_of), middle_send.at[i], middle_recv.at[i], device)

    middle_link = middle_copy(0, 0, 2, across)
    middle_side = middle_copy(1, 2, 2, beside)
    middle_hand = middle_copy(2, 2, 3, partner)
    half_link = middle_copy(3, 0, 2, across, group)
    half_side = middle_copy(4, 2, 2, beside, group)
    half_hand = middle_copy(5, 2, 3, partner, group)
    half_last = middle_copy(6, 2, 3, partner, 1 - group)

    my_rows = pl.ds(pl.multiple_of(member * n_rows, n_rows), n_rows)
    across_rows = pl.ds(pl.multiple_of(((1 - chip) * 2 + core) * n_rows, n_rows), n_rows)
    near = [remote(k_out.at[0, my_rows], k_out.at[0, my_rows], near_send.at[0], near_recv.at[0], partner),
            remote(v_out.at[0, my_rows], v_out.at[0, my_rows], near_send.at[1], near_recv.at[1], partner)]
    far = [remote(kv_stage.at[0], k_out.at[0, my_rows], far_send.at[0], far_recv.at[0], across),
           remote(kv_stage.at[1], v_out.at[0, my_rows], far_send.at[1], far_recv.at[1], across)]
    passed = [remote(k_out.at[0, across_rows], k_out.at[0, across_rows], pass_send.at[0], pass_recv.at[0], partner),
              remote(v_out.at[0, across_rows], v_out.at[0, across_rows], pass_send.at[1], pass_recv.at[1], partner)]
    cross = []
    for h in range(heads):
        near.append(remote(q_stage.at[0, h], q_out.at[h, my_rows], near_send.at[2 + h], near_recv.at[2 + h], partner))
        far.append(remote(q_stage.at[1, 0] if h == 0 else late_out.at[h - 1], q_out.at[h, my_rows], far_send.at[2 + h], far_recv.at[2 + h], across))
        cross.append(remote(q_stage.at[2, h], q_out.at[h, my_rows], cross_send.at[h], cross_recv.at[h], across_other))

    last_h = heads - 1
    lent_rows, kept_rows = pl.ds(0, lent), pl.ds(lent, n_rows - lent)
    my_kept = pl.ds(pl.multiple_of(member * n_rows + lent, lent), n_rows - lent)
    partner_lent = pl.ds(pl.multiple_of((chip * 2 + 1 - core) * n_rows, n_rows), lent)
    lend = remote(q_stage.at[2, last_h, lent_rows], lent_buf, lent_sem.at[0], lent_sem.at[1], partner)
    cross_kept = remote(q_stage.at[2, last_h, kept_rows], q_out.at[last_h, my_kept], cross_send.at[last_h], cross_recv.at[last_h], across_other)
    cross_lent = remote(lent_buf, q_out.at[last_h, partner_lent], lent_sem.at[2], lent_sem.at[3], across)
    my_early = pl.ds(pl.multiple_of(member * n_rows, n_rows), early)
    early_far = remote(late_out.at[0, pl.ds(0, early)], q_out.at[1, my_early], early_sem.at[0], early_sem.at[1], across)

    for j in range(FIRST_HEAD):
        link[j].start()
    for load in loads + [gain_load] + x_loads:
        load.start()

    when(core == 0, lambda: signal(mate_sem, partner))
    when(core == 1, lambda: pl.semaphore_wait(mate_sem, 1))
    signal(pair_sem, across)
    when(group == 1, lambda: signal(ready_sem, beside))
    pl.semaphore_wait(pair_sem, 1)
    for j in range(pieces):
        loads[j].wait()
        if j >= FIRST_HEAD:
            link[j].start()
    when(chip == 0, half_link.start)
    when((chip == 1) & (group == 1), middle_link.start)
    for copy in part:
        copy.start()

    chunks = depth // LANES
    sub = 64

    def norm_step(s, carry):
        here = pl.ds(pl.multiple_of(s * sub, sub), sub)
        total = jnp.zeros((sub, LANES), jnp.float32)
        for c in range(chunks):
            wide = rows_buf[here, c * LANES:(c + 1) * LANES].astype(jnp.float32)
            total = total + wide * wide
        scale = lax.rsqrt(jnp.sum(total, axis=-1, keepdims=True) / depth + EPSILON)
        for c in range(chunks):
            cols = slice(c * LANES, (c + 1) * LANES)
            wide = rows_buf[here, cols].astype(jnp.float32)
            rows_buf[here, cols] = (wide * scale * gain_buf[cols][None, :]).astype(jnp.bfloat16)
        return carry

    def normalize():
        gain_load.wait()
        for load in x_loads:
            load.wait()
        lax.fori_loop(0, n_rows // sub, norm_step, 0)

    def over_tiles(step):
        lax.fori_loop(0, n_rows // dot_tile, lambda i, carry: (step(i * dot_tile), carry)[1], 0)

    def q_block(slot, h, store):
        def step(start):
            tile = rows_buf[pl.ds(pl.multiple_of(start, dot_tile), dot_tile), :]
            store(start, jnp.dot(tile, wq_buf[slot, h], preferred_element_type=jnp.float32).astype(jnp.bfloat16))
        over_tiles(step)

    def kv_block(which, store):
        def step(start):
            tile = rows_buf[pl.ds(pl.multiple_of(start, dot_tile), dot_tile), :]
            both = lax.dot_general(tile, wkv_buf[which], (((1,), (1,)), ((), ())), preferred_element_type=jnp.float32)
            store(start, both.astype(jnp.bfloat16))
        over_tiles(step)

    def rows_at(start):
        return pl.ds(pl.multiple_of(start, dot_tile), dot_tile)

    def own_rows_at(start):
        return pl.ds(pl.multiple_of(member * n_rows + start, dot_tile), dot_tile)

    def own_q(h):
        def store(start, value):
            q_out[h, own_rows_at(start), :] = value
        q_block(0, h, store)

    def staged_q(stage, slot, h):
        def store(start, value):
            q_stage[stage, h, rows_at(start), :] = value
        q_block(slot, h, store)

    def late_q(h):
        def store(start, value):
            late_out[h - 1, rows_at(start), :] = value
        q_block(2, h, store)

    def own_kv():
        def store(start, value):
            k_out[0, own_rows_at(start), :] = value[:, :LANES]
            v_out[0, own_rows_at(start), :] = value[:, LANES:]
        kv_block(0, store)

    def far_kv():
        def store(start, value):
            kv_stage[0, rows_at(start), :] = value[:, :LANES]
            kv_stage[1, rows_at(start), :] = value[:, LANES:]
        kv_block(1, store)

    def from_link(j):
        link[j].wait_recv()
        side[j].start()
        hand[j].start()

    def from_side(j):
        side[j].wait_recv()
        last[j].start()

    def from_middle():
        @pl.when(chip == 0)
        def _():
            @pl.when(group == 1)
            def _():
                middle_link.wait_recv()
                middle_side.start()

            when(group == 0, middle_side.wait_recv)
            middle_hand.start()

        @pl.when(chip == 1)
        def _():
            half_link.wait_recv()
            half_side.start()
            half_hand.start()
            half_side.wait_recv()
            half_last.start()

    def complete_middle():
        when(chip == 0, middle_hand.wait_recv)

        @pl.when(chip == 1)
        def _():
            half_hand.wait_recv()
            half_last.wait_recv()

    def complete(j):
        hand[j].wait_recv()
        last[j].wait_recv()

    @pl.when(group == 0)
    def _():
        pl.semaphore_wait(ready_sem, 1)

    from_link(K_PIECE)
    normalize()
    from_link(V_PIECE)
    part[K_PIECE].wait_recv()
    part[V_PIECE].wait_recv()
    own_kv()
    from_side(K_PIECE)
    near[0].start()
    near[1].start()
    from_link(2)
    from_side(V_PIECE)
    complete(K_PIECE)
    complete(V_PIECE)
    far_kv()
    far[0].start()
    far[1].start()
    own_q(0)
    from_link(3)
    own_q(1)
    from_side(2)
    staged_q(1, 2, 0)
    from_link(4)
    complete(2)
    staged_q(2, 3, 0)

    @pl.when(core == 1)
    def _():
        far[FIRST_HEAD].start()

    from_side(3)
    complete(3)
    staged_q(2, 3, 1)
    cross[0].start()
    late_q(1)
    from_side(4)
    from_middle()
    cross[1].start()
    complete(4)
    complete_middle()
    staged_q(2, 3, 2)
    late_q(2)
    when(core == 0, lend.start)
    own_q(2)

    @pl.when(core == 1)
    def _():
        lend.wait_recv()
        cross_lent.start()
        early_far.start()
        cross[last_h].start()

    @pl.when(core == 0)
    def _():
        cross_kept.start()
        for copy in far[FIRST_HEAD:]:
            copy.start()

    for h in range(heads):
        part[FIRST_HEAD + h].wait_recv()
        staged_q(0, 1, h)
        if h:
            near[2 + h - 1].start()
    far[0].wait_recv()
    passed[0].start()
    far[1].wait_recv()
    passed[1].start()
    near[2 + heads - 1].start()

    for copy in part + link + hand + side + last:
        copy.wait_send()

    @pl.when(chip == 0)
    def _():
        half_link.wait_send()
        middle_hand.wait_send()
        when(group == 1, middle_side.wait_send)

    @pl.when(chip == 1)
    def _():
        when(group == 1, middle_link.wait_send)
        for copy in (half_side, half_hand, half_last):
            copy.wait_send()

    for copy in near + passed + cross[:last_h]:
        copy.wait()
    for copy in far[:FIRST_HEAD]:
        copy.wait_send()
    far[FIRST_HEAD].wait()

    @pl.when(core == 0)
    def _():
        for copy in far[FIRST_HEAD + 1:]:
            copy.wait()
        lend.wait_send()
        cross_kept.wait_send()
        cross[last_h].wait_recv()

    @pl.when(core == 1)
    def _():
        cross[last_h].wait_send()
        early_far.wait()
        cross_lent.wait()
        cross_kept.wait_recv()


def finish_kernel(q_ref, k_ref, v_ref, q_out, k_out, v_out, sems, *, early):
    member = lax.axis_index("tp")
    chip, core = member // 2, member % 2
    n_rows = q_ref.shape[1] // 4
    here, there = [], []
    for ref, out in ((q_ref, q_out), (k_ref, k_out), (v_ref, v_out)):
        for h in range(ref.shape[0]):
            for cut in range(4):
                where = pl.ds(pl.multiple_of(((3 - 2 * chip + cut + 1) % 4) * n_rows, n_rows), n_rows)
                copy = pltpu.make_async_copy(ref.at[h, where], out.at[h, where], sems.at[len(here) + len(there)])
                (there if cut == 3 and ref is q_ref and h else here).append(copy)

    for copy in here:
        copy.start()

    early_rows = pl.ds(pl.multiple_of((3 - 2 * chip) * n_rows, n_rows), early)
    early_copy = pltpu.make_async_copy(q_ref.at[1, early_rows], q_out.at[1, early_rows], sems.at[len(here) + len(there)])

    @pl.when(core == 1)
    def _():
        early_copy.start()

    @pl.when(core == 0)
    def _():
        for copy in there:
            copy.start()

    for copy in here:
        copy.wait()

    @pl.when(core == 1)
    def _():
        early_copy.wait()

    @pl.when(core == 0)
    def _():
        for copy in there:
            copy.wait()


def late_cut(early, n_rows, i):
    return pl.ds(early, n_rows - early) if i == 0 else pl.ds(0, n_rows)


def late_kernel(after_ref, late_out, late_in, send_sem, recv_sem, *, early):
    group, member = lax.axis_index("dp"), lax.axis_index("tp")

    @pl.when(member % 2 == 1)
    def _():
        across = (group, (member + 2) % 4)
        barrier = pltpu.get_barrier_semaphore()
        pl.semaphore_signal(barrier, inc=1, device_id=across, device_id_type=MESH)
        pl.semaphore_wait(barrier, 1)
        copies = [
            pltpu.make_async_remote_copy(src_ref=late_out.at[i, cut], dst_ref=late_in.at[i, cut], send_sem=send_sem.at[i],
                                         recv_sem=recv_sem.at[i], device_id=across, device_id_type=MESH)
            for i, cut in enumerate(late_cut(early, late_out.shape[1], i) for i in range(late_out.shape[0]))
        ]
        for copy in copies:
            copy.start()
        for copy in copies:
            copy.wait()


def patch_kernel(before_ref, late_ref, q_out, sems, *, early):
    member = lax.axis_index("tp")
    n_rows = late_ref.shape[1]

    @pl.when(member % 2 == 1)
    def _():
        base = ((member + 2) % 4) * n_rows
        copies = []
        for i in range(late_ref.shape[0]):
            cut = late_cut(early, n_rows, i)
            where = pl.ds(pl.multiple_of(base + cut.start, early), cut.size)
            copies.append(pltpu.make_async_copy(late_ref.at[i, cut], q_out.at[1 + i, where], sems.at[i]))
        for copy in copies:
            copy.start()
        for copy in copies:
            copy.wait()


def solution(mesh):
    def local_step(x_rows, norm_gain, w_q, w_k, w_v):
        n_rows, depth = x_rows.shape
        heads, width = w_q.shape[1:]
        share = w_k.shape[1]
        members = mesh.shape["tp"]
        pieces = FIRST_HEAD + heads
        all_rows = members * n_rows
        dma = pltpu.SemaphoreType.DMA
        norm_tile = n_rows // 4
        shift, lent, early = 56, 128, 128
        vmem = pl.BlockSpec(memory_space=pltpu.VMEM)
        results = tuple(jax.ShapeDtypeStruct((n, all_rows, width), jnp.bfloat16) for n in (heads, 1, 1))
        hbm = pl.BlockSpec(memory_space=pltpu.HBM)
        late_shape = jax.ShapeDtypeStruct((heads - 1, n_rows, width), jnp.bfloat16)
        q, k, v, late = pl.pallas_call(
            functools.partial(qkv_kernel, norm_tile=norm_tile, dot_tile=256, shift=shift, lent=lent, early=early),
            out_shape=results + (late_shape,),
            in_specs=[hbm] * 5,
            out_specs=(vmem,) * 4,
            scratch_shapes=[
                pltpu.VMEM((n_rows, depth), jnp.bfloat16),
                pltpu.VMEM((depth,), jnp.float32),
                pltpu.VMEM((4, heads, depth, width), jnp.bfloat16),
                pltpu.VMEM((2, 4 * share, depth), jnp.bfloat16),
                pltpu.VMEM((3, heads, n_rows, width), jnp.bfloat16),
                pltpu.VMEM((2, n_rows, width), jnp.bfloat16),
                dma((4,)), dma(()), dma((pieces,)),
                *[dma((pieces,)) for _ in range(10)],
                dma((7,)), dma((7,)), pltpu.SemaphoreType.REGULAR, pltpu.SemaphoreType.REGULAR, pltpu.SemaphoreType.REGULAR,
                pltpu.VMEM((lent, width), jnp.bfloat16), dma((4,)), dma((2,)),
                dma((pieces,)), dma((pieces,)), dma((pieces,)), dma((pieces,)),
                dma((heads,)), dma((heads,)), dma((2,)), dma((2,)),
            ],
            compiler_params=pltpu.CompilerParams(collective_id=0, has_side_effects=True, vmem_limit_bytes=36 * 1024 * 1024),
            cost_estimate=pl.CostEstimate(flops=2 * n_rows * depth * 2048, bytes_accessed=16 * 1024 * 1024, transcendentals=0),
            name="qkv",
        )(*[pltpu.with_memory_space_constraint(a, pltpu.HBM) for a in (x_rows, norm_gain, w_q.transpose(1, 0, 2), w_k.T, w_v.T)])
        q, k, v = pl.pallas_call(
            functools.partial(finish_kernel, early=early),
            out_shape=results,
            in_specs=[vmem] * 3,
            out_specs=(hbm,) * 3,
            scratch_shapes=[dma((4 * (heads + 2) + 1,))],
            compiler_params=pltpu.CompilerParams(vmem_limit_bytes=16 * 1024 * 1024),
            name="finish",
        )(q, k, v)
        late = pl.pallas_call(
            functools.partial(late_kernel, early=early),
            out_shape=late_shape,
            in_specs=[hbm, vmem],
            out_specs=vmem,
            scratch_shapes=[dma((heads - 1,)), dma((heads - 1,))],
            compiler_params=pltpu.CompilerParams(collective_id=1, has_side_effects=True, vmem_limit_bytes=16 * 1024 * 1024),
            name="late",
        )(pltpu.with_memory_space_constraint(q, pltpu.HBM), late)
        q = pl.pallas_call(
            functools.partial(patch_kernel, early=early),
            out_shape=results[0],
            in_specs=[hbm, vmem],
            out_specs=hbm,
            scratch_shapes=[dma((heads - 1,))],
            input_output_aliases={0: 0},
            compiler_params=pltpu.CompilerParams(vmem_limit_bytes=16 * 1024 * 1024),
            name="patch",
        )(q, late)
        return q.transpose(1, 0, 2), k.transpose(1, 0, 2), v.transpose(1, 0, 2)

    return jax.shard_map(
        local_step, mesh=mesh,
        in_specs=(P(("dp", "tp"), None), P(None), P(None, "tp", None), P(None, "tp"), P(None, "tp")),
        out_specs=(P("dp", "tp", None), P("dp", "tp", None), P("dp", "tp", None)),
        check_vma=False,
    )
```

```python
import functools

import jax
import jax.numpy as jnp
from jax import lax
from jax.experimental import pallas as pl
from jax.experimental.pallas import tpu as pltpu
from jax.sharding import PartitionSpec as P

EPSILON = 1e-6
MESH = pl.DeviceIdType.MESH
LANES = 128
K_PIECE, V_PIECE, FIRST_HEAD = 0, 1, 2


def qkv_kernel(
    x_hbm, gain_hbm, wq_hbm, wk_hbm, wv_hbm,
    q_out, k_out, v_out, late_out,
    rows_buf, gain_buf, wq_buf, wkv_buf, q_stage, kv_stage,
    x_sem, gain_sem, load_sem,
    part_send, part_recv, link_send, link_recv, core_send, core_recv, side_send, side_recv, last_send, last_recv,
    middle_send, middle_recv, ready_sem, pair_sem, mate_sem, lent_buf, lent_sem, early_sem,
    near_send, near_recv, far_send, far_recv, cross_send, cross_recv, pass_send, pass_recv,
    *, norm_tile, dot_tile, shift, lent, early,
):
    n_rows, depth = rows_buf.shape
    heads = wq_hbm.shape[0]
    share = wk_hbm.shape[0]
    half = depth // 2
    pieces = FIRST_HEAD + heads

    group, member = lax.axis_index("dp"), lax.axis_index("tp")
    chip, core = member // 2, member % 2
    partner = (group, chip * 2 + (1 - core))
    across = (group, (1 - chip) * 2 + core)
    across_other = (group, (1 - chip) * 2 + (1 - core))
    beside = (1 - group, member)

    sources = [wk_hbm, wv_hbm] + [wq_hbm.at[h] for h in range(heads)]

    last_head = pieces - 1
    middle = pl.ds(half - shift, 2 * shift)

    def piece_at(j, slot, depth_half=None):
        if j < FIRST_HEAD:
            rows = pl.ds(pl.multiple_of(j * 2 * share + core * share, share), share)
            if depth_half is None:
                return wkv_buf.at[slot // 2, rows]
            return wkv_buf.at[slot // 2, rows, pl.ds(pl.multiple_of(depth_half * half, half), half)]
        if depth_half is None:
            return wq_buf.at[slot, j - FIRST_HEAD]
        if j == last_head:
            start = pl.multiple_of(depth_half * (half + shift), 8)
            return wq_buf.at[slot, j - FIRST_HEAD, pl.ds(start, half - shift)]
        return wq_buf.at[slot, j - FIRST_HEAD, pl.ds(pl.multiple_of(depth_half * half, half), half)]

    barrier = pltpu.get_barrier_semaphore()

    def signal(sem, device):
        pl.semaphore_signal(sem, inc=1, device_id=device, device_id_type=MESH)

    def when(condition, act):
        pl.when(condition)(act)

    signal(barrier, across)
    when(core == 1, lambda: signal(barrier, partner))
    when(group == 0, lambda: signal(barrier, beside))
    pl.semaphore_wait(barrier, 2 + group - core)

    loads = [pltpu.make_async_copy(sources[j], piece_at(j, 0), load_sem.at[j]) for j in range(pieces)]
    gain_load = pltpu.make_async_copy(gain_hbm, gain_buf, gain_sem)
    n_tiles = n_rows // norm_tile
    x_loads = [
        pltpu.make_async_copy(x_hbm.at[pl.ds(i * norm_tile, norm_tile)], rows_buf.at[pl.ds(i * norm_tile, norm_tile)], x_sem.at[i])
        for i in range(n_tiles)
    ]

    def remote(src, dst, send, recv, device):
        return pltpu.make_async_remote_copy(src_ref=src, dst_ref=dst, send_sem=send, recv_sem=recv, device_id=device, device_id_type=MESH)

    part, link, hand, side, last = [], [], [], [], []
    for j in range(pieces):
        part.append(remote(piece_at(j, 0), piece_at(j, 0 if j < FIRST_HEAD else 1), part_send.at[j], part_recv.at[j], partner))
        sent = sources[j].at[:, pl.ds(pl.multiple_of(group * half, half), half)] if j < FIRST_HEAD else piece_at(j, 0, group)
        link.append(remote(sent, piece_at(j, 2, group), link_send.at[j], link_recv.at[j], across))
        arrived, other_half = piece_at(j, 2, group), piece_at(j, 2, 1 - group)
        hand.append(remote(arrived, piece_at(j, 2 if j < FIRST_HEAD else 3, group), core_send.at[j], core_recv.at[j], partner))
        side.append(remote(arrived, arrived, side_send.at[j], side_recv.at[j], beside))
        last.append(remote(other_half, piece_at(j, 2 if j < FIRST_HEAD else 3, 1 - group), last_send.at[j], last_recv.at[j], partner))

    def middle_at(slot, part_of=None):
        if part_of is None:
            return wq_buf.at[slot, heads - 1, middle]
        return wq_buf.at[slot, heads - 1, pl.ds(pl.multiple_of(half - shift + part_of * shift, 8), shift)]

    def middle_copy(i, source_slot, slot, device, part_of=None):
        return remote(middle_at(source_slot, part_of), middle_at(slot, part_of), middle_send.at[i], middle_recv.at[i], device)

    middle_link = middle_copy(0, 0, 2, across)
    middle_side = middle_copy(1, 2, 2, beside)
    middle_hand = middle_copy(2, 2, 3, partner)
    half_link = middle_copy(3, 0, 2, across, group)
    half_side = middle_copy(4, 2, 2, beside, group)
    half_hand = middle_copy(5, 2, 3, partner, group)
    half_last = middle_copy(6, 2, 3, partner, 1 - group)

    my_rows = pl.ds(pl.multiple_of(member * n_rows, n_rows), n_rows)
    across_rows = pl.ds(pl.multiple_of(((1 - chip) * 2 + core) * n_rows, n_rows), n_rows)
    near = [remote(k_out.at[0, my_rows], k_out.at[0, my_rows], near_send.at[0], near_recv.at[0], partner),
            remote(v_out.at[0, my_rows], v_out.at[0, my_rows], near_send.at[1], near_recv.at[1], partner)]
    far = [remote(kv_stage.at[0], k_out.at[0, my_rows], far_send.at[0], far_recv.at[0], across),
           remote(kv_stage.at[1], v_out.at[0, my_rows], far_send.at[1], far_recv.at[1], across)]
    passed = [remote(k_out.at[0, across_rows], k_out.at[0, across_rows], pass_send.at[0], pass_recv.at[0], partner),
              remote(v_out.at[0, across_rows], v_out.at[0, across_rows], pass_send.at[1], pass_recv.at[1], partner)]
    cross = []
    for h in range(heads):
        near.append(remote(q_stage.at[0, h], q_out.at[h, my_rows], near_send.at[2 + h], near_recv.at[2 + h], partner))
        far.append(remote(q_stage.at[1, 0] if h == 0 else late_out.at[h - 1], q_out.at[h, my_rows], far_send.at[2 + h], far_recv.at[2 + h], across))
        cross.append(remote(q_stage.at[2, h], q_out.at[h, my_rows], cross_send.at[h], cross_recv.at[h], across_other))

    last_h = heads - 1
    lent_rows, kept_rows = pl.ds(0, lent), pl.ds(lent, n_rows - lent)
    my_kept = pl.ds(pl.multiple_of(member * n_rows + lent, LANES), n_rows - lent)
    partner_lent = pl.ds(pl.multiple_of((chip * 2 + 1 - core) * n_rows, n_rows), lent)
    lend = remote(q_stage.at[2, last_h, lent_rows], lent_buf, lent_sem.at[0], lent_sem.at[1], partner)
    cross_kept = remote(q_stage.at[2, last_h, kept_rows], q_out.at[last_h, my_kept], cross_send.at[last_h], cross_recv.at[last_h], across_other)
    cross_lent = remote(lent_buf, q_out.at[last_h, partner_lent], lent_sem.at[2], lent_sem.at[3], across)
    my_early = pl.ds(pl.multiple_of(member * n_rows, n_rows), early)
    early_far = remote(late_out.at[last_h - 1, pl.ds(0, early)], q_out.at[last_h, my_early], early_sem.at[0], early_sem.at[1], across)

    for j in range(FIRST_HEAD):
        link[j].start()
    for load in loads + [gain_load] + x_loads:
        load.start()

    when(core == 0, lambda: signal(mate_sem, partner))
    when(core == 1, lambda: pl.semaphore_wait(mate_sem, 1))
    signal(pair_sem, across)
    when(group == 1, lambda: signal(ready_sem, beside))
    pl.semaphore_wait(pair_sem, 1)
    for j in range(pieces):
        loads[j].wait()
        if j >= FIRST_HEAD:
            link[j].start()
    when(chip == 0, half_link.start)
    when((chip == 1) & (group == 1), middle_link.start)
    for copy in part:
        copy.start()

    chunks = depth // LANES
    sub = 64

    def norm_step(s, carry):
        here = pl.ds(pl.multiple_of(s * sub, sub), sub)
        total = jnp.zeros((sub, LANES), jnp.float32)
        for c in range(chunks):
            wide = rows_buf[here, c * LANES:(c + 1) * LANES].astype(jnp.float32)
            total = total + wide * wide
        scale = lax.rsqrt(jnp.sum(total, axis=-1, keepdims=True) / depth + EPSILON)
        for c in range(chunks):
            cols = slice(c * LANES, (c + 1) * LANES)
            wide = rows_buf[here, cols].astype(jnp.float32)
            rows_buf[here, cols] = (wide * scale * gain_buf[cols][None, :]).astype(jnp.bfloat16)
        return carry

    def normalize():
        gain_load.wait()
        for load in x_loads:
            load.wait()
        lax.fori_loop(0, n_rows // sub, norm_step, 0)

    def over_tiles(step):
        lax.fori_loop(0, n_rows // dot_tile, lambda i, carry: (step(i * dot_tile), carry)[1], 0)

    def q_block(slot, h, store):
        def step(start):
            tile = rows_buf[pl.ds(pl.multiple_of(start, dot_tile), dot_tile), :]
            store(start, jnp.dot(tile, wq_buf[slot, h], preferred_element_type=jnp.float32).astype(jnp.bfloat16))
        over_tiles(step)

    def kv_block(which, store):
        def step(start):
            tile = rows_buf[pl.ds(pl.multiple_of(start, dot_tile), dot_tile), :]
            both = lax.dot_general(tile, wkv_buf[which], (((1,), (1,)), ((), ())), preferred_element_type=jnp.float32)
            store(start, both.astype(jnp.bfloat16))
        over_tiles(step)

    def rows_at(start):
        return pl.ds(pl.multiple_of(start, dot_tile), dot_tile)

    def own_rows_at(start):
        return pl.ds(pl.multiple_of(member * n_rows + start, dot_tile), dot_tile)

    def own_q(h):
        def store(start, value):
            q_out[h, own_rows_at(start), :] = value
        q_block(0, h, store)

    def staged_q(stage, slot, h):
        def store(start, value):
            q_stage[stage, h, rows_at(start), :] = value
        q_block(slot, h, store)

    def late_q(h):
        def store(start, value):
            late_out[h - 1, rows_at(start), :] = value
        q_block(2, h, store)

    def own_kv():
        def store(start, value):
            k_out[0, own_rows_at(start), :] = value[:, :LANES]
            v_out[0, own_rows_at(start), :] = value[:, LANES:]
        kv_block(0, store)

    def far_kv():
        def store(start, value):
            kv_stage[0, rows_at(start), :] = value[:, :LANES]
            kv_stage[1, rows_at(start), :] = value[:, LANES:]
        kv_block(1, store)

    def from_link(j):
        link[j].wait_recv()
        side[j].start()
        hand[j].start()

    def from_side(j):
        side[j].wait_recv()
        last[j].start()

    def from_middle():
        @pl.when(chip == 0)
        def _():
            @pl.when(group == 1)
            def _():
                middle_link.wait_recv()
                middle_side.start()

            when(group == 0, middle_side.wait_recv)
            middle_hand.start()

        @pl.when(chip == 1)
        def _():
            half_link.wait_recv()
            half_side.start()
            half_hand.start()
            half_side.wait_recv()
            half_last.start()

    def complete_middle():
        when(chip == 0, middle_hand.wait_recv)

        @pl.when(chip == 1)
        def _():
            half_hand.wait_recv()
            half_last.wait_recv()

    def complete(j):
        hand[j].wait_recv()
        last[j].wait_recv()

    @pl.when(group == 0)
    def _():
        pl.semaphore_wait(ready_sem, 1)

    from_link(K_PIECE)
    normalize()
    from_link(V_PIECE)
    part[K_PIECE].wait_recv()
    part[V_PIECE].wait_recv()
    own_kv()
    from_side(K_PIECE)
    near[0].start()
    near[1].start()
    from_link(2)
    from_side(V_PIECE)
    complete(K_PIECE)
    complete(V_PIECE)
    far_kv()
    far[0].start()
    far[1].start()
    own_q(0)
    from_link(3)
    own_q(1)
    from_side(2)
    staged_q(1, 2, 0)
    from_link(4)
    complete(2)
    staged_q(2, 3, 0)

    @pl.when(core == 1)
    def _():
        far[FIRST_HEAD].start()

    from_side(3)
    complete(3)
    staged_q(2, 3, 1)
    cross[0].start()
    late_q(1)
    from_side(4)
    from_middle()
    cross[1].start()
    complete(4)
    complete_middle()
    staged_q(2, 3, 2)
    late_q(2)
    when(core == 0, lend.start)
    own_q(2)

    @pl.when(core == 1)
    def _():
        cross[last_h].start()
        far[FIRST_HEAD + 1].start()
        lend.wait_recv()
        cross_lent.start()
        early_far.start()

    @pl.when(core == 0)
    def _():
        cross_kept.start()
        far[FIRST_HEAD].start()

    for h in range(heads):
        part[FIRST_HEAD + h].wait_recv()
        staged_q(0, 1, h)
        if h:
            near[2 + h - 1].start()
    far[0].wait_recv()
    passed[0].start()
    far[1].wait_recv()
    passed[1].start()
    near[2 + heads - 1].start()

    for copy in part + link + hand + side + last:
        copy.wait_send()

    @pl.when(chip == 0)
    def _():
        half_link.wait_send()
        middle_hand.wait_send()
        when(group == 1, middle_side.wait_send)

    @pl.when(chip == 1)
    def _():
        when(group == 1, middle_link.wait_send)
        for copy in (half_side, half_hand, half_last):
            copy.wait_send()

    for copy in near + passed + cross[:last_h]:
        copy.wait()
    for copy in far[:FIRST_HEAD]:
        copy.wait_send()
    far[FIRST_HEAD].wait()

    @pl.when(core == 0)
    def _():
        lend.wait_send()
        cross_kept.wait_send()
        cross[last_h].wait_recv()

    @pl.when(core == 1)
    def _():
        cross[last_h].wait_send()
        far[FIRST_HEAD + 1].wait()
        early_far.wait()
        cross_lent.wait()
        cross_kept.wait_recv()


def late_cuts(early, n_rows, core):
    return [(0, 0, n_rows), (1, 0, n_rows)] if core == 0 else [(1, early, n_rows - early)]


def finish_kernel(q_ref, k_ref, v_ref, q_out, k_out, v_out, sems, *, early):
    member = lax.axis_index("tp")
    core = member % 2
    n_rows = q_ref.shape[1] // 4
    late_base = ((member + 2) % 4) * n_rows
    always, one_only = [], []

    def copy_of(ref, out, h, where):
        return pltpu.make_async_copy(ref.at[h, where], out.at[h, where], sems.at[len(always) + len(one_only)])

    for ref, out in ((q_ref, q_out), (k_ref, k_out), (v_ref, v_out)):
        for h in range(ref.shape[0]):
            for cut in range(4):
                where = pl.ds(pl.multiple_of(((member + 3 + cut) % 4) * n_rows, n_rows), n_rows)
                if cut < 3 or ref is not q_ref or h == 0:
                    always.append(copy_of(ref, out, h, where))
                elif h == 1:
                    one_only.append(copy_of(ref, out, h, where))
                else:
                    one_only.append(copy_of(ref, out, h, pl.ds(pl.multiple_of(late_base, n_rows), early)))

    for copy in always:
        copy.start()

    @pl.when(core == 1)
    def _():
        for copy in one_only:
            copy.start()

    for copy in always:
        copy.wait()

    @pl.when(core == 1)
    def _():
        for copy in one_only:
            copy.wait()


def late_kernel(after_ref, late_out, late_in, send_sem, recv_sem, *, early):
    group, member = lax.axis_index("dp"), lax.axis_index("tp")
    across = (group, (member + 2) % 4)
    barrier = pltpu.get_barrier_semaphore()
    pl.semaphore_signal(barrier, inc=1, device_id=across, device_id_type=MESH)
    pl.semaphore_wait(barrier, 1)

    def exchange(core):
        copies = []
        for i, start, size in late_cuts(early, late_out.shape[1], core):
            cut = pl.ds(start, size)
            copies.append(pltpu.make_async_remote_copy(src_ref=late_out.at[i, cut], dst_ref=late_in.at[i, cut], send_sem=send_sem.at[i],
                                                       recv_sem=recv_sem.at[i], device_id=across, device_id_type=MESH))
        for copy in copies:
            copy.start()
        for copy in copies:
            copy.wait()

    for core in range(2):
        pl.when(member % 2 == core)(functools.partial(exchange, core))


def patch_kernel(before_ref, late_ref, q_out, sems, *, early):
    member = lax.axis_index("tp")
    n_rows = late_ref.shape[1]
    base = ((member + 2) % 4) * n_rows

    def put(core):
        copies = []
        for i, start, size in late_cuts(early, n_rows, core):
            where = pl.ds(pl.multiple_of(base + start, 64), size)
            copies.append(pltpu.make_async_copy(late_ref.at[i, pl.ds(start, size)], q_out.at[1 + i, where], sems.at[i]))
        for copy in copies:
            copy.start()
        for copy in copies:
            copy.wait()

    for core in range(2):
        pl.when(member % 2 == core)(functools.partial(put, core))


def solution(mesh):
    def local_step(x_rows, norm_gain, w_q, w_k, w_v):
        n_rows, depth = x_rows.shape
        heads, width = w_q.shape[1:]
        share = w_k.shape[1]
        members = mesh.shape["tp"]
        pieces = FIRST_HEAD + heads
        all_rows = members * n_rows
        dma = pltpu.SemaphoreType.DMA
        norm_tile = n_rows // 4
        shift, lent, early = 56, 640, 448
        vmem = pl.BlockSpec(memory_space=pltpu.VMEM)
        results = tuple(jax.ShapeDtypeStruct((n, all_rows, width), jnp.bfloat16) for n in (heads, 1, 1))
        hbm = pl.BlockSpec(memory_space=pltpu.HBM)
        late_shape = jax.ShapeDtypeStruct((heads - 1, n_rows, width), jnp.bfloat16)
        q, k, v, late = pl.pallas_call(
            functools.partial(qkv_kernel, norm_tile=norm_tile, dot_tile=256, shift=shift, lent=lent, early=early),
            out_shape=results + (late_shape,),
            in_specs=[hbm] * 5,
            out_specs=(vmem,) * 4,
            scratch_shapes=[
                pltpu.VMEM((n_rows, depth), jnp.bfloat16),
                pltpu.VMEM((depth,), jnp.float32),
                pltpu.VMEM((4, heads, depth, width), jnp.bfloat16),
                pltpu.VMEM((2, 4 * share, depth), jnp.bfloat16),
                pltpu.VMEM((3, heads, n_rows, width), jnp.bfloat16),
                pltpu.VMEM((2, n_rows, width), jnp.bfloat16),
                dma((4,)), dma(()), dma((pieces,)),
                *[dma((pieces,)) for _ in range(10)],
                dma((7,)), dma((7,)), pltpu.SemaphoreType.REGULAR, pltpu.SemaphoreType.REGULAR, pltpu.SemaphoreType.REGULAR,
                pltpu.VMEM((lent, width), jnp.bfloat16), dma((4,)), dma((2,)),
                dma((pieces,)), dma((pieces,)), dma((pieces,)), dma((pieces,)),
                dma((heads,)), dma((heads,)), dma((2,)), dma((2,)),
            ],
            compiler_params=pltpu.CompilerParams(collective_id=0, has_side_effects=True, vmem_limit_bytes=36 * 1024 * 1024),
            cost_estimate=pl.CostEstimate(flops=2 * n_rows * depth * 2048, bytes_accessed=16 * 1024 * 1024, transcendentals=0),
            name="qkv",
        )(*[pltpu.with_memory_space_constraint(a, pltpu.HBM) for a in (x_rows, norm_gain, w_q.transpose(1, 0, 2), w_k.T, w_v.T)])
        q, k, v = pl.pallas_call(
            functools.partial(finish_kernel, early=early),
            out_shape=results,
            in_specs=[vmem] * 3,
            out_specs=(hbm,) * 3,
            scratch_shapes=[dma((4 * (heads + 2),))],
            compiler_params=pltpu.CompilerParams(vmem_limit_bytes=16 * 1024 * 1024),
            name="finish",
        )(q, k, v)
        late = pl.pallas_call(
            functools.partial(late_kernel, early=early),
            out_shape=late_shape,
            in_specs=[hbm, vmem],
            out_specs=vmem,
            scratch_shapes=[dma((heads - 1,)), dma((heads - 1,))],
            compiler_params=pltpu.CompilerParams(collective_id=1, has_side_effects=True, vmem_limit_bytes=16 * 1024 * 1024),
            name="late",
        )(pltpu.with_memory_space_constraint(q, pltpu.HBM), late)
        q = pl.pallas_call(
            functools.partial(patch_kernel, early=early),
            out_shape=results[0],
            in_specs=[hbm, vmem],
            out_specs=hbm,
            scratch_shapes=[dma((heads - 1,))],
            input_output_aliases={0: 0},
            compiler_params=pltpu.CompilerParams(vmem_limit_bytes=16 * 1024 * 1024),
            name="patch",
        )(q, late)
        return q.transpose(1, 0, 2), k.transpose(1, 0, 2), v.transpose(1, 0, 2)

    return jax.shard_map(
        local_step, mesh=mesh,
        in_specs=(P(("dp", "tp"), None), P(None), P(None, "tp", None), P(None, "tp"), P(None, "tp")),
        out_specs=(P("dp", "tp", None), P("dp", "tp", None), P("dp", "tp", None)),
        check_vma=False,
    )
```

```python
import functools

import jax
import jax.numpy as jnp
from jax import lax
from jax.experimental import pallas as pl
from jax.experimental.pallas import tpu as pltpu
from jax.sharding import PartitionSpec as P

EPSILON = 1e-6
MESH = pl.DeviceIdType.MESH
LANES = 128
K_PIECE, V_PIECE, FIRST_HEAD = 0, 1, 2


def qkv_kernel(
    x_hbm, gain_hbm, wq_hbm, wk_hbm, wv_hbm,
    q_out, k_out, v_out, late_out,
    rows_buf, gain_buf, wq_buf, wkv_buf, q_stage, kv_stage,
    x_sem, gain_sem, load_sem,
    part_send, part_recv, link_send, link_recv, core_send, core_recv, side_send, side_recv, last_send, last_recv,
    middle_send, middle_recv, ready_sem, pair_sem, mate_sem, lent_buf, lent_sem, early_sem,
    near_send, near_recv, far_send, far_recv, cross_send, cross_recv, pass_send, pass_recv,
    *, norm_tile, dot_tile, shift, lent, early,
):
    n_rows, depth = rows_buf.shape
    heads = wq_hbm.shape[0]
    share = wk_hbm.shape[0]
    half = depth // 2
    pieces = FIRST_HEAD + heads

    group, member = lax.axis_index("dp"), lax.axis_index("tp")
    chip, core = member // 2, member % 2
    partner = (group, chip * 2 + (1 - core))
    across = (group, (1 - chip) * 2 + core)
    across_other = (group, (1 - chip) * 2 + (1 - core))
    beside = (1 - group, member)

    sources = [wk_hbm, wv_hbm] + [wq_hbm.at[h] for h in range(heads)]

    last_head = pieces - 1
    middle = pl.ds(half - shift, 2 * shift)

    def piece_at(j, slot, depth_half=None):
        if j < FIRST_HEAD:
            rows = pl.ds(pl.multiple_of(j * 2 * share + core * share, share), share)
            if depth_half is None:
                return wkv_buf.at[slot // 2, rows]
            return wkv_buf.at[slot // 2, rows, pl.ds(pl.multiple_of(depth_half * half, half), half)]
        if depth_half is None:
            return wq_buf.at[slot, j - FIRST_HEAD]
        if j == last_head:
            start = pl.multiple_of(depth_half * (half + shift), 8)
            return wq_buf.at[slot, j - FIRST_HEAD, pl.ds(start, half - shift)]
        return wq_buf.at[slot, j - FIRST_HEAD, pl.ds(pl.multiple_of(depth_half * half, half), half)]

    barrier = pltpu.get_barrier_semaphore()

    def signal(sem, device):
        pl.semaphore_signal(sem, inc=1, device_id=device, device_id_type=MESH)

    def when(condition, act):
        pl.when(condition)(act)

    signal(barrier, across)
    when(core == 1, lambda: signal(barrier, partner))
    when(group == 0, lambda: signal(barrier, beside))
    pl.semaphore_wait(barrier, 2 + group - core)

    loads = [pltpu.make_async_copy(sources[j], piece_at(j, 0), load_sem.at[j]) for j in range(pieces)]
    gain_load = pltpu.make_async_copy(gain_hbm, gain_buf, gain_sem)
    n_tiles = n_rows // norm_tile
    x_loads = [
        pltpu.make_async_copy(x_hbm.at[pl.ds(i * norm_tile, norm_tile)], rows_buf.at[pl.ds(i * norm_tile, norm_tile)], x_sem.at[i])
        for i in range(n_tiles)
    ]

    def remote(src, dst, send, recv, device):
        return pltpu.make_async_remote_copy(src_ref=src, dst_ref=dst, send_sem=send, recv_sem=recv, device_id=device, device_id_type=MESH)

    part, link, hand, side, last = [], [], [], [], []
    for j in range(pieces):
        part.append(remote(piece_at(j, 0), piece_at(j, 0 if j < FIRST_HEAD else 1), part_send.at[j], part_recv.at[j], partner))
        sent = sources[j].at[:, pl.ds(pl.multiple_of(group * half, half), half)] if j < FIRST_HEAD else piece_at(j, 0, group)
        link.append(remote(sent, piece_at(j, 2, group), link_send.at[j], link_recv.at[j], across))
        arrived, other_half = piece_at(j, 2, group), piece_at(j, 2, 1 - group)
        hand.append(remote(arrived, piece_at(j, 2 if j < FIRST_HEAD else 3, group), core_send.at[j], core_recv.at[j], partner))
        side.append(remote(arrived, arrived, side_send.at[j], side_recv.at[j], beside))
        last.append(remote(other_half, piece_at(j, 2 if j < FIRST_HEAD else 3, 1 - group), last_send.at[j], last_recv.at[j], partner))

    def middle_at(slot, part_of=None):
        if part_of is None:
            return wq_buf.at[slot, heads - 1, middle]
        return wq_buf.at[slot, heads - 1, pl.ds(pl.multiple_of(half - shift + part_of * shift, 8), shift)]

    def middle_copy(i, source_slot, slot, device, part_of=None):
        return remote(middle_at(source_slot, part_of), middle_at(slot, part_of), middle_send.at[i], middle_recv.at[i], device)

    middle_link = middle_copy(0, 0, 2, across)
    middle_side = middle_copy(1, 2, 2, beside)
    middle_hand = middle_copy(2, 2, 3, partner)
    half_link = middle_copy(3, 0, 2, across, group)
    half_side = middle_copy(4, 2, 2, beside, group)
    half_hand = middle_copy(5, 2, 3, partner, group)
    half_last = middle_copy(6, 2, 3, partner, 1 - group)

    my_rows = pl.ds(pl.multiple_of(member * n_rows, n_rows), n_rows)
    across_rows = pl.ds(pl.multiple_of(((1 - chip) * 2 + core) * n_rows, n_rows), n_rows)
    near = [remote(k_out.at[0, my_rows], k_out.at[0, my_rows], near_send.at[0], near_recv.at[0], partner),
            remote(v_out.at[0, my_rows], v_out.at[0, my_rows], near_send.at[1], near_recv.at[1], partner)]
    far = [remote(kv_stage.at[0], k_out.at[0, my_rows], far_send.at[0], far_recv.at[0], across),
           remote(kv_stage.at[1], v_out.at[0, my_rows], far_send.at[1], far_recv.at[1], across)]
    passed = [remote(k_out.at[0, across_rows], k_out.at[0, across_rows], pass_send.at[0], pass_recv.at[0], partner),
              remote(v_out.at[0, across_rows], v_out.at[0, across_rows], pass_send.at[1], pass_recv.at[1], partner)]
    cross = []
    for h in range(heads):
        near.append(remote(q_stage.at[0, h], q_out.at[h, my_rows], near_send.at[2 + h], near_recv.at[2 + h], partner))
        far.append(remote(q_stage.at[1, 0] if h == 0 else late_out.at[h - 1], q_out.at[h, my_rows], far_send.at[2 + h], far_recv.at[2 + h], across))
        cross.append(remote(q_stage.at[2, h], q_out.at[h, my_rows], cross_send.at[h], cross_recv.at[h], across_other))

    last_h = heads - 1
    lent_rows, kept_rows = pl.ds(0, lent), pl.ds(lent, n_rows - lent)
    my_kept = pl.ds(pl.multiple_of(member * n_rows + lent, lent), n_rows - lent)
    partner_lent = pl.ds(pl.multiple_of((chip * 2 + 1 - core) * n_rows, n_rows), lent)
    lend = remote(q_stage.at[2, last_h, lent_rows], lent_buf, lent_sem.at[0], lent_sem.at[1], partner)
    cross_kept = remote(q_stage.at[2, last_h, kept_rows], q_out.at[last_h, my_kept], cross_send.at[last_h], cross_recv.at[last_h], across_other)
    cross_lent = remote(lent_buf, q_out.at[last_h, partner_lent], lent_sem.at[2], lent_sem.at[3], across)
    my_early = pl.ds(pl.multiple_of(member * n_rows, n_rows), early)
    early_far = remote(late_out.at[:, pl.ds(0, early)], q_out.at[pl.ds(1, heads - 1), my_early], early_sem.at[0], early_sem.at[1], across)

    for j in range(FIRST_HEAD):
        link[j].start()
    for load in loads + [gain_load] + x_loads:
        load.start()

    when(core == 0, lambda: signal(mate_sem, partner))
    when(core == 1, lambda: pl.semaphore_wait(mate_sem, 1))
    signal(pair_sem, across)
    when(group == 1, lambda: signal(ready_sem, beside))
    pl.semaphore_wait(pair_sem, 1)
    for j in range(pieces):
        loads[j].wait()
        if j >= FIRST_HEAD:
            link[j].start()
    when(chip == 0, half_link.start)
    when((chip == 1) & (group == 1), middle_link.start)
    for copy in part:
        copy.start()

    chunks = depth // LANES
    sub = 64

    def norm_step(s, carry):
        here = pl.ds(pl.multiple_of(s * sub, sub), sub)
        total = jnp.zeros((sub, LANES), jnp.float32)
        for c in range(chunks):
            wide = rows_buf[here, c * LANES:(c + 1) * LANES].astype(jnp.float32)
            total = total + wide * wide
        scale = lax.rsqrt(jnp.sum(total, axis=-1, keepdims=True) / depth + EPSILON)
        for c in range(chunks):
            cols = slice(c * LANES, (c + 1) * LANES)
            wide = rows_buf[here, cols].astype(jnp.float32)
            rows_buf[here, cols] = (wide * scale * gain_buf[cols][None, :]).astype(jnp.bfloat16)
        return carry

    def normalize():
        gain_load.wait()
        for load in x_loads:
            load.wait()
        lax.fori_loop(0, n_rows // sub, norm_step, 0)

    def over_tiles(step):
        lax.fori_loop(0, n_rows // dot_tile, lambda i, carry: (step(i * dot_tile), carry)[1], 0)

    def q_block(slot, h, store):
        def step(start):
            tile = rows_buf[pl.ds(pl.multiple_of(start, dot_tile), dot_tile), :]
            store(start, jnp.dot(tile, wq_buf[slot, h], preferred_element_type=jnp.float32).astype(jnp.bfloat16))
        over_tiles(step)

    def kv_block(which, store):
        def step(start):
            tile = rows_buf[pl.ds(pl.multiple_of(start, dot_tile), dot_tile), :]
            both = lax.dot_general(tile, wkv_buf[which], (((1,), (1,)), ((), ())), preferred_element_type=jnp.float32)
            store(start, both.astype(jnp.bfloat16))
        over_tiles(step)

    def rows_at(start):
        return pl.ds(pl.multiple_of(start, dot_tile), dot_tile)

    def own_rows_at(start):
        return pl.ds(pl.multiple_of(member * n_rows + start, dot_tile), dot_tile)

    def own_q(h):
        def store(start, value):
            q_out[h, own_rows_at(start), :] = value
        q_block(0, h, store)

    def staged_q(stage, slot, h):
        def store(start, value):
            q_stage[stage, h, rows_at(start), :] = value
        q_block(slot, h, store)

    def late_q(h):
        def store(start, value):
            late_out[h - 1, rows_at(start), :] = value
        q_block(2, h, store)

    def own_kv():
        def store(start, value):
            k_out[0, own_rows_at(start), :] = value[:, :LANES]
            v_out[0, own_rows_at(start), :] = value[:, LANES:]
        kv_block(0, store)

    def far_kv():
        def store(start, value):
            kv_stage[0, rows_at(start), :] = value[:, :LANES]
            kv_stage[1, rows_at(start), :] = value[:, LANES:]
        kv_block(1, store)

    def from_link(j):
        link[j].wait_recv()
        side[j].start()
        hand[j].start()

    def from_side(j):
        side[j].wait_recv()
        last[j].start()

    def from_middle():
        @pl.when(chip == 0)
        def _():
            @pl.when(group == 1)
            def _():
                middle_link.wait_recv()
                middle_side.start()

            when(group == 0, middle_side.wait_recv)
            middle_hand.start()

        @pl.when(chip == 1)
        def _():
            half_link.wait_recv()
            half_side.start()
            half_hand.start()
            half_side.wait_recv()
            half_last.start()

    def complete_middle():
        when(chip == 0, middle_hand.wait_recv)

        @pl.when(chip == 1)
        def _():
            half_hand.wait_recv()
            half_last.wait_recv()

    def complete(j):
        hand[j].wait_recv()
        last[j].wait_recv()

    @pl.when(group == 0)
    def _():
        pl.semaphore_wait(ready_sem, 1)

    from_link(K_PIECE)
    normalize()
    from_link(V_PIECE)
    part[K_PIECE].wait_recv()
    part[V_PIECE].wait_recv()
    own_kv()
    from_side(K_PIECE)
    near[0].start()
    near[1].start()
    from_link(2)
    from_side(V_PIECE)
    complete(K_PIECE)
    complete(V_PIECE)
    far_kv()
    far[0].start()
    far[1].start()
    own_q(0)
    from_link(3)
    own_q(1)
    from_side(2)
    staged_q(1, 2, 0)
    from_link(4)
    complete(2)
    staged_q(2, 3, 0)

    @pl.when(core == 1)
    def _():
        far[FIRST_HEAD].start()

    from_side(3)
    complete(3)
    staged_q(2, 3, 1)
    cross[0].start()
    late_q(1)
    from_side(4)
    from_middle()
    cross[1].start()
    complete(4)
    complete_middle()
    staged_q(2, 3, 2)
    late_q(2)
    when(core == 0, lend.start)
    own_q(2)

    @pl.when(core == 1)
    def _():
        lend.wait_recv()
        cross_lent.start()
        early_far.start()
        cross[last_h].start()

    @pl.when(core == 0)
    def _():
        cross_kept.start()
        for copy in far[FIRST_HEAD:]:
            copy.start()

    for h in range(heads):
        part[FIRST_HEAD + h].wait_recv()
        staged_q(0, 1, h)
        if h:
            near[2 + h - 1].start()
    far[0].wait_recv()
    passed[0].start()
    far[1].wait_recv()
    passed[1].start()
    near[2 + heads - 1].start()

    for copy in part + link + hand + side + last:
        copy.wait_send()

    @pl.when(chip == 0)
    def _():
        half_link.wait_send()
        middle_hand.wait_send()
        when(group == 1, middle_side.wait_send)

    @pl.when(chip == 1)
    def _():
        when(group == 1, middle_link.wait_send)
        for copy in (half_side, half_hand, half_last):
            copy.wait_send()

    for copy in near + passed + cross[:last_h]:
        copy.wait()
    for copy in far[:FIRST_HEAD]:
        copy.wait_send()
    far[FIRST_HEAD].wait()

    @pl.when(core == 0)
    def _():
        for copy in far[FIRST_HEAD + 1:]:
            copy.wait()
        lend.wait_send()
        cross_kept.wait_send()
        cross[last_h].wait_recv()

    @pl.when(core == 1)
    def _():
        cross[last_h].wait_send()
        early_far.wait()
        cross_lent.wait()
        cross_kept.wait_recv()


def finish_kernel(q_ref, k_ref, v_ref, q_out, k_out, v_out, sems, *, early):
    member = lax.axis_index("tp")
    core = member % 2
    heads, n_rows = q_ref.shape[0], q_ref.shape[1] // 4
    late_heads = pl.ds(1, heads - 1)

    def copy_of(i, ref, out, *where):
        return pltpu.make_async_copy(ref.at[where], out.at[where], sems.at[i])

    def rows(ahead, size):
        return pl.ds(pl.multiple_of(((member + ahead) % 4) * n_rows, n_rows), size)

    always = [copy_of(i, q_ref, q_out, late_heads, rows(ahead, n_rows)) for i, ahead in enumerate((0, 1, 3))]
    always += [copy_of(3, q_ref, q_out, 0), copy_of(4, k_ref, k_out, 0), copy_of(5, v_ref, v_out, 0)]
    whole = copy_of(6, q_ref, q_out, late_heads, rows(2, n_rows))
    begun = copy_of(6, q_ref, q_out, late_heads, rows(2, early))
    for copy in always:
        copy.start()
    pl.when(core == 0)(whole.start)
    pl.when(core == 1)(begun.start)
    for copy in always:
        copy.wait()
    pl.when(core == 0)(whole.wait)
    pl.when(core == 1)(begun.wait)


def late_kernel(after_ref, late_out, late_in, send_sem, recv_sem, *, early):
    group, member = lax.axis_index("dp"), lax.axis_index("tp")

    @pl.when(member % 2 == 1)
    def _():
        across = (group, (member + 2) % 4)
        barrier = pltpu.get_barrier_semaphore()
        pl.semaphore_signal(barrier, inc=1, device_id=across, device_id_type=MESH)
        pl.semaphore_wait(barrier, 1)
        rest = pl.ds(early, late_out.shape[1] - early)
        copy = pltpu.make_async_remote_copy(src_ref=late_out.at[:, rest], dst_ref=late_in.at[:, rest], send_sem=send_sem, recv_sem=recv_sem,
                                            device_id=across, device_id_type=MESH)
        copy.start()
        copy.wait()


def patch_kernel(before_ref, late_ref, q_out, sem, *, early):
    member = lax.axis_index("tp")
    late_heads, n_rows, _ = late_ref.shape

    @pl.when(member % 2 == 1)
    def _():
        size = n_rows - early
        where = pl.ds(pl.multiple_of(((member + 2) % 4) * n_rows + early, early), size)
        copy = pltpu.make_async_copy(late_ref.at[:, pl.ds(early, size)], q_out.at[pl.ds(1, late_heads), where], sem)
        copy.start()
        copy.wait()


def solution(mesh):
    def local_step(x_rows, norm_gain, w_q, w_k, w_v):
        n_rows, depth = x_rows.shape
        heads, width = w_q.shape[1:]
        share = w_k.shape[1]
        members = mesh.shape["tp"]
        pieces = FIRST_HEAD + heads
        all_rows = members * n_rows
        dma = pltpu.SemaphoreType.DMA
        norm_tile = n_rows // 4
        shift, lent, early = 56, 128, 64
        vmem = pl.BlockSpec(memory_space=pltpu.VMEM)
        results = tuple(jax.ShapeDtypeStruct((n, all_rows, width), jnp.bfloat16) for n in (heads, 1, 1))
        hbm = pl.BlockSpec(memory_space=pltpu.HBM)
        late_shape = jax.ShapeDtypeStruct((heads - 1, n_rows, width), jnp.bfloat16)
        q, k, v, late = pl.pallas_call(
            functools.partial(qkv_kernel, norm_tile=norm_tile, dot_tile=256, shift=shift, lent=lent, early=early),
            out_shape=results + (late_shape,),
            in_specs=[hbm] * 5,
            out_specs=(vmem,) * 4,
            scratch_shapes=[
                pltpu.VMEM((n_rows, depth), jnp.bfloat16),
                pltpu.VMEM((depth,), jnp.float32),
                pltpu.VMEM((4, heads, depth, width), jnp.bfloat16),
                pltpu.VMEM((2, 4 * share, depth), jnp.bfloat16),
                pltpu.VMEM((3, heads, n_rows, width), jnp.bfloat16),
                pltpu.VMEM((2, n_rows, width), jnp.bfloat16),
                dma((4,)), dma(()), dma((pieces,)),
                *[dma((pieces,)) for _ in range(10)],
                dma((7,)), dma((7,)), pltpu.SemaphoreType.REGULAR, pltpu.SemaphoreType.REGULAR, pltpu.SemaphoreType.REGULAR,
                pltpu.VMEM((lent, width), jnp.bfloat16), dma((4,)), dma((2,)),
                dma((pieces,)), dma((pieces,)), dma((pieces,)), dma((pieces,)),
                dma((heads,)), dma((heads,)), dma((2,)), dma((2,)),
            ],
            compiler_params=pltpu.CompilerParams(collective_id=0, has_side_effects=True, vmem_limit_bytes=36 * 1024 * 1024),
            cost_estimate=pl.CostEstimate(flops=2 * n_rows * depth * 2048, bytes_accessed=16 * 1024 * 1024, transcendentals=0),
            name="qkv",
        )(*[pltpu.with_memory_space_constraint(a, pltpu.HBM) for a in (x_rows, norm_gain, w_q.transpose(1, 0, 2), w_k.T, w_v.T)])
        q, k, v = pl.pallas_call(
            functools.partial(finish_kernel, early=early),
            out_shape=results,
            in_specs=[vmem] * 3,
            out_specs=(hbm,) * 3,
            scratch_shapes=[dma((7,))],
            compiler_params=pltpu.CompilerParams(vmem_limit_bytes=16 * 1024 * 1024),
            name="finish",
        )(q, k, v)
        late = pl.pallas_call(
            functools.partial(late_kernel, early=early),
            out_shape=late_shape,
            in_specs=[hbm, vmem],
            out_specs=vmem,
            scratch_shapes=[dma(()), dma(())],
            compiler_params=pltpu.CompilerParams(collective_id=1, has_side_effects=True, vmem_limit_bytes=16 * 1024 * 1024),
            name="late",
        )(pltpu.with_memory_space_constraint(q, pltpu.HBM), late)
        q = pl.pallas_call(
            functools.partial(patch_kernel, early=early),
            out_shape=results[0],
            in_specs=[hbm, vmem],
            out_specs=hbm,
            scratch_shapes=[dma(())],
            input_output_aliases={0: 0},
            compiler_params=pltpu.CompilerParams(vmem_limit_bytes=16 * 1024 * 1024),
            name="patch",
        )(q, late)
        return q.transpose(1, 0, 2), k.transpose(1, 0, 2), v.transpose(1, 0, 2)

    return jax.shard_map(
        local_step, mesh=mesh,
        in_specs=(P(("dp", "tp"), None), P(None), P(None, "tp", None), P(None, "tp"), P(None, "tp")),
        out_specs=(P("dp", "tp", None), P("dp", "tp", None), P("dp", "tp", None)),
        check_vma=False,
    )
```

```python
import functools

import jax
import jax.numpy as jnp
from jax import lax
from jax.experimental import pallas as pl
from jax.experimental.pallas import tpu as pltpu
from jax.sharding import PartitionSpec as P

EPSILON = 1e-6
MESH = pl.DeviceIdType.MESH
LANES = 128
K_PIECE, V_PIECE, FIRST_HEAD = 0, 1, 2


def qkv_kernel(
    x_hbm, gain_hbm, wq_hbm, wk_hbm, wv_hbm,
    q_out, k_out, v_out, late_out,
    rows_buf, gain_buf, wq_buf, wkv_buf, q_stage, kv_stage,
    x_sem, gain_sem, load_sem,
    part_send, part_recv, link_send, link_recv, core_send, core_recv, side_send, side_recv, last_send, last_recv,
    middle_send, middle_recv, ready_sem, pair_sem, mate_sem, lent_buf, lent_sem, early_sem,
    near_send, near_recv, far_send, far_recv, cross_send, cross_recv, pass_send, pass_recv,
    *, norm_tile, dot_tile, shift, lent, early,
):
    n_rows, depth = rows_buf.shape
    heads = wq_hbm.shape[0]
    share = wk_hbm.shape[0]
    half = depth // 2
    pieces = FIRST_HEAD + heads

    group, member = lax.axis_index("dp"), lax.axis_index("tp")
    chip, core = lax.div(member, 2), lax.rem(member, 2)
    partner = (group, chip * 2 + (1 - core))
    across = (group, (1 - chip) * 2 + core)
    across_other = (group, (1 - chip) * 2 + (1 - core))
    beside = (1 - group, member)

    sources = [wk_hbm, wv_hbm] + [wq_hbm.at[h] for h in range(heads)]

    last_head = pieces - 1
    middle = pl.ds(half - shift, 2 * shift)

    def piece_at(j, slot, depth_half=None):
        if j < FIRST_HEAD:
            rows = pl.ds(pl.multiple_of(j * 2 * share + core * share, share), share)
            if depth_half is None:
                return wkv_buf.at[slot // 2, rows]
            return wkv_buf.at[slot // 2, rows, pl.ds(pl.multiple_of(depth_half * half, half), half)]
        if depth_half is None:
            return wq_buf.at[slot, j - FIRST_HEAD]
        if j == last_head:
            start = pl.multiple_of(depth_half * (half + shift), 8)
            return wq_buf.at[slot, j - FIRST_HEAD, pl.ds(start, half - shift)]
        return wq_buf.at[slot, j - FIRST_HEAD, pl.ds(pl.multiple_of(depth_half * half, half), half)]

    barrier = pltpu.get_barrier_semaphore()

    def signal(sem, device):
        pl.semaphore_signal(sem, inc=1, device_id=device, device_id_type=MESH)

    def when(condition, act):
        pl.when(condition)(act)

    signal(barrier, across)
    when(core == 1, lambda: signal(barrier, partner))
    when(group == 0, lambda: signal(barrier, beside))
    pl.semaphore_wait(barrier, 2 + group - core)

    loads = [pltpu.make_async_copy(sources[j], piece_at(j, 0), load_sem.at[j]) for j in range(pieces)]
    gain_load = pltpu.make_async_copy(gain_hbm, gain_buf, gain_sem)
    n_tiles = n_rows // norm_tile
    x_loads = [
        pltpu.make_async_copy(x_hbm.at[pl.ds(i * norm_tile, norm_tile)], rows_buf.at[pl.ds(i * norm_tile, norm_tile)], x_sem.at[i])
        for i in range(n_tiles)
    ]

    def remote(src, dst, send, recv, device):
        return pltpu.make_async_remote_copy(src_ref=src, dst_ref=dst, send_sem=send, recv_sem=recv, device_id=device, device_id_type=MESH)

    part, link, hand, side, last = [], [], [], [], []
    for j in range(pieces):
        part.append(remote(piece_at(j, 0), piece_at(j, 0 if j < FIRST_HEAD else 1), part_send.at[j], part_recv.at[j], partner))
        sent = sources[j].at[:, pl.ds(pl.multiple_of(group * half, half), half)] if j < FIRST_HEAD else piece_at(j, 0, group)
        link.append(remote(sent, piece_at(j, 2, group), link_send.at[j], link_recv.at[j], across))
        arrived, other_half = piece_at(j, 2, group), piece_at(j, 2, 1 - group)
        hand.append(remote(arrived, piece_at(j, 2 if j < FIRST_HEAD else 3, group), core_send.at[j], core_recv.at[j], partner))
        side.append(remote(arrived, arrived, side_send.at[j], side_recv.at[j], beside))
        last.append(remote(other_half, piece_at(j, 2 if j < FIRST_HEAD else 3, 1 - group), last_send.at[j], last_recv.at[j], partner))

    def middle_at(slot, part_of=None):
        if part_of is None:
            return wq_buf.at[slot, heads - 1, middle]
        return wq_buf.at[slot, heads - 1, pl.ds(pl.multiple_of(half - shift + part_of * shift, 8), shift)]

    def middle_copy(i, source_slot, slot, device, part_of=None):
        return remote(middle_at(source_slot, part_of), middle_at(slot, part_of), middle_send.at[i], middle_recv.at[i], device)

    middle_link = middle_copy(0, 0, 2, across)
    middle_side = middle_copy(1, 2, 2, beside)
    middle_hand = middle_copy(2, 2, 3, partner)
    half_link = middle_copy(3, 0, 2, across, group)
    half_side = middle_copy(4, 2, 2, beside, group)
    half_hand = middle_copy(5, 2, 3, partner, group)
    half_last = middle_copy(6, 2, 3, partner, 1 - group)

    my_rows = pl.ds(pl.multiple_of(member * n_rows, n_rows), n_rows)
    across_rows = pl.ds(pl.multiple_of(((1 - chip) * 2 + core) * n_rows, n_rows), n_rows)
    near = [remote(k_out.at[0, my_rows], k_out.at[0, my_rows], near_send.at[0], near_recv.at[0], partner),
            remote(v_out.at[0, my_rows], v_out.at[0, my_rows], near_send.at[1], near_recv.at[1], partner)]
    far = [remote(kv_stage.at[0], k_out.at[0, my_rows], far_send.at[0], far_recv.at[0], across),
           remote(kv_stage.at[1], v_out.at[0, my_rows], far_send.at[1], far_recv.at[1], across)]
    passed = [remote(k_out.at[0, across_rows], k_out.at[0, across_rows], pass_send.at[0], pass_recv.at[0], partner),
              remote(v_out.at[0, across_rows], v_out.at[0, across_rows], pass_send.at[1], pass_recv.at[1], partner)]
    cross = []
    for h in range(heads):
        near.append(remote(q_stage.at[0, h], q_out.at[h, my_rows], near_send.at[2 + h], near_recv.at[2 + h], partner))
        far.append(remote(q_stage.at[1, 0] if h == 0 else late_out.at[h - 1], q_out.at[h, my_rows], far_send.at[2 + h], far_recv.at[2 + h], across))
        cross.append(remote(q_stage.at[2, h], q_out.at[h, my_rows], cross_send.at[h], cross_recv.at[h], across_other))

    last_h = heads - 1
    lent_rows, kept_rows = pl.ds(0, lent), pl.ds(lent, n_rows - lent)
    my_kept = pl.ds(pl.multiple_of(member * n_rows + lent, lent), n_rows - lent)
    partner_lent = pl.ds(pl.multiple_of((chip * 2 + 1 - core) * n_rows, n_rows), lent)
    lend = remote(q_stage.at[2, last_h, lent_rows], lent_buf, lent_sem.at[0], lent_sem.at[1], partner)
    cross_kept = remote(q_stage.at[2, last_h, kept_rows], q_out.at[last_h, my_kept], cross_send.at[last_h], cross_recv.at[last_h], across_other)
    cross_lent = remote(lent_buf, q_out.at[last_h, partner_lent], lent_sem.at[2], lent_sem.at[3], across)
    early_far = []
    for rows in early:
        my_early = pl.ds(pl.multiple_of(member * n_rows, n_rows), rows)
        early_far.append(remote(late_out.at[:, pl.ds(0, rows)], q_out.at[pl.ds(1, heads - 1), my_early], early_sem.at[0], early_sem.at[1], across))

    for j in range(FIRST_HEAD):
        link[j].start()
    for load in loads + [gain_load] + x_loads:
        load.start()

    when(core == 0, lambda: signal(mate_sem, partner))
    when(core == 1, lambda: pl.semaphore_wait(mate_sem, 1))
    signal(pair_sem, across)
    when(group == 1, lambda: signal(ready_sem, beside))
    pl.semaphore_wait(pair_sem, 1)
    for j in range(pieces):
        loads[j].wait()
        if j >= FIRST_HEAD:
            link[j].start()
    when(chip == 0, half_link.start)
    when((chip == 1) & (group == 1), middle_link.start)
    for copy in part:
        copy.start()

    chunks = depth // LANES
    sub = 64

    def norm_step(s, carry):
        here = pl.ds(pl.multiple_of(s * sub, sub), sub)
        total = jnp.zeros((sub, LANES), jnp.float32)
        for c in range(chunks):
            wide = rows_buf[here, c * LANES:(c + 1) * LANES].astype(jnp.float32)
            total = total + wide * wide
        scale = lax.rsqrt(jnp.sum(total, axis=-1, keepdims=True) / depth + EPSILON)
        for c in range(chunks):
            cols = slice(c * LANES, (c + 1) * LANES)
            wide = rows_buf[here, cols].astype(jnp.float32)
            rows_buf[here, cols] = (wide * scale * gain_buf[cols][None, :]).astype(jnp.bfloat16)
        return carry

    def normalize():
        gain_load.wait()
        for load in x_loads:
            load.wait()
        lax.fori_loop(0, n_rows // sub, norm_step, 0)

    def over_tiles(step):
        lax.fori_loop(0, n_rows // dot_tile, lambda i, carry: (step(i * dot_tile), carry)[1], 0)

    def q_block(slot, h, store):
        def step(start):
            tile = rows_buf[pl.ds(pl.multiple_of(start, dot_tile), dot_tile), :]
            store(start, jnp.dot(tile, wq_buf[slot, h], preferred_element_type=jnp.float32).astype(jnp.bfloat16))
        over_tiles(step)

    def kv_block(which, store):
        def step(start):
            tile = rows_buf[pl.ds(pl.multiple_of(start, dot_tile), dot_tile), :]
            both = lax.dot_general(tile, wkv_buf[which], (((1,), (1,)), ((), ())), preferred_element_type=jnp.float32)
            store(start, both.astype(jnp.bfloat16))
        over_tiles(step)

    def rows_at(start):
        return pl.ds(pl.multiple_of(start, dot_tile), dot_tile)

    def own_rows_at(start):
        return pl.ds(pl.multiple_of(member * n_rows + start, dot_tile), dot_tile)

    def own_q(h):
        def store(start, value):
            q_out[h, own_rows_at(start), :] = value
        q_block(0, h, store)

    def staged_q(stage, slot, h):
        def store(start, value):
            q_stage[stage, h, rows_at(start), :] = value
        q_block(slot, h, store)

    def late_q(h):
        def store(start, value):
            late_out[h - 1, rows_at(start), :] = value
        q_block(2, h, store)

    def own_kv():
        def store(start, value):
            k_out[0, own_rows_at(start), :] = value[:, :LANES]
            v_out[0, own_rows_at(start), :] = value[:, LANES:]
        kv_block(0, store)

    def far_kv():
        def store(start, value):
            kv_stage[0, rows_at(start), :] = value[:, :LANES]
            kv_stage[1, rows_at(start), :] = value[:, LANES:]
        kv_block(1, store)

    def from_link(j):
        link[j].wait_recv()
        side[j].start()
        hand[j].start()

    def from_side(j):
        side[j].wait_recv()
        last[j].start()

    def from_middle():
        @pl.when(chip == 0)
        def _():
            @pl.when(group == 1)
            def _():
                middle_link.wait_recv()
                middle_side.start()

            when(group == 0, middle_side.wait_recv)
            middle_hand.start()

        @pl.when(chip == 1)
        def _():
            half_link.wait_recv()
            half_side.start()
            half_hand.start()
            half_side.wait_recv()
            half_last.start()

    def complete_middle():
        when(chip == 0, middle_hand.wait_recv)

        @pl.when(chip == 1)
        def _():
            half_hand.wait_recv()
            half_last.wait_recv()

    def complete(j):
        hand[j].wait_recv()
        last[j].wait_recv()

    @pl.when(group == 0)
    def _():
        pl.semaphore_wait(ready_sem, 1)

    from_link(K_PIECE)
    normalize()
    from_link(V_PIECE)
    part[K_PIECE].wait_recv()
    part[V_PIECE].wait_recv()
    own_kv()
    from_side(K_PIECE)
    near[0].start()
    near[1].start()
    from_link(2)
    from_side(V_PIECE)
    complete(K_PIECE)
    complete(V_PIECE)
    far_kv()
    far[0].start()
    far[1].start()
    own_q(0)
    from_link(3)
    own_q(1)
    from_side(2)
    staged_q(1, 2, 0)
    from_link(4)
    complete(2)
    staged_q(2, 3, 0)

    @pl.when(core == 1)
    def _():
        far[FIRST_HEAD].start()

    from_side(3)
    complete(3)
    staged_q(2, 3, 1)
    cross[0].start()
    late_q(1)
    from_side(4)
    from_middle()
    cross[1].start()
    complete(4)
    complete_middle()
    staged_q(2, 3, 2)
    late_q(2)
    when(core == 0, lend.start)
    own_q(2)

    @pl.when(core == 1)
    def _():
        lend.wait_recv()
        cross_lent.start()
        for c in range(2):
            when(chip == c, early_far[c].start)
        cross[last_h].start()

    @pl.when(core == 0)
    def _():
        cross_kept.start()
        for copy in far[FIRST_HEAD:]:
            copy.start()

    for h in range(heads):
        part[FIRST_HEAD + h].wait_recv()
        staged_q(0, 1, h)
        if h:
            near[2 + h - 1].start()
    far[0].wait_recv()
    passed[0].start()
    far[1].wait_recv()
    passed[1].start()
    near[2 + heads - 1].start()

    for copy in part + link + hand + side + last:
        copy.wait_send()

    @pl.when(chip == 0)
    def _():
        half_link.wait_send()
        middle_hand.wait_send()
        when(group == 1, middle_side.wait_send)

    @pl.when(chip == 1)
    def _():
        when(group == 1, middle_link.wait_send)
        for copy in (half_side, half_hand, half_last):
            copy.wait_send()

    for copy in near + passed + cross[:last_h]:
        copy.wait()
    for copy in far[:FIRST_HEAD]:
        copy.wait_send()
    far[FIRST_HEAD].wait()

    @pl.when(core == 0)
    def _():
        for copy in far[FIRST_HEAD + 1:]:
            copy.wait()
        lend.wait_send()
        cross_kept.wait_send()
        cross[last_h].wait_recv()

    @pl.when(core == 1)
    def _():
        cross[last_h].wait_send()
        for c in range(2):
            when(chip == c, early_far[c].wait_send)
            when(chip == c, early_far[1 - c].wait_recv)
        cross_lent.wait()
        cross_kept.wait_recv()


def finish_kernel(q_ref, k_ref, v_ref, q_out, k_out, v_out, sems, *, early):
    member = lax.axis_index("tp")
    core = member % 2
    heads, n_rows = q_ref.shape[0], q_ref.shape[1] // 4
    late_heads = pl.ds(1, heads - 1)

    def copy_of(i, ref, out, *where):
        return pltpu.make_async_copy(ref.at[where], out.at[where], sems.at[i])

    def rows(ahead, size):
        return pl.ds(pl.multiple_of(((member + ahead) % 4) * n_rows, n_rows), size)

    always = [copy_of(i, q_ref, q_out, late_heads, rows(ahead, n_rows)) for i, ahead in enumerate((0, 1, 3))]
    always += [copy_of(3, q_ref, q_out, 0), copy_of(4, k_ref, k_out, 0), copy_of(5, v_ref, v_out, 0)]
    whole = copy_of(6, q_ref, q_out, late_heads, rows(2, n_rows))
    begun = [copy_of(6, q_ref, q_out, late_heads, rows(2, early[1 - chip])) for chip in range(2)]
    for copy in always:
        copy.start()
    pl.when(core == 0)(whole.start)
    for chip in range(2):
        pl.when(member == 2 * chip + 1)(begun[chip].start)
    for copy in always:
        copy.wait()
    pl.when(core == 0)(whole.wait)
    for chip in range(2):
        pl.when(member == 2 * chip + 1)(begun[chip].wait)


def late_kernel(after_ref, late_out, late_in, send_sem, recv_sem, *, early):
    group, member = lax.axis_index("dp"), lax.axis_index("tp")

    def exchange(chip):
        across = (group, 2 * (1 - chip) + 1)
        barrier = pltpu.get_barrier_semaphore()
        pl.semaphore_signal(barrier, inc=1, device_id=across, device_id_type=MESH)
        pl.semaphore_wait(barrier, 1)
        copies = []
        for rows in early:
            rest = pl.ds(rows, late_out.shape[1] - rows)
            copies.append(pltpu.make_async_remote_copy(src_ref=late_out.at[:, rest], dst_ref=late_in.at[:, rest], send_sem=send_sem,
                                                       recv_sem=recv_sem, device_id=across, device_id_type=MESH))
        copies[chip].start()
        copies[chip].wait_send()
        copies[1 - chip].wait_recv()

    for chip in range(2):
        pl.when(member == 2 * chip + 1)(functools.partial(exchange, chip))


def patch_kernel(before_ref, late_ref, q_out, sem, *, early):
    member = lax.axis_index("tp")
    late_heads, n_rows, _ = late_ref.shape

    def put(chip):
        start = early[1 - chip]
        base = (2 * (1 - chip) + 1) * n_rows
        copy = pltpu.make_async_copy(late_ref.at[:, pl.ds(start, n_rows - start)],
                                     q_out.at[pl.ds(1, late_heads), pl.ds(base + start, n_rows - start)], sem)
        copy.start()
        copy.wait()

    for chip in range(2):
        pl.when(member == 2 * chip + 1)(functools.partial(put, chip))


def solution(mesh):
    def local_step(x_rows, norm_gain, w_q, w_k, w_v):
        n_rows, depth = x_rows.shape
        heads, width = w_q.shape[1:]
        share = w_k.shape[1]
        members = mesh.shape["tp"]
        pieces = FIRST_HEAD + heads
        all_rows = members * n_rows
        dma = pltpu.SemaphoreType.DMA
        norm_tile = n_rows // 4
        shift, lent, early = 56, 128, (64, 128)
        vmem = pl.BlockSpec(memory_space=pltpu.VMEM)
        results = tuple(jax.ShapeDtypeStruct((n, all_rows, width), jnp.bfloat16) for n in (heads, 1, 1))
        hbm = pl.BlockSpec(memory_space=pltpu.HBM)
        late_shape = jax.ShapeDtypeStruct((heads - 1, n_rows, width), jnp.bfloat16)
        q, k, v, late = pl.pallas_call(
            functools.partial(qkv_kernel, norm_tile=norm_tile, dot_tile=256, shift=shift, lent=lent, early=early),
            out_shape=results + (late_shape,),
            in_specs=[hbm] * 5,
            out_specs=(vmem,) * 4,
            scratch_shapes=[
                pltpu.VMEM((n_rows, depth), jnp.bfloat16),
                pltpu.VMEM((depth,), jnp.float32),
                pltpu.VMEM((4, heads, depth, width), jnp.bfloat16),
                pltpu.VMEM((2, 4 * share, depth), jnp.bfloat16),
                pltpu.VMEM((3, heads, n_rows, width), jnp.bfloat16),
                pltpu.VMEM((2, n_rows, width), jnp.bfloat16),
                dma((4,)), dma(()), dma((pieces,)),
                *[dma((pieces,)) for _ in range(10)],
                dma((7,)), dma((7,)), pltpu.SemaphoreType.REGULAR, pltpu.SemaphoreType.REGULAR, pltpu.SemaphoreType.REGULAR,
                pltpu.VMEM((lent, width), jnp.bfloat16), dma((4,)), dma((2,)),
                dma((pieces,)), dma((pieces,)), dma((pieces,)), dma((pieces,)),
                dma((heads,)), dma((heads,)), dma((2,)), dma((2,)),
            ],
            compiler_params=pltpu.CompilerParams(collective_id=0, has_side_effects=True, vmem_limit_bytes=36 * 1024 * 1024),
            cost_estimate=pl.CostEstimate(flops=2 * n_rows * depth * 2048, bytes_accessed=16 * 1024 * 1024, transcendentals=0),
            name="qkv",
        )(*[pltpu.with_memory_space_constraint(a, pltpu.HBM) for a in (x_rows, norm_gain, w_q.transpose(1, 0, 2), w_k.T, w_v.T)])
        q, k, v = pl.pallas_call(
            functools.partial(finish_kernel, early=early),
            out_shape=results,
            in_specs=[vmem] * 3,
            out_specs=(hbm,) * 3,
            scratch_shapes=[dma((7,))],
            compiler_params=pltpu.CompilerParams(vmem_limit_bytes=16 * 1024 * 1024),
            name="finish",
        )(q, k, v)
        late = pl.pallas_call(
            functools.partial(late_kernel, early=early),
            out_shape=late_shape,
            in_specs=[hbm, vmem],
            out_specs=vmem,
            scratch_shapes=[dma(()), dma(())],
            compiler_params=pltpu.CompilerParams(collective_id=1, has_side_effects=True, vmem_limit_bytes=16 * 1024 * 1024),
            name="late",
        )(pltpu.with_memory_space_constraint(q, pltpu.HBM), late)
        q = pl.pallas_call(
            functools.partial(patch_kernel, early=early),
            out_shape=results[0],
            in_specs=[hbm, vmem],
            out_specs=hbm,
            scratch_shapes=[dma(())],
            input_output_aliases={0: 0},
            compiler_params=pltpu.CompilerParams(vmem_limit_bytes=16 * 1024 * 1024),
            name="patch",
        )(q, late)
        return q.transpose(1, 0, 2), k.transpose(1, 0, 2), v.transpose(1, 0, 2)

    return jax.shard_map(
        local_step, mesh=mesh,
        in_specs=(P(("dp", "tp"), None), P(None), P(None, "tp", None), P(None, "tp"), P(None, "tp")),
        out_specs=(P("dp", "tp", None), P("dp", "tp", None), P("dp", "tp", None)),
        check_vma=False,
    )
```

```python
import functools

import jax
import jax.numpy as jnp
from jax import lax
from jax.experimental import pallas as pl
from jax.experimental.pallas import tpu as pltpu
from jax.sharding import PartitionSpec as P

EPSILON = 1e-6
MESH = pl.DeviceIdType.MESH
LANES = 128
K_PIECE, V_PIECE, FIRST_HEAD = 0, 1, 2


def qkv_kernel(
    x_hbm, gain_hbm, wq_hbm, wk_hbm, wv_hbm,
    q_out, k_out, v_out, late_out,
    rows_buf, gain_buf, wq_buf, wkv_buf, q_stage, kv_stage,
    x_sem, gain_sem, load_sem,
    part_send, part_recv, link_send, link_recv, core_send, core_recv, side_send, side_recv, last_send, last_recv,
    middle_send, middle_recv, ready_sem, pair_sem, mate_sem, lent_buf, lent_sem, early_sem,
    near_send, near_recv, far_send, far_recv, cross_send, cross_recv, pass_send, pass_recv,
    *, norm_tile, dot_tile, shift, lent, early,
):
    n_rows, depth = rows_buf.shape
    heads = wq_hbm.shape[0]
    share = wk_hbm.shape[0]
    half = depth // 2
    pieces = FIRST_HEAD + heads

    group, member = lax.axis_index("dp"), lax.axis_index("tp")
    chip, core = lax.div(member, 2), lax.rem(member, 2)
    partner = (group, chip * 2 + (1 - core))
    across = (group, (1 - chip) * 2 + core)
    across_other = (group, (1 - chip) * 2 + (1 - core))
    beside = (1 - group, member)

    sources = [wk_hbm, wv_hbm] + [wq_hbm.at[h] for h in range(heads)]

    last_head = pieces - 1
    middle = pl.ds(half - shift, 2 * shift)

    def piece_at(j, slot, depth_half=None):
        if j < FIRST_HEAD:
            rows = pl.ds(pl.multiple_of(j * 2 * share + core * share, share), share)
            if depth_half is None:
                return wkv_buf.at[slot // 2, rows]
            return wkv_buf.at[slot // 2, rows, pl.ds(pl.multiple_of(depth_half * half, half), half)]
        if depth_half is None:
            return wq_buf.at[slot, j - FIRST_HEAD]
        if j == last_head:
            start = pl.multiple_of(depth_half * (half + shift), 8)
            return wq_buf.at[slot, j - FIRST_HEAD, pl.ds(start, half - shift)]
        return wq_buf.at[slot, j - FIRST_HEAD, pl.ds(pl.multiple_of(depth_half * half, half), half)]

    barrier = pltpu.get_barrier_semaphore()

    def signal(sem, device):
        pl.semaphore_signal(sem, inc=1, device_id=device, device_id_type=MESH)

    def when(condition, act):
        pl.when(condition)(act)

    signal(barrier, across)
    when(core == 1, lambda: signal(barrier, partner))
    when(group == 0, lambda: signal(barrier, beside))
    pl.semaphore_wait(barrier, 2 + group - core)

    loads = [pltpu.make_async_copy(sources[j], piece_at(j, 0), load_sem.at[j]) for j in range(pieces)]
    gain_load = pltpu.make_async_copy(gain_hbm, gain_buf, gain_sem)
    n_tiles = n_rows // norm_tile
    x_loads = [
        pltpu.make_async_copy(x_hbm.at[pl.ds(i * norm_tile, norm_tile)], rows_buf.at[pl.ds(i * norm_tile, norm_tile)], x_sem.at[i])
        for i in range(n_tiles)
    ]

    def remote(src, dst, send, recv, device):
        return pltpu.make_async_remote_copy(src_ref=src, dst_ref=dst, send_sem=send, recv_sem=recv, device_id=device, device_id_type=MESH)

    part, link, hand, side, last = [], [], [], [], []
    for j in range(pieces):
        part.append(remote(piece_at(j, 0), piece_at(j, 0 if j < FIRST_HEAD else 1), part_send.at[j], part_recv.at[j], partner))
        sent = sources[j].at[:, pl.ds(pl.multiple_of(group * half, half), half)] if j < FIRST_HEAD else piece_at(j, 0, group)
        link.append(remote(sent, piece_at(j, 2, group), link_send.at[j], link_recv.at[j], across))
        arrived, other_half = piece_at(j, 2, group), piece_at(j, 2, 1 - group)
        hand.append(remote(arrived, piece_at(j, 2 if j < FIRST_HEAD else 3, group), core_send.at[j], core_recv.at[j], partner))
        side.append(remote(arrived, arrived, side_send.at[j], side_recv.at[j], beside))
        last.append(remote(other_half, piece_at(j, 2 if j < FIRST_HEAD else 3, 1 - group), last_send.at[j], last_recv.at[j], partner))

    def middle_at(slot, part_of=None):
        if part_of is None:
            return wq_buf.at[slot, heads - 1, middle]
        return wq_buf.at[slot, heads - 1, pl.ds(pl.multiple_of(half - shift + part_of * shift, 8), shift)]

    def middle_copy(i, source_slot, slot, device, part_of=None):
        return remote(middle_at(source_slot, part_of), middle_at(slot, part_of), middle_send.at[i], middle_recv.at[i], device)

    middle_link = middle_copy(0, 0, 2, across)
    middle_side = middle_copy(1, 2, 2, beside)
    middle_hand = middle_copy(2, 2, 3, partner)
    half_link = middle_copy(3, 0, 2, across, group)
    half_side = middle_copy(4, 2, 2, beside, group)
    half_hand = middle_copy(5, 2, 3, partner, group)
    half_last = middle_copy(6, 2, 3, partner, 1 - group)

    my_rows = pl.ds(pl.multiple_of(member * n_rows, n_rows), n_rows)
    across_rows = pl.ds(pl.multiple_of(((1 - chip) * 2 + core) * n_rows, n_rows), n_rows)
    near = [remote(k_out.at[0, my_rows], k_out.at[0, my_rows], near_send.at[0], near_recv.at[0], partner),
            remote(v_out.at[0, my_rows], v_out.at[0, my_rows], near_send.at[1], near_recv.at[1], partner)]
    far = [remote(kv_stage.at[0], k_out.at[0, my_rows], far_send.at[0], far_recv.at[0], across),
           remote(kv_stage.at[1], v_out.at[0, my_rows], far_send.at[1], far_recv.at[1], across)]
    passed = [remote(k_out.at[0, across_rows], k_out.at[0, across_rows], pass_send.at[0], pass_recv.at[0], partner),
              remote(v_out.at[0, across_rows], v_out.at[0, across_rows], pass_send.at[1], pass_recv.at[1], partner)]
    cross = []
    for h in range(heads):
        near.append(remote(q_stage.at[0, h], q_out.at[h, my_rows], near_send.at[2 + h], near_recv.at[2 + h], partner))
        far.append(remote(q_stage.at[1, 0] if h == 0 else late_out.at[h - 1], q_out.at[h, my_rows], far_send.at[2 + h], far_recv.at[2 + h], across))
        cross.append(remote(q_stage.at[2, h], q_out.at[h, my_rows], cross_send.at[h], cross_recv.at[h], across_other))

    last_h = heads - 1
    lent_rows, kept_rows = pl.ds(0, lent), pl.ds(lent, n_rows - lent)
    my_kept = pl.ds(pl.multiple_of(member * n_rows + lent, lent), n_rows - lent)
    partner_lent = pl.ds(pl.multiple_of((chip * 2 + 1 - core) * n_rows, n_rows), lent)
    lend = remote(q_stage.at[2, last_h, lent_rows], lent_buf, lent_sem.at[0], lent_sem.at[1], partner)
    cross_kept = remote(q_stage.at[2, last_h, kept_rows], q_out.at[last_h, my_kept], cross_send.at[last_h], cross_recv.at[last_h], across_other)
    cross_lent = remote(lent_buf, q_out.at[last_h, partner_lent], lent_sem.at[2], lent_sem.at[3], across)
    early_far = []
    for rows in early:
        my_early = pl.ds(pl.multiple_of(member * n_rows, n_rows), rows)
        early_far.append(remote(late_out.at[:, pl.ds(0, rows)], q_out.at[pl.ds(1, heads - 1), my_early], early_sem.at[0], early_sem.at[1], across))

    for j in range(FIRST_HEAD):
        link[j].start()
    for load in loads + [gain_load] + x_loads:
        load.start()

    when(core == 0, lambda: signal(mate_sem, partner))
    when(core == 1, lambda: pl.semaphore_wait(mate_sem, 1))
    signal(pair_sem, across)
    when(group == 1, lambda: signal(ready_sem, beside))
    pl.semaphore_wait(pair_sem, 1)
    for j in range(pieces):
        loads[j].wait()
        if j >= FIRST_HEAD:
            link[j].start()
    when(chip == 0, half_link.start)
    when((chip == 1) & (group == 1), middle_link.start)
    for copy in part:
        copy.start()

    chunks = depth // LANES
    sub = 64

    def norm_step(s, carry):
        here = pl.ds(pl.multiple_of(s * sub, sub), sub)
        total = jnp.zeros((sub, LANES), jnp.float32)
        for c in range(chunks):
            wide = rows_buf[here, c * LANES:(c + 1) * LANES].astype(jnp.float32)
            total = total + wide * wide
        scale = lax.rsqrt(jnp.sum(total, axis=-1, keepdims=True) / depth + EPSILON)
        for c in range(chunks):
            cols = slice(c * LANES, (c + 1) * LANES)
            wide = rows_buf[here, cols].astype(jnp.float32)
            rows_buf[here, cols] = (wide * scale * gain_buf[cols][None, :]).astype(jnp.bfloat16)
        return carry

    def normalize():
        gain_load.wait()
        for load in x_loads:
            load.wait()
        lax.fori_loop(0, n_rows // sub, norm_step, 0)

    def over_tiles(step):
        lax.fori_loop(0, n_rows // dot_tile, lambda i, carry: (step(i * dot_tile), carry)[1], 0)

    def q_block(slot, h, store):
        def step(start):
            tile = rows_buf[pl.ds(pl.multiple_of(start, dot_tile), dot_tile), :]
            store(start, jnp.dot(tile, wq_buf[slot, h], preferred_element_type=jnp.float32).astype(jnp.bfloat16))
        over_tiles(step)

    def kv_block(which, store):
        def step(start):
            tile = rows_buf[pl.ds(pl.multiple_of(start, dot_tile), dot_tile), :]
            both = lax.dot_general(tile, wkv_buf[which], (((1,), (1,)), ((), ())), preferred_element_type=jnp.float32)
            store(start, both.astype(jnp.bfloat16))
        over_tiles(step)

    def rows_at(start):
        return pl.ds(pl.multiple_of(start, dot_tile), dot_tile)

    def own_rows_at(start):
        return pl.ds(pl.multiple_of(member * n_rows + start, dot_tile), dot_tile)

    def own_q(h):
        def store(start, value):
            q_out[h, own_rows_at(start), :] = value
        q_block(0, h, store)

    def staged_q(stage, slot, h):
        def store(start, value):
            q_stage[stage, h, rows_at(start), :] = value
        q_block(slot, h, store)

    def late_q(h):
        def store(start, value):
            late_out[h - 1, rows_at(start), :] = value
        q_block(2, h, store)

    def own_kv():
        def store(start, value):
            k_out[0, own_rows_at(start), :] = value[:, :LANES]
            v_out[0, own_rows_at(start), :] = value[:, LANES:]
        kv_block(0, store)

    def far_kv():
        def store(start, value):
            kv_stage[0, rows_at(start), :] = value[:, :LANES]
            kv_stage[1, rows_at(start), :] = value[:, LANES:]
        kv_block(1, store)

    def from_link(j):
        link[j].wait_recv()
        side[j].start()
        hand[j].start()

    def from_side(j):
        side[j].wait_recv()
        last[j].start()

    def from_middle():
        @pl.when(chip == 0)
        def _():
            @pl.when(group == 1)
            def _():
                middle_link.wait_recv()
                middle_side.start()

            when(group == 0, middle_side.wait_recv)
            middle_hand.start()

        @pl.when(chip == 1)
        def _():
            half_link.wait_recv()
            half_side.start()
            half_hand.start()
            half_side.wait_recv()
            half_last.start()

    def complete_middle():
        when(chip == 0, middle_hand.wait_recv)

        @pl.when(chip == 1)
        def _():
            half_hand.wait_recv()
            half_last.wait_recv()

    def complete(j):
        hand[j].wait_recv()
        last[j].wait_recv()

    @pl.when(group == 0)
    def _():
        pl.semaphore_wait(ready_sem, 1)

    from_link(K_PIECE)
    normalize()
    from_link(V_PIECE)
    part[K_PIECE].wait_recv()
    part[V_PIECE].wait_recv()
    own_kv()
    from_side(K_PIECE)
    near[0].start()
    near[1].start()
    from_link(2)
    from_side(V_PIECE)
    complete(K_PIECE)
    complete(V_PIECE)
    far_kv()
    far[0].start()
    far[1].start()
    own_q(0)
    from_link(3)
    own_q(1)
    from_side(2)
    staged_q(1, 2, 0)
    from_link(4)
    complete(2)
    staged_q(2, 3, 0)

    @pl.when(core == 1)
    def _():
        far[FIRST_HEAD].start()

    from_side(3)
    complete(3)
    staged_q(2, 3, 1)
    cross[0].start()
    late_q(1)
    from_side(4)
    from_middle()
    cross[1].start()
    complete(4)
    complete_middle()
    staged_q(2, 3, 2)
    late_q(2)
    when(core == 0, lend.start)
    own_q(2)

    @pl.when(core == 1)
    def _():
        lend.wait_recv()
        cross_lent.start()
        for c in range(2):
            when(chip == c, early_far[c].start)
        cross[last_h].start()

    @pl.when(core == 0)
    def _():
        cross_kept.start()
        for copy in far[FIRST_HEAD:]:
            copy.start()

    for h in range(heads):
        part[FIRST_HEAD + h].wait_recv()
        staged_q(0, 1, h)
        if h:
            near[2 + h - 1].start()
    far[0].wait_recv()
    passed[0].start()
    far[1].wait_recv()
    passed[1].start()
    near[2 + heads - 1].start()

    for copy in part + link + hand + side + last:
        copy.wait_send()

    @pl.when(chip == 0)
    def _():
        half_link.wait_send()
        middle_hand.wait_send()
        when(group == 1, middle_side.wait_send)

    @pl.when(chip == 1)
    def _():
        when(group == 1, middle_link.wait_send)
        for copy in (half_side, half_hand, half_last):
            copy.wait_send()

    for copy in near + passed + cross[:last_h]:
        copy.wait()
    for copy in far[:FIRST_HEAD]:
        copy.wait_send()
    far[FIRST_HEAD].wait()

    @pl.when(core == 0)
    def _():
        for copy in far[FIRST_HEAD + 1:]:
            copy.wait()
        lend.wait_send()
        cross_kept.wait_send()
        cross[last_h].wait_recv()

    @pl.when(core == 1)
    def _():
        cross[last_h].wait_send()
        for c in range(2):
            when(chip == c, early_far[c].wait_send)
            when(chip == c, early_far[1 - c].wait_recv)
        cross_lent.wait()
        cross_kept.wait_recv()


def finish_kernel(q_ref, k_ref, v_ref, q_out, k_out, v_out, sems, *, early):
    member = lax.axis_index("tp")
    core = member % 2
    heads, n_rows = q_ref.shape[0], q_ref.shape[1] // 4
    late_heads = pl.ds(1, heads - 1)

    def copy_of(i, ref, out, *where):
        return pltpu.make_async_copy(ref.at[where], out.at[where], sems.at[i])

    def rows(ahead, size):
        return pl.ds(pl.multiple_of(((member + ahead) % 4) * n_rows, n_rows), size)

    always = [copy_of(i, q_ref, q_out, late_heads, rows(ahead, n_rows)) for i, ahead in enumerate((0, 1, 3))]
    always += [copy_of(3, q_ref, q_out, 0), copy_of(4, k_ref, k_out, 0), copy_of(5, v_ref, v_out, 0)]
    whole = copy_of(6, q_ref, q_out, late_heads, rows(2, n_rows))
    begun = [copy_of(6, q_ref, q_out, late_heads, rows(2, early[1 - chip])) for chip in range(2)]
    for copy in always:
        copy.start()
    pl.when(core == 0)(whole.start)
    for chip in range(2):
        pl.when(member == 2 * chip + 1)(begun[chip].start)
    for copy in always:
        copy.wait()
    pl.when(core == 0)(whole.wait)
    for chip in range(2):
        pl.when(member == 2 * chip + 1)(begun[chip].wait)


def late_kernel(after_ref, late_out, late_in, send_sem, recv_sem, *, early):
    group, member = lax.axis_index("dp"), lax.axis_index("tp")

    def exchange(chip):
        across = (group, 2 * (1 - chip) + 1)
        barrier = pltpu.get_barrier_semaphore()
        pl.semaphore_signal(barrier, inc=1, device_id=across, device_id_type=MESH)
        pl.semaphore_wait(barrier, 1)
        copies = []
        for rows in early:
            rest = pl.ds(rows, late_out.shape[1] - rows)
            copies.append(pltpu.make_async_remote_copy(src_ref=late_out.at[:, rest], dst_ref=late_in.at[:, rest], send_sem=send_sem,
                                                       recv_sem=recv_sem, device_id=across, device_id_type=MESH))
        copies[chip].start()
        copies[chip].wait_send()
        copies[1 - chip].wait_recv()

    for chip in range(2):
        pl.when(member == 2 * chip + 1)(functools.partial(exchange, chip))


def patch_kernel(before_ref, late_ref, q_out, sem, *, early):
    member = lax.axis_index("tp")
    late_heads, n_rows, _ = late_ref.shape

    def put(chip):
        start = early[1 - chip]
        base = (2 * (1 - chip) + 1) * n_rows
        copy = pltpu.make_async_copy(late_ref.at[:, pl.ds(start, n_rows - start)],
                                     q_out.at[pl.ds(1, late_heads), pl.ds(base + start, n_rows - start)], sem)
        copy.start()
        copy.wait()

    for chip in range(2):
        pl.when(member == 2 * chip + 1)(functools.partial(put, chip))


def solution(mesh):
    def local_step(x_rows, norm_gain, w_q, w_k, w_v):
        n_rows, depth = x_rows.shape
        heads, width = w_q.shape[1:]
        share = w_k.shape[1]
        members = mesh.shape["tp"]
        pieces = FIRST_HEAD + heads
        all_rows = members * n_rows
        dma = pltpu.SemaphoreType.DMA
        norm_tile = n_rows // 4
        shift, lent, early = 56, 32, (112, 176)
        vmem = pl.BlockSpec(memory_space=pltpu.VMEM)
        results = tuple(jax.ShapeDtypeStruct((n, all_rows, width), jnp.bfloat16) for n in (heads, 1, 1))
        hbm = pl.BlockSpec(memory_space=pltpu.HBM)
        late_shape = jax.ShapeDtypeStruct((heads - 1, n_rows, width), jnp.bfloat16)
        q, k, v, late = pl.pallas_call(
            functools.partial(qkv_kernel, norm_tile=norm_tile, dot_tile=256, shift=shift, lent=lent, early=early),
            out_shape=results + (late_shape,),
            in_specs=[hbm] * 5,
            out_specs=(vmem,) * 4,
            scratch_shapes=[
                pltpu.VMEM((n_rows, depth), jnp.bfloat16),
                pltpu.VMEM((depth,), jnp.float32),
                pltpu.VMEM((4, heads, depth, width), jnp.bfloat16),
                pltpu.VMEM((2, 4 * share, depth), jnp.bfloat16),
                pltpu.VMEM((3, heads, n_rows, width), jnp.bfloat16),
                pltpu.VMEM((2, n_rows, width), jnp.bfloat16),
                dma((4,)), dma(()), dma((pieces,)),
                *[dma((pieces,)) for _ in range(10)],
                dma((7,)), dma((7,)), pltpu.SemaphoreType.REGULAR, pltpu.SemaphoreType.REGULAR, pltpu.SemaphoreType.REGULAR,
                pltpu.VMEM((lent, width), jnp.bfloat16), dma((4,)), dma((2,)),
                dma((pieces,)), dma((pieces,)), dma((pieces,)), dma((pieces,)),
                dma((heads,)), dma((heads,)), dma((2,)), dma((2,)),
            ],
            compiler_params=pltpu.CompilerParams(collective_id=0, has_side_effects=True, vmem_limit_bytes=36 * 1024 * 1024),
            cost_estimate=pl.CostEstimate(flops=2 * n_rows * depth * 2048, bytes_accessed=16 * 1024 * 1024, transcendentals=0),
            name="qkv",
        )(*[pltpu.with_memory_space_constraint(a, pltpu.HBM) for a in (x_rows, norm_gain, w_q.transpose(1, 0, 2), w_k.T, w_v.T)])
        q, k, v = pl.pallas_call(
            functools.partial(finish_kernel, early=early),
            out_shape=results,
            in_specs=[vmem] * 3,
            out_specs=(hbm,) * 3,
            scratch_shapes=[dma((7,))],
            compiler_params=pltpu.CompilerParams(vmem_limit_bytes=16 * 1024 * 1024),
            name="finish",
        )(q, k, v)
        late = pl.pallas_call(
            functools.partial(late_kernel, early=early),
            out_shape=late_shape,
            in_specs=[hbm, vmem],
            out_specs=vmem,
            scratch_shapes=[dma(()), dma(())],
            compiler_params=pltpu.CompilerParams(collective_id=1, has_side_effects=True, vmem_limit_bytes=16 * 1024 * 1024),
            name="late",
        )(pltpu.with_memory_space_constraint(q, pltpu.HBM), late)
        q = pl.pallas_call(
            functools.partial(patch_kernel, early=early),
            out_shape=results[0],
            in_specs=[hbm, vmem],
            out_specs=hbm,
            scratch_shapes=[dma(())],
            input_output_aliases={0: 0},
            compiler_params=pltpu.CompilerParams(vmem_limit_bytes=16 * 1024 * 1024),
            name="patch",
        )(q, late)
        return q.transpose(1, 0, 2), k.transpose(1, 0, 2), v.transpose(1, 0, 2)

    return jax.shard_map(
        local_step, mesh=mesh,
        in_specs=(P(("dp", "tp"), None), P(None), P(None, "tp", None), P(None, "tp"), P(None, "tp")),
        out_specs=(P("dp", "tp", None), P("dp", "tp", None), P("dp", "tp", None)),
        check_vma=False,
    )
```

```python
import functools

import jax
import jax.numpy as jnp
from jax import lax
from jax.experimental import pallas as pl
from jax.experimental.pallas import tpu as pltpu
from jax.sharding import PartitionSpec as P

EPSILON = 1e-6
MESH = pl.DeviceIdType.MESH
LANES = 128
K_PIECE, V_PIECE, FIRST_HEAD = 0, 1, 2


def qkv_kernel(
    x_hbm, gain_hbm, wq_hbm, wk_hbm, wv_hbm,
    q_out, k_out, v_out, late_out,
    rows_buf, gain_buf, wq_buf, wkv_buf, q_stage, kv_stage,
    x_sem, gain_sem, load_sem,
    part_send, part_recv, link_send, link_recv, core_send, core_recv, side_send, side_recv, last_send, last_recv,
    middle_send, middle_recv, ready_sem, pair_sem, mate_sem, lent_buf, lent_sem, early_sem,
    near_send, near_recv, far_send, far_recv, cross_send, cross_recv, pass_send, pass_recv,
    *, norm_tile, dot_tile, shift, lent, early,
):
    n_rows, depth = rows_buf.shape
    heads = wq_hbm.shape[0]
    share = wk_hbm.shape[0]
    half = depth // 2
    pieces = FIRST_HEAD + heads

    group, member = lax.axis_index("dp"), lax.axis_index("tp")
    chip, core = lax.div(member, 2), lax.rem(member, 2)
    partner = (group, chip * 2 + (1 - core))
    across = (group, (1 - chip) * 2 + core)
    across_other = (group, (1 - chip) * 2 + (1 - core))
    beside = (1 - group, member)

    sources = [wk_hbm, wv_hbm] + [wq_hbm.at[h] for h in range(heads)]

    last_head = pieces - 1
    middle = pl.ds(half - shift, 2 * shift)

    def piece_at(j, slot, depth_half=None):
        if j < FIRST_HEAD:
            rows = pl.ds(pl.multiple_of(j * 2 * share + core * share, share), share)
            if depth_half is None:
                return wkv_buf.at[slot // 2, rows]
            return wkv_buf.at[slot // 2, rows, pl.ds(pl.multiple_of(depth_half * half, half), half)]
        if depth_half is None:
            return wq_buf.at[slot, j - FIRST_HEAD]
        if j == last_head:
            start = pl.multiple_of(depth_half * (half + shift), 8)
            return wq_buf.at[slot, j - FIRST_HEAD, pl.ds(start, half - shift)]
        return wq_buf.at[slot, j - FIRST_HEAD, pl.ds(pl.multiple_of(depth_half * half, half), half)]

    barrier = pltpu.get_barrier_semaphore()

    def signal(sem, device):
        pl.semaphore_signal(sem, inc=1, device_id=device, device_id_type=MESH)

    def when(condition, act):
        pl.when(condition)(act)

    signal(barrier, across)
    when(core == 1, lambda: signal(barrier, partner))
    when(group == 0, lambda: signal(barrier, beside))
    pl.semaphore_wait(barrier, 2 + group - core)

    loads = [pltpu.make_async_copy(sources[j], piece_at(j, 0), load_sem.at[j]) for j in range(pieces)]
    gain_load = pltpu.make_async_copy(gain_hbm, gain_buf, gain_sem)
    n_tiles = n_rows // norm_tile
    x_loads = [
        pltpu.make_async_copy(x_hbm.at[pl.ds(i * norm_tile, norm_tile)], rows_buf.at[pl.ds(i * norm_tile, norm_tile)], x_sem.at[i])
        for i in range(n_tiles)
    ]

    def remote(src, dst, send, recv, device):
        return pltpu.make_async_remote_copy(src_ref=src, dst_ref=dst, send_sem=send, recv_sem=recv, device_id=device, device_id_type=MESH)

    part, link, hand, side, last = [], [], [], [], []
    for j in range(pieces):
        part.append(remote(piece_at(j, 0), piece_at(j, 0 if j < FIRST_HEAD else 1), part_send.at[j], part_recv.at[j], partner))
        sent = sources[j].at[:, pl.ds(pl.multiple_of(group * half, half), half)] if j < FIRST_HEAD else piece_at(j, 0, group)
        link.append(remote(sent, piece_at(j, 2, group), link_send.at[j], link_recv.at[j], across))
        arrived, other_half = piece_at(j, 2, group), piece_at(j, 2, 1 - group)
        hand.append(remote(arrived, piece_at(j, 2 if j < FIRST_HEAD else 3, group), core_send.at[j], core_recv.at[j], partner))
        side.append(remote(arrived, arrived, side_send.at[j], side_recv.at[j], beside))
        last.append(remote(other_half, piece_at(j, 2 if j < FIRST_HEAD else 3, 1 - group), last_send.at[j], last_recv.at[j], partner))

    def middle_at(slot, part_of=None):
        if part_of is None:
            return wq_buf.at[slot, heads - 1, middle]
        return wq_buf.at[slot, heads - 1, pl.ds(pl.multiple_of(half - shift + part_of * shift, 8), shift)]

    def middle_copy(i, source_slot, slot, device, part_of=None):
        return remote(middle_at(source_slot, part_of), middle_at(slot, part_of), middle_send.at[i], middle_recv.at[i], device)

    middle_link = middle_copy(0, 0, 2, across)
    middle_side = middle_copy(1, 2, 2, beside)
    middle_hand = middle_copy(2, 2, 3, partner)
    half_link = middle_copy(3, 0, 2, across, group)
    half_side = middle_copy(4, 2, 2, beside, group)
    half_hand = middle_copy(5, 2, 3, partner, group)
    half_last = middle_copy(6, 2, 3, partner, 1 - group)

    my_rows = pl.ds(pl.multiple_of(member * n_rows, n_rows), n_rows)
    across_rows = pl.ds(pl.multiple_of(((1 - chip) * 2 + core) * n_rows, n_rows), n_rows)
    near = [remote(k_out.at[0, my_rows], k_out.at[0, my_rows], near_send.at[0], near_recv.at[0], partner),
            remote(v_out.at[0, my_rows], v_out.at[0, my_rows], near_send.at[1], near_recv.at[1], partner)]
    far = [remote(kv_stage.at[0], k_out.at[0, my_rows], far_send.at[0], far_recv.at[0], across),
           remote(kv_stage.at[1], v_out.at[0, my_rows], far_send.at[1], far_recv.at[1], across)]
    passed = [remote(k_out.at[0, across_rows], k_out.at[0, across_rows], pass_send.at[0], pass_recv.at[0], partner),
              remote(v_out.at[0, across_rows], v_out.at[0, across_rows], pass_send.at[1], pass_recv.at[1], partner)]
    cross = []
    for h in range(heads):
        near.append(remote(q_stage.at[0, h], q_out.at[h, my_rows], near_send.at[2 + h], near_recv.at[2 + h], partner))
        far.append(remote(q_stage.at[1, 0] if h == 0 else late_out.at[h - 1], q_out.at[h, my_rows], far_send.at[2 + h], far_recv.at[2 + h], across))
        cross.append(remote(q_stage.at[2, h], q_out.at[h, my_rows], cross_send.at[h], cross_recv.at[h], across_other))

    last_h = heads - 1
    lent_rows, kept_rows = pl.ds(0, lent), pl.ds(lent, n_rows - lent)
    my_kept = pl.ds(pl.multiple_of(member * n_rows + lent, lent), n_rows - lent)
    partner_lent = pl.ds(pl.multiple_of((chip * 2 + 1 - core) * n_rows, n_rows), lent)
    lend = remote(q_stage.at[2, last_h, lent_rows], lent_buf, lent_sem.at[0], lent_sem.at[1], partner)
    cross_kept = remote(q_stage.at[2, last_h, kept_rows], q_out.at[last_h, my_kept], cross_send.at[last_h], cross_recv.at[last_h], across_other)
    cross_lent = remote(lent_buf, q_out.at[last_h, partner_lent], lent_sem.at[2], lent_sem.at[3], across)
    early_far = []
    for rows in early:
        my_early = pl.ds(pl.multiple_of(member * n_rows, n_rows), rows)
        early_far.append(remote(late_out.at[:, pl.ds(0, rows)], q_out.at[pl.ds(1, heads - 1), my_early], early_sem.at[0], early_sem.at[1], across))

    for j in range(FIRST_HEAD):
        link[j].start()
    for load in loads + [gain_load] + x_loads:
        load.start()

    when(core == 0, lambda: signal(mate_sem, partner))
    when(core == 1, lambda: pl.semaphore_wait(mate_sem, 1))
    signal(pair_sem, across)
    when(group == 1, lambda: signal(ready_sem, beside))
    pl.semaphore_wait(pair_sem, 1)
    for j in range(pieces):
        loads[j].wait()
        if j >= FIRST_HEAD:
            link[j].start()
    when(chip == 0, half_link.start)
    when((chip == 1) & (group == 1), middle_link.start)
    for copy in part:
        copy.start()

    chunks = depth // LANES
    sub = 64

    def norm_step(s, carry):
        here = pl.ds(pl.multiple_of(s * sub, sub), sub)
        total = jnp.zeros((sub, LANES), jnp.float32)
        for c in range(chunks):
            wide = rows_buf[here, c * LANES:(c + 1) * LANES].astype(jnp.float32)
            total = total + wide * wide
        scale = lax.rsqrt(jnp.sum(total, axis=-1, keepdims=True) / depth + EPSILON)
        for c in range(chunks):
            cols = slice(c * LANES, (c + 1) * LANES)
            wide = rows_buf[here, cols].astype(jnp.float32)
            rows_buf[here, cols] = (wide * scale * gain_buf[cols][None, :]).astype(jnp.bfloat16)
        return carry

    def normalize():
        gain_load.wait()
        for load in x_loads:
            load.wait()
        lax.fori_loop(0, n_rows // sub, norm_step, 0)

    def over_tiles(step):
        lax.fori_loop(0, n_rows // dot_tile, lambda i, carry: (step(i * dot_tile), carry)[1], 0)

    def q_block(slot, h, store):
        def step(start):
            tile = rows_buf[pl.ds(pl.multiple_of(start, dot_tile), dot_tile), :]
            store(start, jnp.dot(tile, wq_buf[slot, h], preferred_element_type=jnp.float32).astype(jnp.bfloat16))
        over_tiles(step)

    def kv_block(which, store):
        def step(start):
            tile = rows_buf[pl.ds(pl.multiple_of(start, dot_tile), dot_tile), :]
            both = lax.dot_general(tile, wkv_buf[which], (((1,), (1,)), ((), ())), preferred_element_type=jnp.float32)
            store(start, both.astype(jnp.bfloat16))
        over_tiles(step)

    def rows_at(start):
        return pl.ds(pl.multiple_of(start, dot_tile), dot_tile)

    def own_rows_at(start):
        return pl.ds(pl.multiple_of(member * n_rows + start, dot_tile), dot_tile)

    def own_q(h):
        def store(start, value):
            q_out[h, own_rows_at(start), :] = value
        q_block(0, h, store)

    def staged_q(stage, slot, h):
        def store(start, value):
            q_stage[stage, h, rows_at(start), :] = value
        q_block(slot, h, store)

    def late_q(h):
        def store(start, value):
            late_out[h - 1, rows_at(start), :] = value
        q_block(2, h, store)

    def own_kv():
        def store(start, value):
            k_out[0, own_rows_at(start), :] = value[:, :LANES]
            v_out[0, own_rows_at(start), :] = value[:, LANES:]
        kv_block(0, store)

    def far_kv():
        def store(start, value):
            kv_stage[0, rows_at(start), :] = value[:, :LANES]
            kv_stage[1, rows_at(start), :] = value[:, LANES:]
        kv_block(1, store)

    def from_link(j):
        link[j].wait_recv()
        side[j].start()
        hand[j].start()

    def from_side(j):
        side[j].wait_recv()
        last[j].start()

    def from_middle():
        @pl.when(chip == 0)
        def _():
            @pl.when(group == 1)
            def _():
                middle_link.wait_recv()
                middle_side.start()

            when(group == 0, middle_side.wait_recv)
            middle_hand.start()

        @pl.when(chip == 1)
        def _():
            half_link.wait_recv()
            half_side.start()
            half_hand.start()
            half_side.wait_recv()
            half_last.start()

    def complete_middle():
        when(chip == 0, middle_hand.wait_recv)

        @pl.when(chip == 1)
        def _():
            half_hand.wait_recv()
            half_last.wait_recv()

    def complete(j):
        hand[j].wait_recv()
        last[j].wait_recv()

    @pl.when(group == 0)
    def _():
        pl.semaphore_wait(ready_sem, 1)

    from_link(K_PIECE)
    normalize()
    from_link(V_PIECE)
    part[K_PIECE].wait_recv()
    part[V_PIECE].wait_recv()
    own_kv()
    from_side(K_PIECE)
    near[0].start()
    near[1].start()
    from_link(2)
    from_side(V_PIECE)
    complete(K_PIECE)
    complete(V_PIECE)
    far_kv()
    far[0].start()
    far[1].start()
    own_q(0)
    from_link(3)
    own_q(1)
    from_side(2)
    staged_q(1, 2, 0)
    from_link(4)
    complete(2)
    staged_q(2, 3, 0)

    @pl.when(core == 1)
    def _():
        far[FIRST_HEAD].start()

    from_side(3)
    complete(3)
    staged_q(2, 3, 1)
    cross[0].start()
    late_q(1)
    from_side(4)
    from_middle()
    cross[1].start()
    complete(4)
    complete_middle()
    staged_q(2, 3, 2)
    late_q(2)
    when(core == 0, lend.start)
    own_q(2)

    @pl.when(core == 1)
    def _():
        lend.wait_recv()
        cross_lent.start()
        for c in range(2):
            when(chip == c, early_far[c].start)
        cross[last_h].start()

    @pl.when(core == 0)
    def _():
        cross_kept.start()
        for copy in far[FIRST_HEAD:]:
            copy.start()

    for h in range(heads):
        part[FIRST_HEAD + h].wait_recv()
        staged_q(0, 1, h)
        if h:
            near[2 + h - 1].start()
    far[0].wait_recv()
    passed[0].start()
    far[1].wait_recv()
    passed[1].start()
    near[2 + heads - 1].start()

    for copy in part + link + hand + side + last:
        copy.wait_send()

    @pl.when(chip == 0)
    def _():
        half_link.wait_send()
        middle_hand.wait_send()
        when(group == 1, middle_side.wait_send)

    @pl.when(chip == 1)
    def _():
        when(group == 1, middle_link.wait_send)
        for copy in (half_side, half_hand, half_last):
            copy.wait_send()

    for copy in near + passed + cross[:last_h]:
        copy.wait()
    for copy in far[:FIRST_HEAD]:
        copy.wait_send()
    far[FIRST_HEAD].wait()

    @pl.when(core == 0)
    def _():
        for copy in far[FIRST_HEAD + 1:]:
            copy.wait()
        lend.wait_send()
        cross_kept.wait_send()
        cross[last_h].wait_recv()

    @pl.when(core == 1)
    def _():
        cross[last_h].wait_send()
        for c in range(2):
            when(chip == c, early_far[c].wait_send)
            when(chip == c, early_far[1 - c].wait_recv)
        cross_lent.wait()
        cross_kept.wait_recv()


def finish_kernel(q_ref, k_ref, v_ref, q_out, k_out, v_out, sems, *, early):
    member = lax.axis_index("tp")
    core = member % 2
    heads, n_rows = q_ref.shape[0], q_ref.shape[1] // 4
    late_heads = pl.ds(1, heads - 1)

    def copy_of(i, ref, out, *where):
        return pltpu.make_async_copy(ref.at[where], out.at[where], sems.at[i])

    def rows(ahead, size):
        return pl.ds(pl.multiple_of(((member + ahead) % 4) * n_rows, n_rows), size)

    always = [copy_of(i, q_ref, q_out, late_heads, rows(ahead, n_rows)) for i, ahead in enumerate((0, 1, 3))]
    always += [copy_of(3, q_ref, q_out, 0), copy_of(4, k_ref, k_out, 0), copy_of(5, v_ref, v_out, 0)]
    whole = copy_of(6, q_ref, q_out, late_heads, rows(2, n_rows))
    begun = [copy_of(6, q_ref, q_out, late_heads, rows(2, early[1 - chip])) for chip in range(2)]
    for copy in always:
        copy.start()
    pl.when(core == 0)(whole.start)
    for chip in range(2):
        pl.when(member == 2 * chip + 1)(begun[chip].start)
    for copy in always:
        copy.wait()
    pl.when(core == 0)(whole.wait)
    for chip in range(2):
        pl.when(member == 2 * chip + 1)(begun[chip].wait)


def late_kernel(after_ref, late_out, late_in, send_sem, recv_sem, *, early):
    group, member = lax.axis_index("dp"), lax.axis_index("tp")

    def exchange(chip):
        across = (group, 2 * (1 - chip) + 1)
        barrier = pltpu.get_barrier_semaphore()
        pl.semaphore_signal(barrier, inc=1, device_id=across, device_id_type=MESH)
        pl.semaphore_wait(barrier, 1)
        copies = []
        for rows in early:
            rest = pl.ds(rows, late_out.shape[1] - rows)
            copies.append(pltpu.make_async_remote_copy(src_ref=late_out.at[:, rest], dst_ref=late_in.at[:, rest], send_sem=send_sem,
                                                       recv_sem=recv_sem, device_id=across, device_id_type=MESH))
        copies[chip].start()
        copies[chip].wait_send()
        copies[1 - chip].wait_recv()

    for chip in range(2):
        pl.when(member == 2 * chip + 1)(functools.partial(exchange, chip))


def patch_kernel(before_ref, late_ref, q_out, sem, *, early):
    member = lax.axis_index("tp")
    late_heads, n_rows, _ = late_ref.shape

    def put(chip):
        start = early[1 - chip]
        base = (2 * (1 - chip) + 1) * n_rows
        copy = pltpu.make_async_copy(late_ref.at[:, pl.ds(start, n_rows - start)],
                                     q_out.at[pl.ds(1, late_heads), pl.ds(base + start, n_rows - start)], sem)
        copy.start()
        copy.wait()

    for chip in range(2):
        pl.when(member == 2 * chip + 1)(functools.partial(put, chip))


def solution(mesh):
    def local_step(x_rows, norm_gain, w_q, w_k, w_v):
        n_rows, depth = x_rows.shape
        heads, width = w_q.shape[1:]
        share = w_k.shape[1]
        members = mesh.shape["tp"]
        pieces = FIRST_HEAD + heads
        all_rows = members * n_rows
        dma = pltpu.SemaphoreType.DMA
        norm_tile = n_rows // 4
        shift, lent, early = 48, 32, (112, 176)
        vmem = pl.BlockSpec(memory_space=pltpu.VMEM)
        results = tuple(jax.ShapeDtypeStruct((n, all_rows, width), jnp.bfloat16) for n in (heads, 1, 1))
        hbm = pl.BlockSpec(memory_space=pltpu.HBM)
        late_shape = jax.ShapeDtypeStruct((heads - 1, n_rows, width), jnp.bfloat16)
        q, k, v, late = pl.pallas_call(
            functools.partial(qkv_kernel, norm_tile=norm_tile, dot_tile=256, shift=shift, lent=lent, early=early),
            out_shape=results + (late_shape,),
            in_specs=[hbm] * 5,
            out_specs=(vmem,) * 4,
            scratch_shapes=[
                pltpu.VMEM((n_rows, depth), jnp.bfloat16),
                pltpu.VMEM((depth,), jnp.float32),
                pltpu.VMEM((4, heads, depth, width), jnp.bfloat16),
                pltpu.VMEM((2, 4 * share, depth), jnp.bfloat16),
                pltpu.VMEM((3, heads, n_rows, width), jnp.bfloat16),
                pltpu.VMEM((2, n_rows, width), jnp.bfloat16),
                dma((4,)), dma(()), dma((pieces,)),
                *[dma((pieces,)) for _ in range(10)],
                dma((7,)), dma((7,)), pltpu.SemaphoreType.REGULAR, pltpu.SemaphoreType.REGULAR, pltpu.SemaphoreType.REGULAR,
                pltpu.VMEM((lent, width), jnp.bfloat16), dma((4,)), dma((2,)),
                dma((pieces,)), dma((pieces,)), dma((pieces,)), dma((pieces,)),
                dma((heads,)), dma((heads,)), dma((2,)), dma((2,)),
            ],
            compiler_params=pltpu.CompilerParams(collective_id=0, has_side_effects=True, vmem_limit_bytes=36 * 1024 * 1024),
            cost_estimate=pl.CostEstimate(flops=2 * n_rows * depth * 2048, bytes_accessed=16 * 1024 * 1024, transcendentals=0),
            name="qkv",
        )(*[pltpu.with_memory_space_constraint(a, pltpu.HBM) for a in (x_rows, norm_gain, w_q.transpose(1, 0, 2), w_k.T, w_v.T)])
        q, k, v = pl.pallas_call(
            functools.partial(finish_kernel, early=early),
            out_shape=results,
            in_specs=[vmem] * 3,
            out_specs=(hbm,) * 3,
            scratch_shapes=[dma((7,))],
            compiler_params=pltpu.CompilerParams(vmem_limit_bytes=16 * 1024 * 1024),
            name="finish",
        )(q, k, v)
        late = pl.pallas_call(
            functools.partial(late_kernel, early=early),
            out_shape=late_shape,
            in_specs=[hbm, vmem],
            out_specs=vmem,
            scratch_shapes=[dma(()), dma(())],
            compiler_params=pltpu.CompilerParams(collective_id=1, has_side_effects=True, vmem_limit_bytes=16 * 1024 * 1024),
            name="late",
        )(pltpu.with_memory_space_constraint(q, pltpu.HBM), late)
        q = pl.pallas_call(
            functools.partial(patch_kernel, early=early),
            out_shape=results[0],
            in_specs=[hbm, vmem],
            out_specs=hbm,
            scratch_shapes=[dma(())],
            input_output_aliases={0: 0},
            compiler_params=pltpu.CompilerParams(vmem_limit_bytes=16 * 1024 * 1024),
            name="patch",
        )(q, late)
        return q.transpose(1, 0, 2), k.transpose(1, 0, 2), v.transpose(1, 0, 2)

    return jax.shard_map(
        local_step, mesh=mesh,
        in_specs=(P(("dp", "tp"), None), P(None), P(None, "tp", None), P(None, "tp"), P(None, "tp")),
        out_specs=(P("dp", "tp", None), P("dp", "tp", None), P("dp", "tp", None)),
        check_vma=False,
    )
```
